128 devices in a mesh: fsdp: 64 (over z, y, x), cp: 2 (over core).
Axes of the slice: x: 4, y: 4, z: 4, core: 2. Of those that a mesh axis runs over, the one named last changes fastest.
Arguments:
- hidden: bfloat16 [64, 1024, 2048], P('fsdp', 'cp')
- doc_ids: int32 [64, 1024], P('fsdp', 'cp')
- doc_pos: int32 [64, 1024], P('fsdp', 'cp')
- grad_out: bfloat16 [64, 1024, 2048], P('fsdp', 'cp')
- w_query: bfloat16 [2048, 8, 256], P('fsdp')
- w_key: bfloat16 [2048, 1, 256], P('fsdp')
- w_value: bfloat16 [2048, 1, 256], P('fsdp')
- w_out: bfloat16 [8, 256, 2048], P(None, None, 'fsdp')
- gain_pre: bfloat16 [2048], P('fsdp')
- gain_post: bfloat16 [2048], P('fsdp')
Outputs:
- output 1: bfloat16 [64, 1024, 2048], P('fsdp', 'cp')
- output 2: bfloat16 [64, 1024, 2048], P('fsdp', 'cp')
- output 3: float32 [2048, 8, 256], P('fsdp')
- output 4: float32 [2048, 1, 256], P('fsdp')
- output 5: float32 [2048, 1, 256], P('fsdp')
- output 6: float32 [8, 256, 2048], P(None, None, 'fsdp')
- output 7: float32 [2048], P('fsdp')
- output 8: float32 [2048], P('fsdp')
All inputs are finite; a program needn't handle non-finite values.
Results may differ from the reference program's by a relative error of at most 0.0170023.
Values are sent between devices in bfloat16 or wider.
A program may use at most 1 GiB of HBM per device.

```python
import jax
import jax.numpy as jnp
from jax import lax

BATCH = 64
SEQ = 1024
DIM = 2048
HEADS = 8
KV_HEADS = 1
HEAD = 256
SOFT_CAP = 50.0
NORM_EPS = 1e-6
ROPE_BASE = 10000.0
GROUPS = HEADS // KV_HEADS
QUERY_BLOCK = min(SEQ, 128)
N_BLOCKS = SEQ // QUERY_BLOCK


def pre_scalar():
    return HEAD if HEAD >= 256 else DIM // HEADS


def setup_inputs(seed: int = 0) -> dict:
    rng_key = jax.random.key(seed)
    sub_keys = jax.random.split(rng_key, 9)
    positions = jnp.arange(SEQ, dtype=jnp.int32)
    draws = jax.random.randint(sub_keys[0], (BATCH, SEQ), 0, SEQ)
    starts = (draws < 2) | (positions[None, :] == 0)
    doc_ids = (jnp.cumsum(starts.astype(jnp.int32), axis=1) - 1).astype(jnp.int32)
    first_pos = lax.cummax(jnp.where(starts, positions[None, :], 0), axis=1)
    doc_pos = (positions[None, :] - first_pos).astype(jnp.int32)
    qk_std = (5.0 * (pre_scalar() / HEAD) ** 0.5) ** 0.5 * DIM ** -0.5
    hidden = jax.random.normal(sub_keys[1], (BATCH, SEQ, DIM), jnp.float32)
    grad_out = jax.random.normal(sub_keys[2], (BATCH, SEQ, DIM), jnp.float32)
    w_query = jax.random.normal(sub_keys[3], (DIM, HEADS, HEAD), jnp.float32) * qk_std
    w_key = jax.random.normal(sub_keys[4], (DIM, KV_HEADS, HEAD), jnp.float32) * qk_std
    w_value = jax.random.normal(sub_keys[5], (DIM, KV_HEADS, HEAD), jnp.float32) * DIM ** -0.5
    w_out = jax.random.normal(sub_keys[6], (HEADS, HEAD, DIM), jnp.float32) * (HEADS * HEAD) ** -0.5
    gain_pre = jax.random.normal(sub_keys[7], (DIM,), jnp.float32) * 0.3
    gain_post = jax.random.normal(sub_keys[8], (DIM,), jnp.float32) * 0.3
    return dict(hidden=hidden.astype(jnp.bfloat16), doc_ids=doc_ids, doc_pos=doc_pos,
                grad_out=grad_out.astype(jnp.bfloat16), w_query=w_query.astype(jnp.bfloat16),
                w_key=w_key.astype(jnp.bfloat16), w_value=w_value.astype(jnp.bfloat16),
                w_out=w_out.astype(jnp.bfloat16), gain_pre=gain_pre.astype(jnp.bfloat16),
                gain_post=gain_post.astype(jnp.bfloat16))


def to_low(values):
    return values.astype(jnp.bfloat16).astype(jnp.float32)


def rms_norm(values, gain_vec):
    inv_rms = lax.rsqrt(jnp.mean(values * values, axis=-1, keepdims=True) + NORM_EPS)
    return values * inv_rms * (1.0 + gain_vec)


def rope_tables(pos_row):
    half_dim = HEAD // 2
    inv_freq = ROPE_BASE ** (-2.0 * jnp.arange(half_dim, dtype=jnp.float32) / HEAD)
    angles = pos_row.astype(jnp.float32)[:, None] * inv_freq[None, :]
    return jnp.cos(angles)[:, None, :], jnp.sin(angles)[:, None, :]


def rotate(values, cos_t, sin_t):
    half_dim = HEAD // 2
    first_half = values[..., :half_dim]
    second_half = values[..., half_dim:]
    return jnp.concatenate([first_half * cos_t - second_half * sin_t,
                            second_half * cos_t + first_half * sin_t], axis=-1)


def attend(q_rot, k_rot, v_proj, id_row):
    q_scale = pre_scalar() ** -0.5
    q_blocks = q_rot.reshape(N_BLOCKS, QUERY_BLOCK, KV_HEADS, GROUPS, HEAD)
    id_blocks = id_row.reshape(N_BLOCKS, QUERY_BLOCK)
    row_blocks = jnp.arange(SEQ).reshape(N_BLOCKS, QUERY_BLOCK)
    key_index = jnp.arange(SEQ)

    def one_block(block_args):
        q_blk, id_blk, row_blk = block_args
        scores = jnp.einsum('qkgh,tkh->kgqt', q_blk, k_rot) * q_scale
        capped = SOFT_CAP * jnp.tanh(scores / SOFT_CAP)
        visible = (id_blk[:, None] == id_row[None, :]) & (key_index[None, :] <= row_blk[:, None])
        capped = jnp.where(visible, capped, -1e30)
        row_peak = lax.stop_gradient(jnp.max(capped, axis=-1, keepdims=True))
        weights = jnp.exp(capped - row_peak)
        attn_prob = weights / jnp.sum(weights, axis=-1, keepdims=True)
        mixed_out = jnp.einsum('kgqt,tkh->qkgh', to_low(attn_prob), v_proj)
        return to_low(mixed_out).reshape(QUERY_BLOCK, HEADS, HEAD)

    block_outs = lax.map(jax.checkpoint(one_block), (q_blocks, id_blocks, row_blocks))
    return block_outs.reshape(SEQ, HEADS, HEAD)


def reference(hidden, doc_ids, doc_pos, grad_out, w_query, w_key, w_value, w_out, gain_pre, gain_post):
    def layer(hidden_in, q_weight, k_weight, v_weight, o_weight, pre_gain, post_gain):
        def one_seq(seq_args):
            row_in, id_row, pos_row = seq_args
            row_f32 = row_in.astype(jnp.float32)
            normed = to_low(rms_norm(row_f32, pre_gain))
            cos_t, sin_t = rope_tables(pos_row)
            q_proj = to_low(jnp.einsum('td,dnh->tnh', normed, q_weight))
            k_proj = to_low(jnp.einsum('td,dnh->tnh', normed, k_weight))
            v_proj = to_low(jnp.einsum('td,dnh->tnh', normed, v_weight))
            q_rot = to_low(rotate(q_proj, cos_t, sin_t))
            k_rot = to_low(rotate(k_proj, cos_t, sin_t))
            attn_out = attend(q_rot, k_rot, v_proj, id_row)
            proj_out = to_low(jnp.einsum('tnh,nhd->td', attn_out, o_weight))
            post_out = to_low(rms_norm(proj_out, post_gain))
            return (row_f32 + post_out).astype(jnp.bfloat16)
        return lax.map(jax.checkpoint(one_seq), (hidden_in, doc_ids, doc_pos))

    out_hidden, back_fn = jax.vjp(layer, hidden, w_query.astype(jnp.float32), w_key.astype(jnp.float32),
                                  w_value.astype(jnp.float32), w_out.astype(jnp.float32),
                                  gain_pre.astype(jnp.float32), gain_post.astype(jnp.float32))
    grad_hidden, grad_w_query, grad_w_key, grad_w_value, grad_w_out, grad_gain_pre, grad_gain_post = back_fn(grad_out)
    return (out_hidden, grad_hidden, grad_w_query, grad_w_key, grad_w_value, grad_w_out, grad_gain_pre, grad_gain_post)
```

```python
import functools

import jax
import jax.numpy as jnp
from jax import lax
from jax.experimental import pallas as pl
from jax.experimental.pallas import tpu as pltpu
from jax.sharding import PartitionSpec as P

SOFT_CAP = 50.0
NORM_EPS = 1e-6
ROPE_BASE = 10000.0
MESH = pl.DeviceIdType.MESH
SIDE = 4
VMEM_MAX = 67_043_328

STREAMS = ((0, 0, 0, 512), (0, 1, 512, 384), (0, 2, 896, 384),
           (1, 0, 0, 256), (1, 1, 256, 384), (1, 2, 640, 384))


def place():
    f = lax.axis_index('fsdp')
    return (f // 16, lax.rem(f // 4, 4), lax.rem(f, 4)), lax.axis_index('cp')


def shifted(coords, dim, delta):
    out = list(coords)
    out[dim] = lax.rem(coords[dim] + delta + SIDE, SIDE)
    return tuple(out)


def device(coords, core):
    return (coords[0] * 16 + coords[1] * 4 + coords[2], core)


def greet(coords, core):
    barrier = pltpu.get_barrier_semaphore()
    for dim in range(3):
        for delta in (1, -1):
            pl.semaphore_signal(barrier, inc=1, device_id=device(shifted(coords, dim, delta), core), device_id_type=MESH)
    pl.semaphore_signal(barrier, inc=1, device_id=device(coords, 1 - core), device_id_type=MESH)
    pl.semaphore_wait(barrier, 7)


def order_of(colour):
    return tuple((colour + i) % 3 for i in range(3))


def region(ref, full, coords, rows, cols):
    idx = [pl.ds(0, SIDE) if d in full else coords[d] for d in range(3)]
    return ref.at[idx[0], idx[1], idx[2], pl.ds(*rows), pl.ds(*cols)]


def gather_kernel(in0, in1, out0, out1, send, recv, sib_send, sib_recv, own_sem):
    coords, core = place()
    greet(coords, core)
    ins, outs = (in0, in1), (out0, out1)
    owns = []
    for g in range(2):
        copy = pltpu.make_async_copy(ins[g], outs[g].at[coords[0], coords[1], coords[2]], own_sem.at[g])
        copy.start()
        owns.append(copy)
    whole, low, high = (0, 32), (0, 16), (16, 16)
    sent, given = [], []

    def cols_of(s, side):
        g, _, off, width = STREAMS[s]
        half = outs[g].shape[-1] // 2
        return (pl.multiple_of(side * half + off, 128), width)

    def send_to(s, p, kind, src, rows, at, to):
        g, colour, _, _ = STREAMS[s]
        full = order_of(colour)[:p]
        cols = cols_of(s, core)
        dst = region(outs[g], full, at, rows, cols)
        copy = pltpu.make_async_remote_copy(
            src if src is not None else dst, dst, send.at[s, p, kind], recv.at[s, p, kind],
            device_id=device(to, core), device_id_type=MESH)
        copy.start()
        sent.append(copy)

    def arrived(s, p, kind):
        g, colour, _, _ = STREAMS[s]
        order = order_of(colour)
        at = shifted(coords, order[p], (-1, 1, -2, 2)[kind])
        rows = (whole, whole, low, high)[kind]
        here = region(outs[g], order[:p], at, rows, cols_of(s, core))
        pltpu.make_async_remote_copy(here, here, send.at[s, p, kind], recv.at[s, p, kind],
                                     device_id=device(coords, 1 - core), device_id_type=MESH).wait_recv()
        copy = pltpu.make_async_remote_copy(here, here, sib_send.at[s, p, kind], sib_recv.at[s, p, kind],
                                            device_id=device(coords, 1 - core), device_id_type=MESH)
        copy.start()
        there = region(outs[g], order[:p], at, rows, cols_of(s, 1 - core))
        given.append((copy, pltpu.make_async_remote_copy(
            there, there, sib_send.at[s, p, kind], sib_recv.at[s, p, kind],
            device_id=device(coords, 1 - core), device_id_type=MESH)))
        return at

    for p in range(3):
        for s, (g, colour, _, _) in enumerate(STREAMS):
            dim = order_of(colour)[p]
            if p > 0:
                arrived(s, p - 1, 2)
                arrived(s, p - 1, 3)
                if s in (0, 3) and p == 1:
                    owns[g].wait()
            src = ins[g].at[:, pl.ds(*cols_of(s, core))] if p == 0 else None
            send_to(s, p, 0, src, whole, coords, shifted(coords, dim, 1))
            send_to(s, p, 1, src, whole, coords, shifted(coords, dim, -1))
        for s, (g, colour, _, _) in enumerate(STREAMS):
            dim = order_of(colour)[p]
            send_to(s, p, 2, None, low, arrived(s, p, 0), shifted(coords, dim, 1))
            send_to(s, p, 3, None, high, arrived(s, p, 1), shifted(coords, dim, -1))
    for s in range(len(STREAMS)):
        arrived(s, 2, 2)
        arrived(s, 2, 3)
    for copy in sent:
        copy.wait_send()
    for out_copy, in_copy in given:
        out_copy.wait_send()
        in_copy.wait_recv()


def gather_weights(w0, w1):
    ns = len(STREAMS)
    shapes = [jax.ShapeDtypeStruct((SIDE, SIDE, SIDE, 32, w.shape[1]), w.dtype) for w in (w0, w1)]
    dma = pltpu.SemaphoreType.DMA
    return pl.pallas_call(
        gather_kernel, name="gather_weights",
        out_shape=shapes,
        in_specs=[pl.BlockSpec(memory_space=pltpu.VMEM)] * 2,
        out_specs=[pl.BlockSpec(memory_space=pl.ANY)] * 2,
        scratch_shapes=[dma((ns, 3, 4))] * 4 + [dma((2,))],
        compiler_params=pltpu.CompilerParams(collective_id=1, has_side_effects=True),
    )(w0, w1)


def scatter_kernel(own0, own1, own_g, sib0, sib1, sib_g, out0, out1, out_g, *scratch):
    ns = len(STREAMS) + 1
    scratch = list(scratch)
    sib_bufs = scratch[:3]
    acc = [[scratch[3 + s * 3 + q] for q in range(3)] for s in range(ns)]
    base = 3 + ns * 3
    sbuf = [[scratch[base + s * 3 + q] for q in range(3)] for s in range(ns)]
    base += ns * 3
    rbuf = [[scratch[base + s * 3 + q] for q in range(3)] for s in range(ns)]
    base += ns * 3
    send, recv, sib_send, sib_recv, fin_send, fin_recv = scratch[base:]
    coords, core = place()
    sibling = device(coords, 1 - core)
    greet(coords, core)
    owns, sibs, outs = (own0, own1, own_g), (sib0, sib1, sib_g), (out0, out1, out_g)
    gifts = []
    for g in range(3):
        copy = pltpu.make_async_remote_copy(sibs[g], sib_bufs[g], sib_send.at[g], sib_recv.at[g],
                                            device_id=sibling, device_id_type=MESH)
        copy.start()
        gifts.append(copy)
    streams = [(2, 0, 0, 128)] + list(STREAMS)
    sent = []

    def lead(order, q, at, n):
        full = order[:2 - q]
        idx = list(at)
        digits = (n // SIDE, lax.rem(n, SIDE)) if len(full) == 2 else (n,)
        for d, digit in zip(sorted(full), digits):
            idx[d] = digit
        return tuple(idx)

    def value(s, q, at, n, r0, nr):
        g, colour, off, width = streams[s]
        order = order_of(colour)
        idx = lead(order, q, at, n)
        if q == 0:
            where = idx + (pl.ds(r0, nr), pl.ds(off, width))
            return owns[g][where] + sib_bufs[g][where].astype(jnp.float32)
        kept = sorted(order[:3 - q])
        m = 0
        for d in kept:
            m = m * SIDE + idx[d]
        return acc[s][q - 1][m, pl.ds(r0, nr), :]

    def step_one(s, q):
        g, colour, _, width = streams[s]
        order = order_of(colour)
        dim = order[2 - q]
        half = rows_of(g) // 2
        n_blocks = SIDE ** (2 - q)
        far, right, left = shifted(coords, dim, 2), shifted(coords, dim, 1), shifted(coords, dim, -1)
        dt = sbuf[s][q].dtype

        def body(n, carry):
            sbuf[s][q][0, n] = value(s, q, far, n, 0, half).astype(dt)
            sbuf[s][q][1, n] = value(s, q, right, n, half, half).astype(dt)
            sbuf[s][q][2, n] = value(s, q, far, n, half, half).astype(dt)
            sbuf[s][q][3, n] = value(s, q, left, n, 0, half).astype(dt)
            return carry
        lax.fori_loop(0, n_blocks, body, 0)
        go(s, q, 0, (0, 2), right)
        go(s, q, 1, (2, 2), left)

    def go(s, q, kind, part, to):
        copy = pltpu.make_async_remote_copy(
            sbuf[s][q].at[pl.ds(*part)], rbuf[s][q].at[pl.ds(*part)], send.at[s, q, kind], recv.at[s, q, kind],
            device_id=device(to, core), device_id_type=MESH)
        copy.start()
        sent.append(copy)

    def got(s, q, kind, part):
        here = rbuf[s][q].at[pl.ds(*part)]
        pltpu.make_async_remote_copy(here, here, send.at[s, q, kind], recv.at[s, q, kind],
                                     device_id=sibling, device_id_type=MESH).wait_recv()

    def step_two(s, q):
        g, colour, _, width = streams[s]
        dim = order_of(colour)[2 - q]
        half = rows_of(g) // 2
        n_blocks = SIDE ** (2 - q)
        right, left = shifted(coords, dim, 1), shifted(coords, dim, -1)
        dt = sbuf[s][q].dtype
        got(s, q, 0, (0, 2))

        def to_right(n, carry):
            sbuf[s][q][4, n] = (value(s, q, right, n, 0, half) + rbuf[s][q][0, n].astype(jnp.float32)).astype(dt)
            return carry
        lax.fori_loop(0, n_blocks, to_right, 0)
        go(s, q, 2, (4, 1), right)
        got(s, q, 1, (2, 2))

        def to_left(n, carry):
            sbuf[s][q][5, n] = (value(s, q, left, n, half, half) + rbuf[s][q][2, n].astype(jnp.float32)).astype(dt)
            return carry
        lax.fori_loop(0, n_blocks, to_left, 0)
        go(s, q, 3, (5, 1), left)

    def step_three(s, q):
        g, colour, _, width = streams[s]
        half = rows_of(g) // 2
        n_blocks = SIDE ** (2 - q)
        got(s, q, 2, (4, 1))
        got(s, q, 3, (5, 1))

        def body(n, carry):
            def low(i):
                return rbuf[s][q][i, n].astype(jnp.float32)
            acc[s][q][n, pl.ds(0, half), :] = value(s, q, coords, n, 0, half) + low(3) + low(4)
            acc[s][q][n, pl.ds(half, half), :] = value(s, q, coords, n, half, half) + low(1) + low(5)
            return carry
        lax.fori_loop(0, n_blocks, body, 0)

    def rows_of(g):
        return owns[g].shape[3]

    for g in (2, 0, 1):
        gifts[g].wait_recv()
        for s in range(ns):
            if streams[s][0] == g:
                step_one(s, 0)
    for q in range(3):
        for s in range(ns):
            step_two(s, q)
        for s in range(ns):
            step_three(s, q)
            if q < 2:
                step_one(s, q + 1)
    fins = []
    for s in range(ns):
        g, _, off, width = streams[s]
        here = outs[g].at[core, :, pl.ds(off, width)]
        outs[g][core, :, pl.ds(off, width)] = acc[s][2][0]
        copy = pltpu.make_async_remote_copy(acc[s][2].at[0], here, fin_send.at[s], fin_recv.at[s],
                                            device_id=sibling, device_id_type=MESH)
        copy.start()
        fins.append((copy, s))
    for copy, s in fins:
        g, _, off, width = streams[s]
        there = outs[g].at[1 - core, :, pl.ds(off, width)]
        copy.wait_send()
        pltpu.make_async_remote_copy(there, there, fin_send.at[s], fin_recv.at[s],
                                     device_id=sibling, device_id_type=MESH).wait_recv()
    for copy in sent + gifts:
        copy.wait_send()


def scatter_grads(own0, own1, own_g, sib0, sib1, sib_g):
    owns, sibs = (own0, own1, own_g), (sib0, sib1, sib_g)
    streams = [(2, 0, 0, 128)] + list(STREAMS)
    ns = len(streams)
    dma = pltpu.SemaphoreType.DMA
    scratch = [pltpu.VMEM(a.shape, a.dtype) for a in sibs]
    for kind in range(3):
        for g, _, _, width in streams:
            rows = owns[g].shape[3]
            dt = sibs[g].dtype
            for q in range(3):
                n = SIDE ** (2 - q)
                scratch.append(pltpu.VMEM((n, rows, width), jnp.float32) if kind == 0
                               else pltpu.VMEM((6, n, rows // 2, width), dt))
    scratch += [dma((ns, 3, 4))] * 2 + [dma((3,))] * 2 + [dma((ns,))] * 2
    return pl.pallas_call(
        scatter_kernel, name="scatter_grads",
        out_shape=[jax.ShapeDtypeStruct((2,) + a.shape[3:], jnp.float32) for a in owns],
        in_specs=[pl.BlockSpec(memory_space=pltpu.VMEM)] * 3 + [pl.BlockSpec(memory_space=pl.ANY)] * 2
        + [pl.BlockSpec(memory_space=pltpu.VMEM)],
        out_specs=[pl.BlockSpec(memory_space=pltpu.VMEM)] * 3,
        scratch_shapes=scratch,
        compiler_params=pltpu.CompilerParams(collective_id=2, has_side_effects=True, vmem_limit_bytes=VMEM_MAX),
    )(own0, own1, own_g, sib0, sib1, sib_g)


def rope_tables(pos_ids, head_dim):
    half_dim = head_dim // 2
    inv_freq = ROPE_BASE ** (-2.0 * jnp.arange(half_dim, dtype=jnp.float32) / head_dim)
    angles = pos_ids.astype(jnp.float32)[..., None] * inv_freq
    return jnp.cos(angles)[..., None, :], jnp.sin(angles)[..., None, :]


def rotate(values, cos_t, sin_t):
    half_dim = values.shape[-1] // 2
    first_half = values[..., :half_dim].astype(jnp.float32)
    second_half = values[..., half_dim:].astype(jnp.float32)
    rotated = jnp.concatenate([first_half * cos_t - second_half * sin_t,
                               second_half * cos_t + first_half * sin_t], axis=-1)
    return rotated.astype(jnp.bfloat16)


def norm_forward(values, gain_vec):
    values_f = values.astype(jnp.float32)
    inv_rms = lax.rsqrt(jnp.mean(values_f * values_f, axis=-1, keepdims=True) + NORM_EPS)
    normed = values_f * inv_rms * (1.0 + gain_vec.astype(jnp.float32))
    return normed.astype(jnp.bfloat16), inv_rms


def norm_backward(values, inv_rms, gain_vec, grads):
    values_f = values.astype(jnp.float32)
    grads_f = grads.astype(jnp.float32)
    scaled = grads_f * (1.0 + gain_vec.astype(jnp.float32))
    d_values = inv_rms * scaled - values_f * inv_rms ** 3 * jnp.mean(scaled * values_f, axis=-1, keepdims=True)
    d_gain = jnp.sum(grads_f * values_f * inv_rms, axis=0)
    return d_values, d_gain


def dot(a, b, dims):
    return lax.dot_general(a, b, ((dims[:1], dims[1:]), ((), ())), preferred_element_type=jnp.float32)


def solution(mesh):
    tok_spec = P('fsdp', 'cp', None)
    ids_spec = P('fsdp', 'cp')
    in_spec = P('fsdp', None, None)
    out_spec = P(None, None, 'fsdp')
    gain_spec = P('fsdp')
    bf, f32 = jnp.bfloat16, jnp.float32

    def layer_local(hidden, doc_ids, doc_pos, grad_out, w_query, w_key, w_value, w_out, gain_pre, gain_post):
        _, n_tok, model_dim = hidden.shape
        hidden, grad_out = hidden[0], grad_out[0]
        n_heads, head_dim = w_query.shape[1], w_query.shape[2]
        rows = w_query.shape[0]
        q_cols = n_heads * head_dim
        core = lax.axis_index('cp')
        w0 = jnp.concatenate([w_query.reshape(rows, q_cols), w_key.reshape(rows, head_dim),
                              w_value.reshape(rows, head_dim)], axis=1)
        w1 = w_out.reshape(q_cols, rows).T
        gains = lax.all_gather(jnp.stack([gain_pre, gain_post]), 'fsdp', axis=1, tiled=True)
        pre_full, post_full = gains[0], gains[1]
        wqkv, wo_t = gather_weights(w0, w1)
        wqkv = wqkv.reshape(model_dim, q_cols + 2 * head_dim)
        wo_t = wo_t.reshape(model_dim, q_cols)
        q_scale = (head_dim if head_dim >= 256 else model_dim // n_heads) ** -0.5

        normed, inv_pre = norm_forward(hidden, pre_full)
        qkv = dot(normed, wqkv, (1, 0)).astype(bf)
        q_proj = qkv[:, :q_cols].reshape(n_tok, n_heads, head_dim)
        k_proj = qkv[:, q_cols:q_cols + head_dim].reshape(n_tok, 1, head_dim)
        v_proj = qkv[:, q_cols + head_dim:]
        cos_t, sin_t = rope_tables(doc_pos[0], head_dim)
        q_rot = rotate(q_proj, cos_t, sin_t)
        k_rot = rotate(k_proj, cos_t, sin_t)[:, 0]

        k_all = lax.all_gather(k_rot, 'cp', axis=0, tiled=True)
        v_all = lax.all_gather(v_proj, 'cp', axis=0, tiled=True)
        ids_all = lax.all_gather(doc_ids, 'cp', axis=1, tiled=True)
        q_index = core * n_tok + jnp.arange(n_tok)
        k_index = jnp.arange(k_all.shape[0])
        visible = (doc_ids[0][:, None] == ids_all[0][None, :]) & (k_index[None, :] <= q_index[:, None])
        scores = jnp.einsum('qhd,td->hqt', q_rot, k_all, preferred_element_type=f32) * q_scale
        tanh_s = jnp.tanh(scores / SOFT_CAP)
        capped = jnp.where(visible, SOFT_CAP * tanh_s, -1e30)
        row_peak = jnp.max(capped, axis=-1, keepdims=True)
        weights = jnp.exp(capped - row_peak)
        attn_prob = weights / jnp.sum(weights, axis=-1, keepdims=True)
        prob_low = attn_prob.astype(bf)
        attn_out = jnp.einsum('hqt,td->qhd', prob_low, v_all, preferred_element_type=f32).astype(bf)
        attn_flat = attn_out.reshape(n_tok, q_cols)
        proj_out = dot(attn_flat, wo_t, (1, 1)).astype(bf)
        post_out, inv_post = norm_forward(proj_out, post_full)
        out_hidden = (hidden.astype(f32) + post_out.astype(f32)).astype(bf)

        d_proj, d_gain_post = norm_backward(proj_out, inv_post, post_full, grad_out)
        d_proj = d_proj.astype(bf)
        d_attn = dot(d_proj, wo_t, (1, 0)).astype(bf).reshape(n_tok, n_heads, head_dim)

        def halves(grads, acts):
            width = acts.shape[1] // 2
            own = dot(grads, lax.dynamic_slice_in_dim(acts, core * width, width, 1), (0, 0))
            other = dot(grads, lax.dynamic_slice_in_dim(acts, (1 - core) * width, width, 1), (0, 0)).astype(bf)
            shape = (SIDE, SIDE, SIDE, rows, width)
            return own.reshape(shape), other.reshape(shape)

        own1, sib1 = halves(d_proj, attn_flat)

        d_prob = jnp.einsum('qhd,td->hqt', d_attn, v_all, preferred_element_type=f32)
        row_dot = jnp.sum(attn_prob * d_prob, axis=-1, keepdims=True)
        d_score = (attn_prob * (d_prob - row_dot) * (1.0 - tanh_s * tanh_s) * q_scale).astype(bf)
        d_q_rot = jnp.einsum('hqt,td->qhd', d_score, k_all, preferred_element_type=f32).astype(bf)
        d_k_part = jnp.einsum('hqt,qhd->td', d_score, q_rot, preferred_element_type=f32).astype(bf)
        d_v_part = jnp.einsum('hqt,qhd->td', prob_low, d_attn, preferred_element_type=f32).astype(bf)
        d_k_rot = lax.psum_scatter(d_k_part, 'cp', scatter_dimension=0, tiled=True)
        d_v_proj = lax.psum_scatter(d_v_part, 'cp', scatter_dimension=0, tiled=True)
        d_q_proj = rotate(d_q_rot, cos_t, -sin_t)
        d_k_proj = rotate(d_k_rot[:, None], cos_t, -sin_t)[:, 0]
        d_qkv = jnp.concatenate([d_q_proj.reshape(n_tok, q_cols), d_k_proj, d_v_proj], axis=1)

        d_normed = dot(d_qkv, wqkv, (1, 1)).astype(bf)
        own0, sib0 = halves(normed, d_qkv)
        d_hidden, d_gain_pre = norm_backward(hidden, inv_pre, pre_full, d_normed)
        grad_hidden = (grad_out.astype(f32) + d_hidden).astype(bf)
        d_gains = jnp.stack([d_gain_pre, d_gain_post]).reshape(2, SIDE, SIDE, SIDE, 1, rows)
        d_gains = jnp.pad(d_gains, ((0, 0), (0, 0), (0, 0), (0, 0), (0, 15), (0, 128 - rows)))
        own_g = lax.dynamic_index_in_dim(d_gains, core, 0, keepdims=False)
        sib_g = lax.dynamic_index_in_dim(d_gains, 1 - core, 0, keepdims=False)
        g0, g1, gg = scatter_grads(own0, own1, own_g, sib0, sib1, sib_g)
        g0 = jnp.concatenate([g0[0], g0[1]], axis=1)
        g1 = jnp.concatenate([g1[0], g1[1]], axis=1)
        return (out_hidden[None], grad_hidden[None], g0[:, :q_cols].reshape(rows, n_heads, head_dim),
                g0[:, q_cols:q_cols + head_dim].reshape(rows, 1, head_dim),
                g0[:, q_cols + head_dim:].reshape(rows, 1, head_dim),
                g1.T.reshape(n_heads, head_dim, rows), gg[0, 0, :rows], gg[1, 0, :rows])

    return jax.shard_map(layer_local, mesh=mesh,
                         in_specs=(tok_spec, ids_spec, ids_spec, tok_spec, in_spec, in_spec, in_spec, out_spec, gain_spec, gain_spec),
                         out_specs=(tok_spec, tok_spec, in_spec, in_spec, in_spec, out_spec, gain_spec, gain_spec),
                         check_vma=False)
```

```python
import functools

import jax
import jax.numpy as jnp
from jax import lax
from jax.experimental import pallas as pl
from jax.experimental.pallas import tpu as pltpu
from jax.sharding import PartitionSpec as P

SOFT_CAP = 50.0
NORM_EPS = 1e-6
ROPE_BASE = 10000.0
MESH = pl.DeviceIdType.MESH
SIDE = 4
VMEM_MAX = 67_043_328

STREAMS = ((2, 0, 0, 128),
           (0, 0, 0, 512), (0, 1, 512, 384), (0, 2, 896, 384),
           (1, 0, 0, 256), (1, 1, 256, 384), (1, 2, 640, 384))


def place():
    f = lax.axis_index('fsdp')
    return (f // 16, lax.rem(f // 4, 4), lax.rem(f, 4)), lax.axis_index('cp')


def shifted(coords, dim, delta):
    out = list(coords)
    out[dim] = lax.rem(coords[dim] + delta + SIDE, SIDE)
    return tuple(out)


def device(coords, core):
    return (coords[0] * 16 + coords[1] * 4 + coords[2], core)


def greet(coords, core):
    barrier = pltpu.get_barrier_semaphore()
    for dim in range(3):
        for delta in (1, -1):
            pl.semaphore_signal(barrier, inc=1, device_id=device(shifted(coords, dim, delta), core), device_id_type=MESH)
    pl.semaphore_signal(barrier, inc=1, device_id=device(coords, 1 - core), device_id_type=MESH)
    pl.semaphore_wait(barrier, 7)


def order_of(colour):
    return tuple((colour + i) % 3 for i in range(3))


def region(ref, full, coords, rows, cols):
    idx = [pl.ds(0, SIDE) if d in full else coords[d] for d in range(3)]
    return ref.at[idx[0], idx[1], idx[2], pl.ds(*rows), pl.ds(*cols)]


def gather_kernel(in0, in1, in2, out0, out1, out2, send, recv, sib_send, sib_recv, own_sem):
    coords, core = place()
    greet(coords, core)
    ins, outs = (in0, in1, in2), (out0, out1, out2)
    owns = []
    for g in range(3):
        copy = pltpu.make_async_copy(ins[g], outs[g].at[coords[0], coords[1], coords[2]], own_sem.at[g])
        copy.start()
        owns.append(copy)
    sent, given = [], []

    def rows_for(s, kind):
        rows = ins[STREAMS[s][0]].shape[0]
        return ((0, rows), (0, rows), (0, rows // 2), (rows // 2, rows // 2))[kind]

    def cols_of(s, side):
        g, _, off, width = STREAMS[s]
        half = outs[g].shape[-1] // 2
        return (pl.multiple_of(side * half + off, 128), width)

    def send_to(s, p, kind, src, at, to):
        g, colour, _, _ = STREAMS[s]
        rows = rows_for(s, kind)
        full = order_of(colour)[:p]
        cols = cols_of(s, core)
        dst = region(outs[g], full, at, rows, cols)
        copy = pltpu.make_async_remote_copy(
            src if src is not None else dst, dst, send.at[s, p, kind], recv.at[s, p, kind],
            device_id=device(to, core), device_id_type=MESH)
        copy.start()
        sent.append(copy)

    def arrived(s, p, kind):
        g, colour, _, _ = STREAMS[s]
        order = order_of(colour)
        at = shifted(coords, order[p], (-1, 1, -2, 2)[kind])
        rows = rows_for(s, kind)
        here = region(outs[g], order[:p], at, rows, cols_of(s, core))
        pltpu.make_async_remote_copy(here, here, send.at[s, p, kind], recv.at[s, p, kind],
                                     device_id=device(coords, 1 - core), device_id_type=MESH).wait_recv()
        copy = pltpu.make_async_remote_copy(here, here, sib_send.at[s, p, kind], sib_recv.at[s, p, kind],
                                            device_id=device(coords, 1 - core), device_id_type=MESH)
        copy.start()
        there = region(outs[g], order[:p], at, rows, cols_of(s, 1 - core))
        given.append((copy, pltpu.make_async_remote_copy(
            there, there, sib_send.at[s, p, kind], sib_recv.at[s, p, kind],
            device_id=device(coords, 1 - core), device_id_type=MESH)))
        return at

    for p in range(3):
        for s, (g, colour, _, _) in enumerate(STREAMS):
            dim = order_of(colour)[p]
            if p > 0:
                arrived(s, p - 1, 2)
                arrived(s, p - 1, 3)
                if p == 1 and (s == 0 or STREAMS[s - 1][0] != g):
                    owns[g].wait()
            src = ins[g].at[:, pl.ds(*cols_of(s, core))] if p == 0 else None
            send_to(s, p, 0, src, coords, shifted(coords, dim, 1))
            send_to(s, p, 1, src, coords, shifted(coords, dim, -1))
        for s, (g, colour, _, _) in enumerate(STREAMS):
            dim = order_of(colour)[p]
            send_to(s, p, 2, None, arrived(s, p, 0), shifted(coords, dim, 1))
            send_to(s, p, 3, None, arrived(s, p, 1), shifted(coords, dim, -1))
    for s in range(len(STREAMS)):
        arrived(s, 2, 2)
        arrived(s, 2, 3)
    for copy in sent:
        copy.wait_send()
    for out_copy, in_copy in given:
        out_copy.wait_send()
        in_copy.wait_recv()


def gather_weights(*ws):
    ns = len(STREAMS)
    shapes = [jax.ShapeDtypeStruct((SIDE, SIDE, SIDE) + w.shape, w.dtype) for w in ws]
    dma = pltpu.SemaphoreType.DMA
    return pl.pallas_call(
        gather_kernel, name="gather_weights",
        out_shape=shapes,
        in_specs=[pl.BlockSpec(memory_space=pltpu.VMEM)] * 3,
        out_specs=[pl.BlockSpec(memory_space=pl.ANY)] * 3,
        scratch_shapes=[dma((ns, 3, 4))] * 4 + [dma((3,))],
        compiler_params=pltpu.CompilerParams(collective_id=1, has_side_effects=True),
    )(*ws)


def scatter_kernel(own0, own1, own_g, sib0, sib1, sib_g, out0, out1, out_g, *scratch):
    ns = len(STREAMS)
    scratch = list(scratch)
    sib_bufs = scratch[:3]
    acc = [[scratch[3 + s * 3 + q] for q in range(3)] for s in range(ns)]
    base = 3 + ns * 3
    sbuf = [[scratch[base + s * 3 + q] for q in range(3)] for s in range(ns)]
    base += ns * 3
    rbuf = [[scratch[base + s * 3 + q] for q in range(3)] for s in range(ns)]
    base += ns * 3
    send, recv, sib_send, sib_recv, fin_send, fin_recv = scratch[base:]
    coords, core = place()
    sibling = device(coords, 1 - core)
    greet(coords, core)
    owns, sibs, outs = (own0, own1, own_g), (sib0, sib1, sib_g), (out0, out1, out_g)
    gifts = []
    for g in range(3):
        copy = pltpu.make_async_remote_copy(sibs[g], sib_bufs[g], sib_send.at[g], sib_recv.at[g],
                                            device_id=sibling, device_id_type=MESH)
        copy.start()
        gifts.append(copy)
    streams = STREAMS
    sent = []

    def lead(order, q, at, n):
        full = order[:2 - q]
        idx = list(at)
        digits = (n // SIDE, lax.rem(n, SIDE)) if len(full) == 2 else (n,)
        for d, digit in zip(sorted(full), digits):
            idx[d] = digit
        return tuple(idx)

    def value(s, q, at, n, r0, nr):
        g, colour, off, width = streams[s]
        order = order_of(colour)
        idx = lead(order, q, at, n)
        if q == 0:
            where = idx + (pl.ds(r0, nr), pl.ds(off, width))
            return owns[g][where] + sib_bufs[g][where].astype(jnp.float32)
        kept = sorted(order[:3 - q])
        m = 0
        for d in kept:
            m = m * SIDE + idx[d]
        return acc[s][q - 1][m, pl.ds(r0, nr), :]

    def step_one(s, q):
        g, colour, _, width = streams[s]
        order = order_of(colour)
        dim = order[2 - q]
        half = rows_of(g) // 2
        n_blocks = SIDE ** (2 - q)
        far, right, left = shifted(coords, dim, 2), shifted(coords, dim, 1), shifted(coords, dim, -1)
        dt = sbuf[s][q].dtype

        def body(n, carry):
            sbuf[s][q][0, n] = value(s, q, far, n, 0, half).astype(dt)
            sbuf[s][q][1, n] = value(s, q, right, n, half, half).astype(dt)
            sbuf[s][q][2, n] = value(s, q, far, n, half, half).astype(dt)
            sbuf[s][q][3, n] = value(s, q, left, n, 0, half).astype(dt)
            return carry
        lax.fori_loop(0, n_blocks, body, 0)
        go(s, q, 0, (0, 2), right)
        go(s, q, 1, (2, 2), left)

    def go(s, q, kind, part, to):
        copy = pltpu.make_async_remote_copy(
            sbuf[s][q].at[pl.ds(*part)], rbuf[s][q].at[pl.ds(*part)], send.at[s, q, kind], recv.at[s, q, kind],
            device_id=device(to, core), device_id_type=MESH)
        copy.start()
        sent.append(copy)

    def got(s, q, kind, part):
        here = rbuf[s][q].at[pl.ds(*part)]
        pltpu.make_async_remote_copy(here, here, send.at[s, q, kind], recv.at[s, q, kind],
                                     device_id=sibling, device_id_type=MESH).wait_recv()

    def step_two(s, q):
        g, colour, _, width = streams[s]
        dim = order_of(colour)[2 - q]
        half = rows_of(g) // 2
        n_blocks = SIDE ** (2 - q)
        right, left = shifted(coords, dim, 1), shifted(coords, dim, -1)
        dt = sbuf[s][q].dtype
        got(s, q, 0, (0, 2))

        def to_right(n, carry):
            sbuf[s][q][4, n] = (value(s, q, right, n, 0, half) + rbuf[s][q][0, n].astype(jnp.float32)).astype(dt)
            return carry
        lax.fori_loop(0, n_blocks, to_right, 0)
        go(s, q, 2, (4, 1), right)
        got(s, q, 1, (2, 2))

        def to_left(n, carry):
            sbuf[s][q][5, n] = (value(s, q, left, n, half, half) + rbuf[s][q][2, n].astype(jnp.float32)).astype(dt)
            return carry
        lax.fori_loop(0, n_blocks, to_left, 0)
        go(s, q, 3, (5, 1), left)

    def step_three(s, q):
        g, colour, _, width = streams[s]
        half = rows_of(g) // 2
        n_blocks = SIDE ** (2 - q)
        got(s, q, 2, (4, 1))
        got(s, q, 3, (5, 1))

        def body(n, carry):
            def low(i):
                return rbuf[s][q][i, n].astype(jnp.float32)
            acc[s][q][n, pl.ds(0, half), :] = value(s, q, coords, n, 0, half) + low(3) + low(4)
            acc[s][q][n, pl.ds(half, half), :] = value(s, q, coords, n, half, half) + low(1) + low(5)
            return carry
        lax.fori_loop(0, n_blocks, body, 0)

    def rows_of(g):
        return owns[g].shape[3]

    for g in (2, 0, 1):
        gifts[g].wait_recv()
        for s in range(ns):
            if streams[s][0] == g:
                step_one(s, 0)
    for q in range(3):
        for s in range(ns):
            step_two(s, q)
        for s in range(ns):
            step_three(s, q)
            if q < 2:
                step_one(s, q + 1)
    fins = []
    for s in range(ns):
        g, _, off, width = streams[s]
        here = outs[g].at[core, :, pl.ds(off, width)]
        outs[g][core, :, pl.ds(off, width)] = acc[s][2][0]
        copy = pltpu.make_async_remote_copy(acc[s][2].at[0], here, fin_send.at[s], fin_recv.at[s],
                                            device_id=sibling, device_id_type=MESH)
        copy.start()
        fins.append((copy, s))
    for copy, s in fins:
        g, _, off, width = streams[s]
        there = outs[g].at[1 - core, :, pl.ds(off, width)]
        copy.wait_send()
        pltpu.make_async_remote_copy(there, there, fin_send.at[s], fin_recv.at[s],
                                     device_id=sibling, device_id_type=MESH).wait_recv()
    for copy in sent + gifts:
        copy.wait_send()


def scatter_grads(own0, own1, own_g, sib0, sib1, sib_g):
    owns, sibs = (own0, own1, own_g), (sib0, sib1, sib_g)
    streams = STREAMS
    ns = len(streams)
    dma = pltpu.SemaphoreType.DMA
    scratch = [pltpu.VMEM(a.shape, a.dtype) for a in sibs]
    for kind in range(3):
        for g, _, _, width in streams:
            rows = owns[g].shape[3]
            dt = sibs[g].dtype
            for q in range(3):
                n = SIDE ** (2 - q)
                scratch.append(pltpu.VMEM((n, rows, width), jnp.float32) if kind == 0
                               else pltpu.VMEM((6, n, rows // 2, width), dt))
    scratch += [dma((ns, 3, 4))] * 2 + [dma((3,))] * 2 + [dma((ns,))] * 2
    return pl.pallas_call(
        scatter_kernel, name="scatter_grads",
        out_shape=[jax.ShapeDtypeStruct((2,) + a.shape[3:], jnp.float32) for a in owns],
        in_specs=[pl.BlockSpec(memory_space=pltpu.VMEM)] * 3 + [pl.BlockSpec(memory_space=pl.ANY)] * 2
        + [pl.BlockSpec(memory_space=pltpu.VMEM)],
        out_specs=[pl.BlockSpec(memory_space=pltpu.VMEM)] * 3,
        scratch_shapes=scratch,
        compiler_params=pltpu.CompilerParams(collective_id=2, has_side_effects=True, vmem_limit_bytes=VMEM_MAX),
    )(own0, own1, own_g, sib0, sib1, sib_g)


LOG2E = 1.4426950408889634
TILE = 256


def nt(a, b):
    return lax.dot_general(a, b, (((1,), (1,)), ((), ())), preferred_element_type=jnp.float32)


def nn(a, b):
    return lax.dot_general(a, b, (((1,), (0,)), ((), ())), preferred_element_type=jnp.float32)


def fill_mask(mask, ids_k, ids_q):
    n_keys, n_q = mask.shape
    core = lax.axis_index('cp')
    for c in range(n_keys // TILE):
        base = jnp.where(c < n_q // TILE, (1 - core) * n_q, core * n_q - n_q) + c * TILE
        for i in range(n_q // TILE):
            k_at = base + lax.broadcasted_iota(jnp.int32, (TILE, TILE), 0)
            q_at = core * n_q + i * TILE + lax.broadcasted_iota(jnp.int32, (TILE, TILE), 1)
            same = ids_k[pl.ds(c * TILE, TILE), :] == ids_q[:, pl.ds(i * TILE, TILE)]
            mask[pl.ds(c * TILE, TILE), pl.ds(i * TILE, TILE)] = jnp.where(same & (k_at <= q_at), 1.0, 0.0)


def keys_for(i, n_q):
    return n_q + (i + 1) * TILE


def attend_kernel(ratio, q_ref, k_ref, v_ref, ids_k, ids_q, o_ref, inv_ref, mask, v_t, w_scr, p_scr):
    n_q = q_ref.shape[0]
    fill_mask(mask, ids_k, ids_q)
    v_t[...] = v_ref[...].T

    def head(h, carry):
        cols = pl.ds(pl.multiple_of(h * TILE, TILE), TILE)
        for i in range(n_q // TILE):
            qi = q_ref[pl.ds(i * TILE, TILE), cols]
            n_keys = keys_for(i, n_q)
            total = jnp.zeros((8, TILE), jnp.float32)
            for c in range(n_keys // TILE):
                t = jnp.tanh(nt(k_ref[pl.ds(c * TILE, TILE), :], qi) * ratio)
                w = jnp.exp2(t * (SOFT_CAP * LOG2E)) * mask[pl.ds(c * TILE, TILE), pl.ds(i * TILE, TILE)]
                w_scr[i, pl.ds(c * TILE, TILE), :] = w
                total = total + jnp.sum(w.reshape(TILE // 8, 8, TILE), axis=0)
            inv = 1.0 / jnp.sum(total, axis=0, keepdims=True)
            inv_ref[h, :, pl.ds(i * TILE, TILE)] = inv
            p_scr[i, pl.ds(0, n_keys), :] = (w_scr[i, pl.ds(0, n_keys), :] * inv).astype(jnp.bfloat16)
            o_t = nn(v_t[:, pl.ds(0, n_keys)], p_scr[i, pl.ds(0, n_keys), :])
            o_ref[pl.ds(i * TILE, TILE), cols] = o_t.T.astype(jnp.bfloat16)
        return carry
    lax.fori_loop(0, q_ref.shape[1] // TILE, head, 0)


def attend(q, k, v, ids_k, ids_q, n_heads, ratio):
    n_q, n_k = q.shape[0], k.shape[0]
    vmem = pl.BlockSpec(memory_space=pltpu.VMEM)
    return pl.pallas_call(
        functools.partial(attend_kernel, ratio), name="attend",
        out_shape=[jax.ShapeDtypeStruct(q.shape, jnp.bfloat16), jax.ShapeDtypeStruct((n_heads, 1, n_q), jnp.float32)],
        in_specs=[vmem] * 5, out_specs=[vmem] * 2,
        scratch_shapes=[pltpu.VMEM((n_k, n_q), jnp.float32), pltpu.VMEM((TILE, n_k), jnp.bfloat16),
                        pltpu.VMEM((n_q // TILE, n_k, TILE), jnp.float32),
                        pltpu.VMEM((n_q // TILE, n_k, TILE), jnp.bfloat16)],
        cost_estimate=pl.CostEstimate(flops=8_000_000_000, bytes_accessed=6_000_000, transcendentals=8_000_000),
    )(q, k, v, ids_k, ids_q)


def attend_back_kernel(ratio, q_ref, do_ref, k_ref, v_ref, ids_k, ids_q, inv_ref, dq_ref, dk_ref, dv_ref,
                       mask, k_t, g_scr, dp_scr, p_scr, ds_scr, dk_acc, dv_acc):
    n_q = q_ref.shape[0]
    fill_mask(mask, ids_k, ids_q)
    k_t[...] = k_ref[...].T
    dk_acc[...] = jnp.zeros_like(dk_acc)
    dv_acc[...] = jnp.zeros_like(dv_acc)

    def head(h, carry):
        cols = pl.ds(pl.multiple_of(h * TILE, TILE), TILE)
        for i in range(n_q // TILE):
            rows = pl.ds(i * TILE, TILE)
            qi, doi = q_ref[rows, cols], do_ref[rows, cols]
            inv = inv_ref[h, :, rows]
            n_keys = keys_for(i, n_q)
            total = jnp.zeros((8, TILE), jnp.float32)
            for c in range(n_keys // TILE):
                at = pl.ds(c * TILE, TILE)
                t = jnp.tanh(nt(k_ref[at, :], qi) * ratio)
                p = jnp.exp2(t * (SOFT_CAP * LOG2E)) * (mask[at, rows] * inv)
                dp = nt(v_ref[at, :], doi)
                p_scr[i, at, :] = p.astype(jnp.bfloat16)
                g_scr[i, at, :] = p * ((1.0 - t * t) * (ratio * SOFT_CAP))
                dp_scr[i, at, :] = dp
                total = total + jnp.sum((p * dp).reshape(TILE // 8, 8, TILE), axis=0)
            row_dot = jnp.sum(total, axis=0, keepdims=True)
            seen = pl.ds(0, n_keys)
            ds_scr[i, seen, :] = ((dp_scr[i, seen, :] - row_dot) * g_scr[i, seen, :]).astype(jnp.bfloat16)
            dq_t = nn(k_t[:, seen], ds_scr[i, seen, :])
            dq_ref[rows, cols] = dq_t.T.astype(jnp.bfloat16)
            dk_acc[seen, :] += nn(ds_scr[i, seen, :], qi)
            dv_acc[seen, :] += nn(p_scr[i, seen, :], doi)
        return carry
    lax.fori_loop(0, q_ref.shape[1] // TILE, head, 0)
    dk_ref[...] = dk_acc[...].astype(jnp.bfloat16)
    dv_ref[...] = dv_acc[...].astype(jnp.bfloat16)


def attend_back(q, do, k, v, ids_k, ids_q, inv_sum, n_heads, ratio):
    n_q, n_k = q.shape[0], k.shape[0]
    vmem = pl.BlockSpec(memory_space=pltpu.VMEM)
    tiles = n_q // TILE
    bf, f32 = jnp.bfloat16, jnp.float32
    return pl.pallas_call(
        functools.partial(attend_back_kernel, ratio), name="attend_back",
        out_shape=[jax.ShapeDtypeStruct(q.shape, bf)] + [jax.ShapeDtypeStruct(k.shape, bf)] * 2,
        in_specs=[vmem] * 7, out_specs=[vmem] * 3,
        scratch_shapes=[pltpu.VMEM((n_k, n_q), f32), pltpu.VMEM((TILE, n_k), bf),
                        pltpu.VMEM((tiles, n_k, TILE), f32), pltpu.VMEM((tiles, n_k, TILE), f32),
                        pltpu.VMEM((tiles, n_k, TILE), bf), pltpu.VMEM((tiles, n_k, TILE), bf),
                        pltpu.VMEM((n_k, TILE), f32), pltpu.VMEM((n_k, TILE), f32)],
        cost_estimate=pl.CostEstimate(flops=16_000_000_000, bytes_accessed=8_000_000, transcendentals=8_000_000),
    )(q, do, k, v, ids_k, ids_q, inv_sum)


def rope_tables(pos_ids, head_dim):
    half_dim = head_dim // 2
    inv_freq = ROPE_BASE ** (-2.0 * jnp.arange(half_dim, dtype=jnp.float32) / head_dim)
    angles = pos_ids.astype(jnp.float32)[..., None] * inv_freq
    return jnp.cos(angles)[..., None, :], jnp.sin(angles)[..., None, :]


def rotate(values, cos_t, sin_t):
    half_dim = values.shape[-1] // 2
    first_half = values[..., :half_dim].astype(jnp.float32)
    second_half = values[..., half_dim:].astype(jnp.float32)
    rotated = jnp.concatenate([first_half * cos_t - second_half * sin_t,
                               second_half * cos_t + first_half * sin_t], axis=-1)
    return rotated.astype(jnp.bfloat16)


def norm_forward(values, gain_vec):
    values_f = values.astype(jnp.float32)
    inv_rms = lax.rsqrt(jnp.mean(values_f * values_f, axis=-1, keepdims=True) + NORM_EPS)
    normed = values_f * inv_rms * (1.0 + gain_vec.astype(jnp.float32))
    return normed.astype(jnp.bfloat16), inv_rms


def norm_backward(values, inv_rms, gain_vec, grads):
    values_f = values.astype(jnp.float32)
    grads_f = grads.astype(jnp.float32)
    scaled = grads_f * (1.0 + gain_vec.astype(jnp.float32))
    d_values = inv_rms * scaled - values_f * inv_rms ** 3 * jnp.mean(scaled * values_f, axis=-1, keepdims=True)
    d_gain = jnp.sum(grads_f * values_f * inv_rms, axis=0)
    return d_values, d_gain


def dot(a, b, dims):
    return lax.dot_general(a, b, ((dims[:1], dims[1:]), ((), ())), preferred_element_type=jnp.float32)


def solution(mesh):
    tok_spec = P('fsdp', 'cp', None)
    ids_spec = P('fsdp', 'cp')
    in_spec = P('fsdp', None, None)
    out_spec = P(None, None, 'fsdp')
    gain_spec = P('fsdp')
    bf, f32 = jnp.bfloat16, jnp.float32

    def layer_local(hidden, doc_ids, doc_pos, grad_out, w_query, w_key, w_value, w_out, gain_pre, gain_post):
        _, n_tok, model_dim = hidden.shape
        hidden, grad_out = hidden[0], grad_out[0]
        n_heads, head_dim = w_query.shape[1], w_query.shape[2]
        rows = w_query.shape[0]
        q_cols = n_heads * head_dim
        core = lax.axis_index('cp')
        w0 = jnp.concatenate([w_query.reshape(rows, q_cols), w_key.reshape(rows, head_dim),
                              w_value.reshape(rows, head_dim)], axis=1)
        w1 = w_out.reshape(q_cols, rows).T
        w2 = jnp.pad(jnp.stack([gain_pre, gain_post]).astype(f32), ((0, 0), (0, 128 - rows))).reshape(1, 256)
        w2 = jnp.pad(w2, ((0, 15), (0, 0)))
        wqkv, wo_t, gains = gather_weights(w0, w1, w2)
        gains = gains[..., 0, :].reshape(model_dim // rows, 256)
        pre_full, post_full = gains[:, :rows].reshape(model_dim), gains[:, 128:128 + rows].reshape(model_dim)
        wqkv = wqkv.reshape(model_dim, q_cols + 2 * head_dim)
        wo_t = wo_t.reshape(model_dim, q_cols)
        q_scale = (head_dim if head_dim >= 256 else model_dim // n_heads) ** -0.5

        normed, inv_pre = norm_forward(hidden, pre_full)
        qkv = dot(normed, wqkv, (1, 0)).astype(bf)
        q_proj = qkv[:, :q_cols].reshape(n_tok, n_heads, head_dim)
        k_proj = qkv[:, q_cols:q_cols + head_dim].reshape(n_tok, 1, head_dim)
        v_proj = qkv[:, q_cols + head_dim:]
        cos_t, sin_t = rope_tables(doc_pos[0], head_dim)
        q_rot = rotate(q_proj, cos_t, sin_t)
        k_rot = rotate(k_proj, cos_t, sin_t)[:, 0]

        swap = [(0, 1), (1, 0)]
        kv_own = jnp.concatenate([k_rot, v_proj], axis=1)
        kv_all = jnp.concatenate([lax.ppermute(kv_own, 'cp', swap), kv_own], axis=0)
        k_all, v_all = kv_all[:, :head_dim], kv_all[:, head_dim:]
        ids_all = jnp.concatenate([lax.ppermute(doc_ids[0], 'cp', swap), doc_ids[0]])[:, None]
        q_flat = q_rot.reshape(n_tok, q_cols)
        ratio = q_scale / SOFT_CAP
        attn_flat, inv_sum = attend(q_flat, k_all, v_all, ids_all, doc_ids, n_heads, ratio)
        proj_out = dot(attn_flat, wo_t, (1, 1)).astype(bf)
        post_out, inv_post = norm_forward(proj_out, post_full)
        out_hidden = (hidden.astype(f32) + post_out.astype(f32)).astype(bf)

        d_proj, d_gain_post = norm_backward(proj_out, inv_post, post_full, grad_out)
        d_proj = d_proj.astype(bf)
        d_attn = dot(d_proj, wo_t, (1, 0)).astype(bf)

        def halves(grads, acts):
            width = acts.shape[1] // 2
            own = dot(grads, lax.dynamic_slice_in_dim(acts, core * width, width, 1), (0, 0))
            other = dot(grads, lax.dynamic_slice_in_dim(acts, (1 - core) * width, width, 1), (0, 0)).astype(bf)
            shape = (SIDE, SIDE, SIDE, rows, width)
            return own.reshape(shape), other.reshape(shape)

        own1, sib1 = halves(d_proj, attn_flat)

        d_q_flat, d_k, d_v = attend_back(q_flat, d_attn, k_all, v_all, ids_all, doc_ids, inv_sum, n_heads, ratio)
        d_kv = jnp.concatenate([d_k, d_v], axis=1)
        d_kv = (d_kv[n_tok:].astype(f32) + lax.ppermute(d_kv[:n_tok], 'cp', swap).astype(f32)).astype(bf)
        d_k_rot, d_v_proj = d_kv[:, :head_dim], d_kv[:, head_dim:]
        d_q_rot = d_q_flat.reshape(n_tok, n_heads, head_dim)
        d_q_proj = rotate(d_q_rot, cos_t, -sin_t)
        d_k_proj = rotate(d_k_rot[:, None], cos_t, -sin_t)[:, 0]
        d_qkv = jnp.concatenate([d_q_proj.reshape(n_tok, q_cols), d_k_proj, d_v_proj], axis=1)

        d_normed = dot(d_qkv, wqkv, (1, 1)).astype(bf)
        own0, sib0 = halves(normed, d_qkv)
        d_hidden, d_gain_pre = norm_backward(hidden, inv_pre, pre_full, d_normed)
        grad_hidden = (grad_out.astype(f32) + d_hidden).astype(bf)
        d_gains = jnp.stack([d_gain_pre, d_gain_post]).reshape(2, SIDE, SIDE, SIDE, 1, rows)
        d_gains = jnp.pad(d_gains, ((0, 0), (0, 0), (0, 0), (0, 0), (0, 15), (0, 128 - rows)))
        own_g = lax.dynamic_index_in_dim(d_gains, core, 0, keepdims=False)
        sib_g = lax.dynamic_index_in_dim(d_gains, 1 - core, 0, keepdims=False)
        g0, g1, gg = scatter_grads(own0, own1, own_g, sib0, sib1, sib_g)
        g0 = jnp.concatenate([g0[0], g0[1]], axis=1)
        g1 = jnp.concatenate([g1[0], g1[1]], axis=1)
        return (out_hidden[None], grad_hidden[None], g0[:, :q_cols].reshape(rows, n_heads, head_dim),
                g0[:, q_cols:q_cols + head_dim].reshape(rows, 1, head_dim),
                g0[:, q_cols + head_dim:].reshape(rows, 1, head_dim),
                g1.T.reshape(n_heads, head_dim, rows), gg[0, 0, :rows], gg[1, 0, :rows])

    return jax.shard_map(layer_local, mesh=mesh,
                         in_specs=(tok_spec, ids_spec, ids_spec, tok_spec, in_spec, in_spec, in_spec, out_spec, gain_spec, gain_spec),
                         out_specs=(tok_spec, tok_spec, in_spec, in_spec, in_spec, out_spec, gain_spec, gain_spec),
                         check_vma=False)
```

```python
import functools

import jax
import jax.numpy as jnp
from jax import lax
from jax.experimental import pallas as pl
from jax.experimental.pallas import tpu as pltpu
from jax.sharding import PartitionSpec as P

SOFT_CAP = 50.0
NORM_EPS = 1e-6
ROPE_BASE = 10000.0
MESH = pl.DeviceIdType.MESH
SIDE = 4
VMEM_MAX = 67_043_328

QKV = ((0, 0, 512), (1, 512, 384), (2, 896, 384))
OUT = ((0, 0, 256), (1, 256, 384), (2, 640, 384))
GAIN = ((0, 0, 128),)
CHUNK = 256


def place():
    f = lax.axis_index('fsdp')
    return (f // 16, lax.rem(f // 4, 4), lax.rem(f, 4)), lax.axis_index('cp')


def shifted(coords, dim, delta):
    out = list(coords)
    out[dim] = lax.rem(coords[dim] + delta + SIDE, SIDE)
    return tuple(out)


def device(coords, core):
    return (coords[0] * 16 + coords[1] * 4 + coords[2], core)


def greet(coords, core):
    barrier = pltpu.get_barrier_semaphore()
    for dim in range(3):
        for delta in (1, -1):
            pl.semaphore_signal(barrier, inc=1, device_id=device(shifted(coords, dim, delta), core), device_id_type=MESH)
    pl.semaphore_signal(barrier, inc=1, device_id=device(coords, 1 - core), device_id_type=MESH)
    pl.semaphore_wait(barrier, 7)


def order_of(colour):
    return tuple((colour + i) % 3 for i in range(3))


def region(ref, full, coords, rows, cols):
    idx = [pl.ds(0, SIDE) if d in full else coords[d] for d in range(3)]
    return ref.at[idx[0], idx[1], idx[2], pl.ds(*rows), pl.ds(*cols)]


class Gather:
    def __init__(self, streams, src, out, send, recv, sib_send, sib_recv):
        self.streams, self.src, self.out = streams, src, out
        self.sems = (send, recv, sib_send, sib_recv)
        self.coords, self.core = place()
        self.rows = out.shape[3]

    def cols(self, s, side):
        _, off, width = self.streams[s]
        return pl.ds(pl.multiple_of(side * (self.out.shape[4] // 2) + off, 128), width)

    def part(self, s, p, kind, at, side):
        full = order_of(self.streams[s][0])[:p]
        idx = [pl.ds(0, SIDE) if d in full else at[d] for d in range(3)]
        half = self.rows // 2
        r0, nr = ((0, self.rows), (0, self.rows), (0, half), (half, half))[kind]
        return self.out.at[idx[0], idx[1], idx[2], pl.ds(r0, nr), self.cols(s, side)]

    def hop(self, s, p, kind):
        dim = order_of(self.streams[s][0])[p]
        at = shifted(self.coords, dim, (0, 0, -1, 1)[kind])
        to = shifted(self.coords, dim, (1, -1, 1, -1)[kind])
        dst = self.part(s, p, kind, at, self.core)
        src = self.src.at[:, self.cols(s, self.core)] if p == 0 and kind < 2 else dst
        return pltpu.make_async_remote_copy(src, dst, self.sems[0].at[s, p, kind], self.sems[1].at[s, p, kind],
                                            device_id=device(to, self.core), device_id_type=MESH)

    def landed(self, s, p, kind, side):
        dim = order_of(self.streams[s][0])[p]
        return self.part(s, p, kind, shifted(self.coords, dim, (-1, 1, -2, 2)[kind]), side)

    def gift(self, s, p, kind, side):
        here = self.landed(s, p, kind, side)
        return pltpu.make_async_remote_copy(here, here, self.sems[2].at[s, p, kind], self.sems[3].at[s, p, kind],
                                            device_id=device(self.coords, 1 - self.core), device_id_type=MESH)

    def arrive(self, s, p, kind):
        here = self.landed(s, p, kind, self.core)
        pltpu.make_async_remote_copy(here, here, self.sems[0].at[s, p, kind], self.sems[1].at[s, p, kind],
                                     device_id=device(self.coords, 1 - self.core), device_id_type=MESH).wait_recv()

    def start(self, s, p):
        self.hop(s, p, 0).start()
        self.hop(s, p, 1).start()

    def middle(self, s, p):
        for kind in (0, 1):
            self.arrive(s, p, kind)
            self.hop(s, p, kind + 2).start()
            self.gift(s, p, kind, self.core).start()

    def finish(self, s, p):
        for kind in (2, 3):
            self.arrive(s, p, kind)
            self.gift(s, p, kind, self.core).start()

    def drain(self, s, p):
        for kind in range(4):
            self.hop(s, p, kind).wait_send()
            self.gift(s, p, kind, self.core).wait_send()
            self.gift(s, p, kind, 1 - self.core).wait_recv()


def gather_kernel(in0, in1, in2, out0, out1, out2, *sems):
    coords, core = place()
    greet(coords, core)
    own_sem = sems[12]
    ins, outs = (in0, in1, in2), (out0, out1, out2)
    owns = [pltpu.make_async_copy(ins[g], outs[g].at[coords[0], coords[1], coords[2]], own_sem.at[g]) for g in range(3)]
    for copy in owns:
        copy.start()
    qkv, out, gain = (Gather(st, ins[g], outs[g], *sems[4 * g:4 * g + 4]) for g, st in enumerate((QKV, OUT, GAIN)))
    work = [(gain, 0)] + [(qkv, s) for s in range(3)] + [(out, s) for s in range(3)]
    for p in range(3):
        if p == 1:
            for copy in owns:
                copy.wait()
        for gather, s in work:
            if p > 0:
                gather.finish(s, p - 1)
            if p < 2 or gather is not out:
                gather.start(s, p)
        for gather, s in work:
            if p < 2 or gather is not out:
                gather.middle(s, p)
    for gather, s in work[:4]:
        gather.finish(s, 2)
    for gather, s in work:
        for p in range(2 if gather is out else 3):
            gather.drain(s, p)


def gather_weights(*ws):
    shapes = [jax.ShapeDtypeStruct((SIDE, SIDE, SIDE) + w.shape, w.dtype) for w in ws]
    dma = pltpu.SemaphoreType.DMA
    return pl.pallas_call(
        gather_kernel, name="gather_weights",
        out_shape=shapes,
        in_specs=[pl.BlockSpec(memory_space=pltpu.VMEM)] * 3,
        out_specs=[pl.BlockSpec(memory_space=pltpu.HBM)] * 3,
        scratch_shapes=[dma((len(st), 3, 4)) for st in (QKV, OUT, GAIN) for _ in range(4)] + [dma((3,))],
        compiler_params=pltpu.CompilerParams(collective_id=1, has_side_effects=True),
    )(*ws)


class Scatter:
    def __init__(self, streams, own, sib, acc, sbuf, rbuf, send, recv):
        self.streams, self.own, self.sib = streams, own, sib
        self.acc, self.sbuf, self.rbuf, self.sems = acc, sbuf, rbuf, (send, recv)
        self.coords, self.core = place()

    def half(self, s):
        return self.acc[s][0].shape[1] // 2

    def dim(self, s, q):
        return order_of(self.streams[s][0])[2 - q]

    def value(self, s, q, at, n, r0):
        colour, off, width = self.streams[s]
        order = order_of(colour)
        nr = self.half(s)
        idx = list(at)
        full = sorted(order[:2 - q])
        for d, digit in zip(full, (n // SIDE, lax.rem(n, SIDE)) if len(full) == 2 else (n,)):
            idx[d] = digit
        if q == 0:
            where = (idx[0] * 16 + idx[1] * 4 + idx[2], pl.ds(r0, nr), pl.ds(off, width))
            return self.own[where] + self.sib[where].astype(jnp.float32)
        m = 0
        for d in sorted(order[:3 - q]):
            m = m * SIDE + idx[d]
        return self.acc[s][q - 1][m, pl.ds(r0, nr), :]

    def hop(self, s, q, kind):
        lo, n = ((0, 2), (2, 2), (4, 1), (5, 1))[kind]
        to = shifted(self.coords, self.dim(s, q), (1, -1, 1, -1)[kind])
        return pltpu.make_async_remote_copy(
            self.sbuf[s][q].at[pl.ds(lo, n)], self.rbuf[s][q].at[pl.ds(lo, n)],
            self.sems[0].at[s, q, kind], self.sems[1].at[s, q, kind],
            device_id=device(to, self.core), device_id_type=MESH)

    def each(self, q, body):
        n = SIDE ** (2 - q)

        def step(i, carry):
            body(i)
            return carry
        lax.fori_loop(0, n, step, 0, unroll=min(n, 2))

    def one(self, s, q):
        dim, half, buf = self.dim(s, q), self.half(s), self.sbuf[s][q]
        far, right, left = (shifted(self.coords, dim, d) for d in (2, 1, -1))

        def to_right(n):
            buf[0, n] = self.value(s, q, far, n, 0).astype(buf.dtype)
            buf[1, n] = self.value(s, q, right, n, half).astype(buf.dtype)

        def to_left(n):
            buf[2, n] = self.value(s, q, far, n, half).astype(buf.dtype)
            buf[3, n] = self.value(s, q, left, n, 0).astype(buf.dtype)
        self.each(q, to_right)
        self.hop(s, q, 0).start()
        self.each(q, to_left)
        self.hop(s, q, 1).start()

    def two(self, s, q):
        dim, half, buf, got = self.dim(s, q), self.half(s), self.sbuf[s][q], self.rbuf[s][q]
        right, left = (shifted(self.coords, dim, d) for d in (1, -1))

        def to_right(n):
            buf[4, n] = (self.value(s, q, right, n, 0) + got[0, n].astype(jnp.float32)).astype(buf.dtype)

        def to_left(n):
            buf[5, n] = (self.value(s, q, left, n, half) + got[2, n].astype(jnp.float32)).astype(buf.dtype)
        self.hop(s, q, 0).wait_recv()
        self.each(q, to_right)
        self.hop(s, q, 2).start()
        self.hop(s, q, 1).wait_recv()
        self.each(q, to_left)
        self.hop(s, q, 3).start()

    def three(self, s, q):
        half, got, acc = self.half(s), self.rbuf[s][q], self.acc[s][q]
        self.hop(s, q, 2).wait_recv()
        self.hop(s, q, 3).wait_recv()

        def keep(n):
            for r0, i, j in ((0, 3, 4), (half, 1, 5)):
                acc[n, pl.ds(r0, half), :] = (self.value(s, q, self.coords, n, r0) + got[i, n].astype(jnp.float32)
                                              + got[j, n].astype(jnp.float32))
        self.each(q, keep)

    def drain(self, s, q):
        for kind in range(4):
            self.hop(s, q, kind).wait_send()


def transpose_into(dst, src):
    def strip(j, carry):
        at = pl.ds(pl.multiple_of(j * CHUNK, CHUNK), CHUNK)
        dst[at, :] = src[:, at].T
        return carry
    lax.fori_loop(0, src.shape[1] // CHUNK, strip, 0)


def grad_chunk(grads_t, acts, dst, side, j):
    half = dst.shape[2]
    rhs = acts[:, pl.ds(pl.multiple_of(side * half + j * CHUNK, CHUNK), CHUNK)]
    n_rows = 512

    def strip(i, carry):
        at = pl.multiple_of(i * n_rows, n_rows)
        out = nn(grads_t[pl.ds(at, n_rows), :], rhs).astype(dst.dtype)
        dst[pl.ds(i * (n_rows // 32), n_rows // 32), :, pl.ds(j * CHUNK, CHUNK)] = out.reshape(n_rows // 32, 32, CHUNK)
        return carry
    lax.fori_loop(0, grads_t.shape[0] // n_rows, strip, 0)


def chunk_gift(src, dst, send, recv, j):
    coords, core = place()
    at = pl.ds(j * CHUNK, CHUNK)
    return pltpu.make_async_remote_copy(src.at[:, :, at], dst.at[:, :, at], send.at[j], recv.at[j],
                                        device_id=device(coords, 1 - core), device_id_type=MESH)


def wire_shapes(streams, dtype, rows, phases):
    return [pltpu.VMEM((6, SIDE ** (2 - q), rows // 2, width), dtype) for _, _, width in streams for q in phases]


def acc_shapes(streams, rows, phases):
    return [((SIDE ** (2 - q), rows, width), jnp.float32) for _, _, width in streams for q in phases]


def scatter_kernel(normed, d_qkv, own_g, sib_g, acc_o0, acc_o1, acc_o2, out_q, out_o, out_g, *scratch):
    scratch = list(scratch)

    def take(n):
        head = scratch[:n]
        del scratch[:n]
        return head
    normed_t, own_q, sib_out, sib_q, sib_in_g = take(5)
    acc_q, sbuf_q, rbuf_q = take(9), take(9), take(9)
    acc_o, sbuf_o, rbuf_o = take(6), take(6), take(6)
    acc_g, sbuf_g, rbuf_g = take(3), take(3), take(3)
    sems = take(6)
    gift_send, gift_recv, gain_sem, fin_send, fin_recv = take(5)
    coords, core = place()
    sibling = device(coords, 1 - core)
    greet(coords, core)

    def triples(flat):
        return [flat[3 * s:3 * s + 3] for s in range(len(flat) // 3)]

    def tails(flat, heads):
        return [[heads[s]] + flat[2 * s:2 * s + 2] for s in range(3)]
    qkv = Scatter(QKV, own_q, sib_q, triples(acc_q), triples(sbuf_q), triples(rbuf_q), *sems[0:2])
    out = Scatter(OUT, None, None, tails(acc_o, (acc_o0, acc_o1, acc_o2)), tails(sbuf_o, (None,) * 3),
                  tails(rbuf_o, (None,) * 3), *sems[2:4])
    gain = Scatter(GAIN, own_g, sib_in_g, triples(acc_g), triples(sbuf_g), triples(rbuf_g), *sems[4:6])
    gain_gift = pltpu.make_async_remote_copy(sib_g, sib_in_g, gain_sem.at[0], gain_sem.at[1],
                                             device_id=sibling, device_id_type=MESH)
    gain_gift.start()
    for s in range(3):
        out.one(s, 1)
    transpose_into(normed_t, normed)
    chunks = own_q.shape[2] // CHUNK
    gifts = [chunk_gift(sib_out, sib_q, gift_send, gift_recv, j) for j in range(chunks)]
    for j in range(chunks):
        grad_chunk(normed_t, d_qkv, sib_out, 1 - core, j)
        gifts[j].start()
    for s in range(3):
        out.two(s, 1)
    gain_gift.wait_recv()
    gain.one(0, 0)
    done = 0
    for s, (_, off, width) in enumerate(QKV):
        while done * CHUNK < off + width:
            grad_chunk(normed_t, d_qkv, own_q, core, done)
            gifts[done].wait_recv()
            done += 1
        qkv.one(s, 0)
        if s == 0:
            for i in range(3):
                out.three(i, 1)
                out.one(i, 2)
    work = [(qkv, s) for s in range(3)] + [(gain, 0)]
    for q in range(3):
        for scatter, s in work:
            scatter.two(s, q)
        if q == 0:
            for s in range(3):
                out.two(s, 2)
        for scatter, s in work:
            scatter.three(s, q)
            if q < 2:
                scatter.one(s, q + 1)
        if q == 0:
            for s in range(3):
                out.three(s, 2)
    fins = []
    k = 0
    for scatter, ref in ((qkv, out_q), (out, out_o), (gain, out_g)):
        for s, (_, off, width) in enumerate(scatter.streams):
            part = scatter.acc[s][2].at[0]
            ref[core, :, pl.ds(off, width)] = scatter.acc[s][2][0]
            here, there = (ref.at[side, :, pl.ds(off, width)] for side in (core, 1 - core))
            pair = [pltpu.make_async_remote_copy(part, side, fin_send.at[k], fin_recv.at[k],
                                                 device_id=sibling, device_id_type=MESH) for side in (here, there)]
            pair[0].start()
            fins.append(pair)
            k += 1
    for mine, theirs in fins:
        mine.wait_send()
        theirs.wait_recv()
    for copy in gifts + [gain_gift]:
        copy.wait_send()
    for scatter, phases in ((qkv, (0, 1, 2)), (out, (1, 2)), (gain, (0, 1, 2))):
        for s in range(len(scatter.streams)):
            for q in phases:
                scatter.drain(s, q)


def scatter_grads(normed, d_qkv, own_g, sib_g, accs):
    bf, f32 = jnp.bfloat16, jnp.float32
    n_tok, model_dim = normed.shape
    half, rows = d_qkv.shape[1] // 2, 32
    blocks = model_dim // rows
    dma = pltpu.SemaphoreType.DMA
    vmem = pl.BlockSpec(memory_space=pltpu.VMEM)
    scratch = [pltpu.VMEM((model_dim, n_tok), bf), pltpu.VMEM((blocks, rows, half), f32),
               pltpu.VMEM((blocks, rows, half), bf), pltpu.VMEM((blocks, rows, half), bf), pltpu.VMEM(sib_g.shape, f32)]
    for streams, dtype, n_rows, phases in ((QKV, bf, rows, (0, 1, 2)), (OUT, bf, rows, (1, 2)), (GAIN, f32, 16, (0, 1, 2))):
        scratch += [pltpu.VMEM(*a) for a in acc_shapes(streams, n_rows, phases)]
        scratch += wire_shapes(streams, dtype, n_rows, phases) * 2
    scratch += [dma((len(st), 3, 4)) for st in (QKV, OUT, GAIN) for _ in range(2)]
    scratch += [dma((half // CHUNK,))] * 2 + [dma((2,))] + [dma((7,))] * 2
    return pl.pallas_call(
        scatter_kernel, name="scatter_grads",
        out_shape=[jax.ShapeDtypeStruct((2, rows, half), f32), jax.ShapeDtypeStruct((2, rows, 1024), f32),
                   jax.ShapeDtypeStruct((2, 16, 128), f32)],
        in_specs=[vmem] * 7, out_specs=[vmem] * 3, scratch_shapes=scratch,
        compiler_params=pltpu.CompilerParams(collective_id=2, has_side_effects=True, vmem_limit_bytes=VMEM_MAX),
    )(normed, d_qkv, own_g, sib_g, *accs)


LOG2E = 1.4426950408889634
TILE = 256


def nt(a, b):
    return lax.dot_general(a, b, (((1,), (1,)), ((), ())), preferred_element_type=jnp.float32)


def nn(a, b):
    return lax.dot_general(a, b, (((1,), (0,)), ((), ())), preferred_element_type=jnp.float32)


def fill_mask(mask, ids_k, ids_q):
    n_keys, n_q = mask.shape
    core = lax.axis_index('cp')
    for c in range(n_keys // TILE):
        base = jnp.where(c < n_q // TILE, (1 - core) * n_q, core * n_q - n_q) + c * TILE
        for i in range(n_q // TILE):
            k_at = base + lax.broadcasted_iota(jnp.int32, (TILE, TILE), 0)
            q_at = core * n_q + i * TILE + lax.broadcasted_iota(jnp.int32, (TILE, TILE), 1)
            same = ids_k[pl.ds(c * TILE, TILE), :] == ids_q[:, pl.ds(i * TILE, TILE)]
            mask[pl.ds(c * TILE, TILE), pl.ds(i * TILE, TILE)] = jnp.where(same & (k_at <= q_at), 1.0, 0.0)


def keys_for(i, n_q):
    return n_q + (i + 1) * TILE


def attend_kernel(ratio, q_ref, k_ref, v_ref, ids_k, ids_q, w_in, o_ref, inv_ref, w_ref, mask, v_t, w_scr, p_scr, *sems):
    n_q = q_ref.shape[0]
    greet(*place())
    out = Gather(OUT, None, w_ref, *sems)
    for s in range(3):
        out.start(s, 2)
    fill_mask(mask, ids_k, ids_q)
    v_t[...] = v_ref[...].T

    def head(h, carry):
        cols = pl.ds(pl.multiple_of(h * TILE, TILE), TILE)
        for i in range(n_q // TILE):
            qi = q_ref[pl.ds(i * TILE, TILE), cols]
            n_keys = keys_for(i, n_q)
            total = jnp.zeros((8, TILE), jnp.float32)
            for c in range(n_keys // TILE):
                t = jnp.tanh(nt(k_ref[pl.ds(c * TILE, TILE), :], qi) * ratio)
                w = jnp.exp2(t * (SOFT_CAP * LOG2E)) * mask[pl.ds(c * TILE, TILE), pl.ds(i * TILE, TILE)]
                w_scr[i, pl.ds(c * TILE, TILE), :] = w
                total = total + jnp.sum(w.reshape(TILE // 8, 8, TILE), axis=0)
            inv = 1.0 / jnp.sum(total, axis=0, keepdims=True)
            inv_ref[h, :, pl.ds(i * TILE, TILE)] = inv
            p_scr[i, pl.ds(0, n_keys), :] = (w_scr[i, pl.ds(0, n_keys), :] * inv).astype(jnp.bfloat16)
            o_t = nn(v_t[:, pl.ds(0, n_keys)], p_scr[i, pl.ds(0, n_keys), :])
            o_ref[pl.ds(i * TILE, TILE), cols] = o_t.T.astype(jnp.bfloat16)

        @pl.when(h == 4)
        def _():
            for s in range(3):
                out.middle(s, 2)
        return carry
    lax.fori_loop(0, q_ref.shape[1] // TILE, head, 0)
    for s in range(3):
        out.finish(s, 2)
    for s in range(3):
        out.drain(s, 2)


def attend(q, k, v, ids_k, ids_q, w_out, n_heads, ratio):
    n_q, n_k = q.shape[0], k.shape[0]
    vmem, hbm = pl.BlockSpec(memory_space=pltpu.VMEM), pl.BlockSpec(memory_space=pltpu.HBM)
    return pl.pallas_call(
        functools.partial(attend_kernel, ratio), name="attend",
        out_shape=[jax.ShapeDtypeStruct(q.shape, jnp.bfloat16), jax.ShapeDtypeStruct((n_heads, 1, n_q), jnp.float32),
                   jax.ShapeDtypeStruct(w_out.shape, w_out.dtype)],
        in_specs=[vmem] * 5 + [hbm], out_specs=[vmem] * 2 + [hbm], input_output_aliases={5: 2},
        scratch_shapes=[pltpu.VMEM((n_k, n_q), jnp.float32), pltpu.VMEM((TILE, n_k), jnp.bfloat16),
                        pltpu.VMEM((n_q // TILE, n_k, TILE), jnp.float32),
                        pltpu.VMEM((n_q // TILE, n_k, TILE), jnp.bfloat16)]
        + [pltpu.SemaphoreType.DMA((3, 3, 4))] * 4,
        compiler_params=pltpu.CompilerParams(collective_id=3, has_side_effects=True),
    )(q, k, v, ids_k, ids_q, w_out)


def attend_back_kernel(ratio, q_ref, do_ref, k_ref, v_ref, ids_k, ids_q, inv_ref, dz_ref, o_ref,
                       dq_ref, dk_ref, dv_ref, acc0, acc1, acc2,
                       mask, k_t, g_scr, dp_scr, p_scr, ds_scr, dk_acc, dv_acc, dz_t, own, sib_out, sib_in, *scratch):
    n_q = q_ref.shape[0]
    coords, core = place()
    greet(coords, core)
    sbuf, rbuf, sems = scratch[0:3], scratch[3:6], scratch[6:8]
    gift_send, gift_recv = scratch[8:10]
    out = Scatter(OUT, own, sib_in, [[a] for a in (acc0, acc1, acc2)], [[b] for b in sbuf], [[b] for b in rbuf], *sems)
    chunks = own.shape[2] // CHUNK
    transpose_into(dz_t, dz_ref)
    gifts = [chunk_gift(sib_out, sib_in, gift_send, gift_recv, j) for j in range(chunks)]
    for j in range(chunks):
        grad_chunk(dz_t, o_ref, sib_out, 1 - core, j)
        gifts[j].start()
    done = 0
    for s, (_, off, width) in enumerate(OUT):
        while done * CHUNK < off + width:
            grad_chunk(dz_t, o_ref, own, core, done)
            gifts[done].wait_recv()
            done += 1
        out.one(s, 0)
    fill_mask(mask, ids_k, ids_q)
    k_t[...] = k_ref[...].T
    dk_acc[...] = jnp.zeros_like(dk_acc)
    dv_acc[...] = jnp.zeros_like(dv_acc)

    def head(h, carry):
        cols = pl.ds(pl.multiple_of(h * TILE, TILE), TILE)
        for i in range(n_q // TILE):
            rows = pl.ds(i * TILE, TILE)
            qi, doi = q_ref[rows, cols], do_ref[rows, cols]
            inv = inv_ref[h, :, rows]
            n_keys = keys_for(i, n_q)
            total = jnp.zeros((8, TILE), jnp.float32)
            for c in range(n_keys // TILE):
                at = pl.ds(c * TILE, TILE)
                t = jnp.tanh(nt(k_ref[at, :], qi) * ratio)
                p = jnp.exp2(t * (SOFT_CAP * LOG2E)) * (mask[at, rows] * inv)
                dp = nt(v_ref[at, :], doi)
                p_scr[i, at, :] = p.astype(jnp.bfloat16)
                g_scr[i, at, :] = p * ((1.0 - t * t) * (ratio * SOFT_CAP))
                dp_scr[i, at, :] = dp
                total = total + jnp.sum((p * dp).reshape(TILE // 8, 8, TILE), axis=0)
            row_dot = jnp.sum(total, axis=0, keepdims=True)
            seen = pl.ds(0, n_keys)
            ds_scr[i, seen, :] = ((dp_scr[i, seen, :] - row_dot) * g_scr[i, seen, :]).astype(jnp.bfloat16)
            dq_t = nn(k_t[:, seen], ds_scr[i, seen, :])
            dq_ref[rows, cols] = dq_t.T.astype(jnp.bfloat16)
            dk_acc[seen, :] += nn(ds_scr[i, seen, :], qi)
            dv_acc[seen, :] += nn(p_scr[i, seen, :], doi)

        @pl.when(h == 3)
        def _():
            for s in range(3):
                out.two(s, 0)
        return carry
    lax.fori_loop(0, q_ref.shape[1] // TILE, head, 0)
    for s in range(3):
        out.three(s, 0)
    for s in range(3):
        out.drain(s, 0)
    for copy in gifts:
        copy.wait_send()
    dk_ref[...] = dk_acc[...].astype(jnp.bfloat16)
    dv_ref[...] = dv_acc[...].astype(jnp.bfloat16)


def attend_back(q, do, k, v, ids_k, ids_q, inv_sum, dz, o, n_heads, ratio):
    n_q, n_k = q.shape[0], k.shape[0]
    vmem = pl.BlockSpec(memory_space=pltpu.VMEM)
    tiles = n_q // TILE
    bf, f32 = jnp.bfloat16, jnp.float32
    return pl.pallas_call(
        functools.partial(attend_back_kernel, ratio), name="attend_back",
        out_shape=[jax.ShapeDtypeStruct(q.shape, bf)] + [jax.ShapeDtypeStruct(k.shape, bf)] * 2
        + [jax.ShapeDtypeStruct(*a) for a in acc_shapes(OUT, 32, (0,))],
        in_specs=[vmem] * 9, out_specs=[vmem] * 6,
        scratch_shapes=[pltpu.VMEM((n_k, n_q), f32), pltpu.VMEM((TILE, n_k), bf),
                        pltpu.VMEM((tiles, n_k, TILE), f32), pltpu.VMEM((tiles, n_k, TILE), f32),
                        pltpu.VMEM((tiles, n_k, TILE), bf), pltpu.VMEM((tiles, n_k, TILE), bf),
                        pltpu.VMEM((n_k, TILE), f32), pltpu.VMEM((n_k, TILE), f32),
                        pltpu.VMEM((dz.shape[1], n_q), bf), pltpu.VMEM((dz.shape[1] // 32, 32, o.shape[1] // 2), f32)]
        + [pltpu.VMEM((dz.shape[1] // 32, 32, o.shape[1] // 2), bf)] * 2
        + wire_shapes(OUT, bf, 32, (0,)) * 2 + [pltpu.SemaphoreType.DMA((3, 3, 4))] * 2
        + [pltpu.SemaphoreType.DMA((o.shape[1] // 2 // CHUNK,))] * 2,
        compiler_params=pltpu.CompilerParams(collective_id=4, has_side_effects=True, vmem_limit_bytes=VMEM_MAX),
    )(q, do, k, v, ids_k, ids_q, inv_sum, dz, o)


def rope_tables(pos_ids, head_dim):
    half_dim = head_dim // 2
    inv_freq = ROPE_BASE ** (-2.0 * jnp.arange(half_dim, dtype=jnp.float32) / head_dim)
    angles = pos_ids.astype(jnp.float32)[..., None] * inv_freq
    return jnp.cos(angles)[..., None, :], jnp.sin(angles)[..., None, :]


def rotate(values, cos_t, sin_t):
    half_dim = values.shape[-1] // 2
    first_half = values[..., :half_dim].astype(jnp.float32)
    second_half = values[..., half_dim:].astype(jnp.float32)
    rotated = jnp.concatenate([first_half * cos_t - second_half * sin_t,
                               second_half * cos_t + first_half * sin_t], axis=-1)
    return rotated.astype(jnp.bfloat16)


def norm_forward(values, gain_vec):
    values_f = values.astype(jnp.float32)
    inv_rms = lax.rsqrt(jnp.mean(values_f * values_f, axis=-1, keepdims=True) + NORM_EPS)
    normed = values_f * inv_rms * (1.0 + gain_vec.astype(jnp.float32))
    return normed.astype(jnp.bfloat16), inv_rms


def norm_backward(values, inv_rms, gain_vec, grads):
    values_f = values.astype(jnp.float32)
    grads_f = grads.astype(jnp.float32)
    scaled = grads_f * (1.0 + gain_vec.astype(jnp.float32))
    d_values = inv_rms * scaled - values_f * inv_rms ** 3 * jnp.mean(scaled * values_f, axis=-1, keepdims=True)
    d_gain = jnp.sum(grads_f * values_f * inv_rms, axis=0)
    return d_values, d_gain


def dot(a, b, dims):
    return lax.dot_general(a, b, ((dims[:1], dims[1:]), ((), ())), preferred_element_type=jnp.float32)


def solution(mesh):
    tok_spec = P('fsdp', 'cp', None)
    ids_spec = P('fsdp', 'cp')
    in_spec = P('fsdp', None, None)
    out_spec = P(None, None, 'fsdp')
    gain_spec = P('fsdp')
    bf, f32 = jnp.bfloat16, jnp.float32

    def layer_local(hidden, doc_ids, doc_pos, grad_out, w_query, w_key, w_value, w_out, gain_pre, gain_post):
        _, n_tok, model_dim = hidden.shape
        hidden, grad_out = hidden[0], grad_out[0]
        n_heads, head_dim = w_query.shape[1], w_query.shape[2]
        rows = w_query.shape[0]
        q_cols = n_heads * head_dim
        core = lax.axis_index('cp')
        w0 = jnp.concatenate([w_query.reshape(rows, q_cols), w_key.reshape(rows, head_dim),
                              w_value.reshape(rows, head_dim)], axis=1)
        w1 = w_out.reshape(q_cols, rows).T
        w2 = jnp.pad(jnp.stack([gain_pre, gain_post]).astype(f32), ((0, 0), (0, 128 - rows))).reshape(1, 256)
        w2 = jnp.pad(w2, ((0, 15), (0, 0)))
        wqkv, wo_t, gains = gather_weights(w0, w1, w2)
        gains = gains[..., 0, :].reshape(model_dim // rows, 256)
        pre_full, post_full = gains[:, :rows].reshape(model_dim), gains[:, 128:128 + rows].reshape(model_dim)
        wqkv = wqkv.reshape(model_dim, q_cols + 2 * head_dim)
        q_scale = (head_dim if head_dim >= 256 else model_dim // n_heads) ** -0.5

        normed, inv_pre = norm_forward(hidden, pre_full)
        qkv = dot(normed, wqkv, (1, 0)).astype(bf)
        q_proj = qkv[:, :q_cols].reshape(n_tok, n_heads, head_dim)
        k_proj = qkv[:, q_cols:q_cols + head_dim].reshape(n_tok, 1, head_dim)
        v_proj = qkv[:, q_cols + head_dim:]
        cos_t, sin_t = rope_tables(doc_pos[0], head_dim)
        q_rot = rotate(q_proj, cos_t, sin_t)
        k_rot = rotate(k_proj, cos_t, sin_t)[:, 0]

        swap = [(0, 1), (1, 0)]
        kv_own = jnp.concatenate([k_rot, v_proj], axis=1)
        kv_all = jnp.concatenate([lax.ppermute(kv_own, 'cp', swap), kv_own], axis=0)
        k_all, v_all = kv_all[:, :head_dim], kv_all[:, head_dim:]
        ids_all = jnp.concatenate([lax.ppermute(doc_ids[0], 'cp', swap), doc_ids[0]])[:, None]
        q_flat = q_rot.reshape(n_tok, q_cols)
        ratio = q_scale / SOFT_CAP
        attn_flat, inv_sum, wo_t = attend(q_flat, k_all, v_all, ids_all, doc_ids, wo_t, n_heads, ratio)
        wo_t = wo_t.reshape(model_dim, q_cols)
        proj_out = dot(attn_flat, wo_t, (1, 1)).astype(bf)
        post_out, inv_post = norm_forward(proj_out, post_full)
        out_hidden = (hidden.astype(f32) + post_out.astype(f32)).astype(bf)

        d_proj, d_gain_post = norm_backward(proj_out, inv_post, post_full, grad_out)
        d_proj = d_proj.astype(bf)
        d_attn = dot(d_proj, wo_t, (1, 0)).astype(bf)

        d_q_flat, d_k, d_v, *accs = attend_back(q_flat, d_attn, k_all, v_all, ids_all, doc_ids, inv_sum, d_proj, attn_flat,
                                                n_heads, ratio)
        d_kv = jnp.concatenate([d_k, d_v], axis=1)
        d_kv = (d_kv[n_tok:].astype(f32) + lax.ppermute(d_kv[:n_tok], 'cp', swap).astype(f32)).astype(bf)
        d_k_rot, d_v_proj = d_kv[:, :head_dim], d_kv[:, head_dim:]
        d_q_rot = d_q_flat.reshape(n_tok, n_heads, head_dim)
        d_q_proj = rotate(d_q_rot, cos_t, -sin_t)
        d_k_proj = rotate(d_k_rot[:, None], cos_t, -sin_t)[:, 0]
        d_qkv = jnp.concatenate([d_q_proj.reshape(n_tok, q_cols), d_k_proj, d_v_proj], axis=1)

        d_normed = dot(d_qkv, wqkv, (1, 1)).astype(bf)
        d_hidden, d_gain_pre = norm_backward(hidden, inv_pre, pre_full, d_normed)
        grad_hidden = (grad_out.astype(f32) + d_hidden).astype(bf)
        d_gains = jnp.stack([d_gain_pre, d_gain_post]).reshape(2, model_dim // rows, 1, rows)
        d_gains = jnp.pad(d_gains, ((0, 0), (0, 0), (0, 15), (0, 128 - rows)))
        own_g = lax.dynamic_index_in_dim(d_gains, core, 0, keepdims=False)
        sib_g = lax.dynamic_index_in_dim(d_gains, 1 - core, 0, keepdims=False)
        g0, g1, gg = scatter_grads(normed, d_qkv, own_g, sib_g, accs)
        g0 = jnp.concatenate([g0[0], g0[1]], axis=1)
        g1 = jnp.concatenate([g1[0], g1[1]], axis=1)
        return (out_hidden[None], grad_hidden[None], g0[:, :q_cols].reshape(rows, n_heads, head_dim),
                g0[:, q_cols:q_cols + head_dim].reshape(rows, 1, head_dim),
                g0[:, q_cols + head_dim:].reshape(rows, 1, head_dim),
                g1.T.reshape(n_heads, head_dim, rows), gg[0, 0, :rows], gg[1, 0, :rows])

    return jax.shard_map(layer_local, mesh=mesh,
                         in_specs=(tok_spec, ids_spec, ids_spec, tok_spec, in_spec, in_spec, in_spec, out_spec, gain_spec, gain_spec),
                         out_specs=(tok_spec, tok_spec, in_spec, in_spec, in_spec, out_spec, gain_spec, gain_spec),
                         check_vma=False)
```

```python
import functools

import jax
import jax.numpy as jnp
from jax import lax
from jax.experimental import pallas as pl
from jax.experimental.pallas import tpu as pltpu
from jax.sharding import PartitionSpec as P

SOFT_CAP = 50.0
NORM_EPS = 1e-6
ROPE_BASE = 10000.0
MESH = pl.DeviceIdType.MESH
SIDE = 4
VMEM_MAX = 67_043_328

QKV_IN = ((0, 0, 256), (1, 512, 256), (2, 896, 256), (0, 256, 256), (1, 768, 128), (2, 1152, 128))
QKV = ((0, 0, 256), (0, 256, 256), (1, 512, 256), (1, 768, 128), (2, 896, 256), (2, 1152, 128))
OUT = ((0, 0, 256), (1, 256, 384), (2, 640, 384))
GAIN = ((0, 0, 128),)
CHUNK = 256


def place():
    f = lax.axis_index('fsdp')
    return (f // 16, lax.rem(f // 4, 4), lax.rem(f, 4)), lax.axis_index('cp')


def shifted(coords, dim, delta):
    out = list(coords)
    out[dim] = lax.rem(coords[dim] + delta + SIDE, SIDE)
    return tuple(out)


def device(coords, core):
    return (coords[0] * 16 + coords[1] * 4 + coords[2], core)


def greet(coords, core):
    barrier = pltpu.get_barrier_semaphore()
    for dim in range(3):
        for delta in (1, -1):
            pl.semaphore_signal(barrier, inc=1, device_id=device(shifted(coords, dim, delta), core), device_id_type=MESH)
    pl.semaphore_signal(barrier, inc=1, device_id=device(coords, 1 - core), device_id_type=MESH)
    pl.semaphore_wait(barrier, 7)


def order_of(colour):
    return tuple((colour + i) % 3 for i in range(3))


def region(ref, full, coords, rows, cols):
    idx = [pl.ds(0, SIDE) if d in full else coords[d] for d in range(3)]
    return ref.at[idx[0], idx[1], idx[2], pl.ds(*rows), pl.ds(*cols)]


class Gather:
    def __init__(self, streams, src, out, send, recv, sib_send, sib_recv):
        self.streams, self.src, self.out = streams, src, out
        self.sems = (send, recv, sib_send, sib_recv)
        self.coords, self.core = place()
        self.rows = out.shape[3]

    def cols(self, s, side):
        _, off, width = self.streams[s]
        return pl.ds(pl.multiple_of(side * (self.out.shape[4] // 2) + off, 128), width)

    def part(self, s, p, kind, at, side):
        full = order_of(self.streams[s][0])[:p]
        idx = [pl.ds(0, SIDE) if d in full else at[d] for d in range(3)]
        half = self.rows // 2
        r0, nr = ((0, self.rows), (0, self.rows), (0, half), (half, half))[kind]
        return self.out.at[idx[0], idx[1], idx[2], pl.ds(r0, nr), self.cols(s, side)]

    def hop(self, s, p, kind):
        dim = order_of(self.streams[s][0])[p]
        at = shifted(self.coords, dim, (0, 0, -1, 1)[kind])
        to = shifted(self.coords, dim, (1, -1, 1, -1)[kind])
        dst = self.part(s, p, kind, at, self.core)
        src = self.src.at[:, self.cols(s, self.core)] if p == 0 and kind < 2 else dst
        return pltpu.make_async_remote_copy(src, dst, self.sems[0].at[s, p, kind], self.sems[1].at[s, p, kind],
                                            device_id=device(to, self.core), device_id_type=MESH)

    def landed(self, s, p, kind, side):
        dim = order_of(self.streams[s][0])[p]
        return self.part(s, p, kind, shifted(self.coords, dim, (-1, 1, -2, 2)[kind]), side)

    def gift(self, s, p, kind, side):
        here = self.landed(s, p, kind, side)
        return pltpu.make_async_remote_copy(here, here, self.sems[2].at[s, p, kind], self.sems[3].at[s, p, kind],
                                            device_id=device(self.coords, 1 - self.core), device_id_type=MESH)

    def arrive(self, s, p, kind):
        here = self.landed(s, p, kind, self.core)
        pltpu.make_async_remote_copy(here, here, self.sems[0].at[s, p, kind], self.sems[1].at[s, p, kind],
                                     device_id=device(self.coords, 1 - self.core), device_id_type=MESH).wait_recv()

    def start(self, s, p):
        self.hop(s, p, 0).start()
        self.hop(s, p, 1).start()

    def middle(self, s, p):
        for kind in (0, 1):
            self.arrive(s, p, kind)
            self.hop(s, p, kind + 2).start()
            self.gift(s, p, kind, self.core).start()

    def finish(self, s, p):
        for kind in (2, 3):
            self.arrive(s, p, kind)
            self.gift(s, p, kind, self.core).start()

    def drain(self, s, p):
        for kind in range(4):
            self.hop(s, p, kind).wait_send()
            self.gift(s, p, kind, self.core).wait_send()
            self.gift(s, p, kind, 1 - self.core).wait_recv()


class Scatter:
    def __init__(self, streams, own, sib, acc, sbuf, rbuf, send, recv):
        self.streams, self.own, self.sib = streams, own, sib
        self.acc, self.sbuf, self.rbuf, self.sems = acc, sbuf, rbuf, (send, recv)
        self.coords, self.core = place()

    def half(self, s):
        return self.acc[s][0].shape[1] // 2

    def dim(self, s, q):
        return order_of(self.streams[s][0])[2 - q]

    def value(self, s, q, at, n, r0):
        colour, off, width = self.streams[s]
        order = order_of(colour)
        nr = self.half(s)
        idx = list(at)
        full = sorted(order[:2 - q])
        for d, digit in zip(full, (n // SIDE, lax.rem(n, SIDE)) if len(full) == 2 else (n,)):
            idx[d] = digit
        if q == 0:
            where = (idx[0] * 16 + idx[1] * 4 + idx[2], pl.ds(r0, nr), pl.ds(off, width))
            return self.own[where] + self.sib[where].astype(jnp.float32)
        m = 0
        for d in sorted(order[:3 - q]):
            m = m * SIDE + idx[d]
        return self.acc[s][q - 1][m, pl.ds(r0, nr), :]

    def hop(self, s, q, kind):
        lo, n = ((0, 2), (2, 2), (4, 1), (5, 1))[kind]
        to = shifted(self.coords, self.dim(s, q), (1, -1, 1, -1)[kind])
        return pltpu.make_async_remote_copy(
            self.sbuf[s][q].at[pl.ds(lo, n)], self.rbuf[s][q].at[pl.ds(lo, n)],
            self.sems[0].at[s, q, kind], self.sems[1].at[s, q, kind],
            device_id=device(to, self.core), device_id_type=MESH)

    def each(self, q, body):
        n = SIDE ** (2 - q)

        def step(i, carry):
            body(i)
            return carry
        lax.fori_loop(0, n, step, 0, unroll=min(n, 2))

    def one(self, s, q):
        dim, half, buf = self.dim(s, q), self.half(s), self.sbuf[s][q]
        far, right, left = (shifted(self.coords, dim, d) for d in (2, 1, -1))

        def to_right(n):
            buf[0, n] = self.value(s, q, far, n, 0).astype(buf.dtype)
            buf[1, n] = self.value(s, q, right, n, half).astype(buf.dtype)

        def to_left(n):
            buf[2, n] = self.value(s, q, far, n, half).astype(buf.dtype)
            buf[3, n] = self.value(s, q, left, n, 0).astype(buf.dtype)
        self.each(q, to_right)
        self.hop(s, q, 0).start()
        self.each(q, to_left)
        self.hop(s, q, 1).start()

    def two(self, s, q):
        dim, half, buf, got = self.dim(s, q), self.half(s), self.sbuf[s][q], self.rbuf[s][q]
        right, left = (shifted(self.coords, dim, d) for d in (1, -1))

        def to_right(n):
            buf[4, n] = (self.value(s, q, right, n, 0) + got[0, n].astype(jnp.float32)).astype(buf.dtype)

        def to_left(n):
            buf[5, n] = (self.value(s, q, left, n, half) + got[2, n].astype(jnp.float32)).astype(buf.dtype)
        self.hop(s, q, 0).wait_recv()
        self.each(q, to_right)
        self.hop(s, q, 2).start()
        self.hop(s, q, 1).wait_recv()
        self.each(q, to_left)
        self.hop(s, q, 3).start()

    def three(self, s, q):
        half, got, acc = self.half(s), self.rbuf[s][q], self.acc[s][q]
        self.hop(s, q, 2).wait_recv()
        self.hop(s, q, 3).wait_recv()

        def keep(n):
            for r0, i, j in ((0, 3, 4), (half, 1, 5)):
                acc[n, pl.ds(r0, half), :] = (self.value(s, q, self.coords, n, r0) + got[i, n].astype(jnp.float32)
                                              + got[j, n].astype(jnp.float32))
        self.each(q, keep)

    def drain(self, s, q):
        for kind in range(4):
            self.hop(s, q, kind).wait_send()


def transpose_into(dst, src):
    def strip(j, carry):
        at = pl.ds(pl.multiple_of(j * CHUNK, CHUNK), CHUNK)
        dst[at, :] = src[:, at].T
        return carry
    lax.fori_loop(0, src.shape[1] // CHUNK, strip, 0)


def grad_chunk(grads_t, acts, dst, side, j):
    half = dst.shape[2]
    rhs = acts[:, pl.ds(pl.multiple_of(side * half + j * CHUNK, CHUNK), CHUNK)]
    n_rows = 512

    def strip(i, carry):
        at = pl.multiple_of(i * n_rows, n_rows)
        out = nn(grads_t[pl.ds(at, n_rows), :], rhs).astype(dst.dtype)
        dst[pl.ds(i * (n_rows // 32), n_rows // 32), :, pl.ds(j * CHUNK, CHUNK)] = out.reshape(n_rows // 32, 32, CHUNK)
        return carry
    lax.fori_loop(0, grads_t.shape[0] // n_rows, strip, 0)


def chunk_gift(src, dst, send, recv, j):
    coords, core = place()
    at = pl.ds(j * CHUNK, CHUNK)
    return pltpu.make_async_remote_copy(src.at[:, :, at], dst.at[:, :, at], send.at[j], recv.at[j],
                                        device_id=device(coords, 1 - core), device_id_type=MESH)


def wire_shapes(streams, dtype, rows, phases):
    return [pltpu.VMEM((6, SIDE ** (2 - q), rows // 2, width), dtype) for _, _, width in streams for q in phases]


def acc_shapes(streams, rows, phases):
    return [((SIDE ** (2 - q), rows, width), jnp.float32) for _, _, width in streams for q in phases]


def scatter_kernel(normed, d_qkv, own_g, sib_g, acc_o0, acc_o1, acc_o2, out_q, out_o, out_g, *scratch):
    scratch = list(scratch)

    def take(n):
        head = scratch[:n]
        del scratch[:n]
        return head
    normed_t, own_q, sib_out, sib_q, sib_in_g = take(5)
    nq = len(QKV)
    acc_q, sbuf_q, rbuf_q = take(3 * nq), take(3 * nq), take(3 * nq)
    acc_o, sbuf_o, rbuf_o = take(6), take(6), take(6)
    acc_g, sbuf_g, rbuf_g = take(3), take(3), take(3)
    sems = take(6)
    gift_send, gift_recv, gain_sem, fin_send, fin_recv = take(5)
    coords, core = place()
    sibling = device(coords, 1 - core)
    greet(coords, core)

    def triples(flat):
        return [flat[3 * s:3 * s + 3] for s in range(len(flat) // 3)]

    def tails(flat, heads):
        return [[heads[s]] + flat[2 * s:2 * s + 2] for s in range(3)]
    qkv = Scatter(QKV, own_q, sib_q, triples(acc_q), triples(sbuf_q), triples(rbuf_q), *sems[0:2])
    out = Scatter(OUT, None, None, tails(acc_o, (acc_o0, acc_o1, acc_o2)), tails(sbuf_o, (None,) * 3),
                  tails(rbuf_o, (None,) * 3), *sems[2:4])
    gain = Scatter(GAIN, own_g, sib_in_g, triples(acc_g), triples(sbuf_g), triples(rbuf_g), *sems[4:6])
    gain_gift = pltpu.make_async_remote_copy(sib_g, sib_in_g, gain_sem.at[0], gain_sem.at[1],
                                             device_id=sibling, device_id_type=MESH)
    gain_gift.start()
    for s in range(3):
        out.one(s, 1)
    transpose_into(normed_t, normed)
    chunks = own_q.shape[2] // CHUNK
    gifts = [chunk_gift(sib_out, sib_q, gift_send, gift_recv, j) for j in range(chunks)]
    for j in range(chunks):
        grad_chunk(normed_t, d_qkv, sib_out, 1 - core, j)
        gifts[j].start()
    for s in range(3):
        out.two(s, 1)
    gain_gift.wait_recv()
    gain.one(0, 0)
    done = 0
    for s, (_, off, width) in enumerate(QKV):
        while done * CHUNK < off + width:
            grad_chunk(normed_t, d_qkv, own_q, core, done)
            gifts[done].wait_recv()
            done += 1
        qkv.one(s, 0)
        if s == 0:
            for i in range(3):
                out.three(i, 1)
                out.one(i, 2)
    work = [(qkv, s) for s in range(nq)] + [(gain, 0)]
    for q in range(3):
        for scatter, s in work:
            scatter.two(s, q)
        if q == 0:
            for s in range(3):
                out.two(s, 2)
        for scatter, s in work:
            scatter.three(s, q)
            if q < 2:
                scatter.one(s, q + 1)
        if q == 0:
            for s in range(3):
                out.three(s, 2)
    fins = []
    k = 0
    for scatter, ref in ((qkv, out_q), (out, out_o), (gain, out_g)):
        for s, (_, off, width) in enumerate(scatter.streams):
            part = scatter.acc[s][2].at[0]
            ref[core, :, pl.ds(off, width)] = scatter.acc[s][2][0]
            here, there = (ref.at[side, :, pl.ds(off, width)] for side in (core, 1 - core))
            pair = [pltpu.make_async_remote_copy(part, side, fin_send.at[k], fin_recv.at[k],
                                                 device_id=sibling, device_id_type=MESH) for side in (here, there)]
            pair[0].start()
            fins.append(pair)
            k += 1
    for mine, theirs in fins:
        mine.wait_send()
        theirs.wait_recv()
    for copy in gifts + [gain_gift]:
        copy.wait_send()
    for scatter, phases in ((qkv, (0, 1, 2)), (out, (1, 2)), (gain, (0, 1, 2))):
        for s in range(len(scatter.streams)):
            for q in phases:
                scatter.drain(s, q)


def scatter_grads(normed, d_qkv, own_g, sib_g, accs):
    bf, f32 = jnp.bfloat16, jnp.float32
    n_tok, model_dim = normed.shape
    half, rows = d_qkv.shape[1] // 2, 32
    blocks = model_dim // rows
    dma = pltpu.SemaphoreType.DMA
    vmem = pl.BlockSpec(memory_space=pltpu.VMEM)
    scratch = [pltpu.VMEM((model_dim, n_tok), bf), pltpu.VMEM((blocks, rows, half), f32),
               pltpu.VMEM((blocks, rows, half), bf), pltpu.VMEM((blocks, rows, half), bf), pltpu.VMEM(sib_g.shape, f32)]
    for streams, dtype, n_rows, phases in ((QKV, bf, rows, (0, 1, 2)), (OUT, bf, rows, (1, 2)), (GAIN, f32, 16, (0, 1, 2))):
        scratch += [pltpu.VMEM(*a) for a in acc_shapes(streams, n_rows, phases)]
        scratch += wire_shapes(streams, dtype, n_rows, phases) * 2
    scratch += [dma((len(st), 3, 4)) for st in (QKV, OUT, GAIN) for _ in range(2)]
    scratch += [dma((half // CHUNK,))] * 2 + [dma((2,))] + [dma((len(QKV) + 4,))] * 2
    return pl.pallas_call(
        scatter_kernel, name="scatter_grads",
        out_shape=[jax.ShapeDtypeStruct((2, rows, half), f32), jax.ShapeDtypeStruct((2, rows, 1024), f32),
                   jax.ShapeDtypeStruct((2, 16, 128), f32)],
        in_specs=[vmem] * 7, out_specs=[vmem] * 3, scratch_shapes=scratch,
        compiler_params=pltpu.CompilerParams(collective_id=2, has_side_effects=True, vmem_limit_bytes=VMEM_MAX),
    )(normed, d_qkv, own_g, sib_g, *accs)


LOG2E = 1.4426950408889634
TILE = 256


def nt(a, b):
    return lax.dot_general(a, b, (((1,), (1,)), ((), ())), preferred_element_type=jnp.float32)


def nn(a, b):
    return lax.dot_general(a, b, (((1,), (0,)), ((), ())), preferred_element_type=jnp.float32)


def fill_mask(mask, pos):
    n_keys, n_q = mask.shape
    core = lax.axis_index('cp')
    for c in range(n_keys // TILE):
        base = jnp.where(c < n_q // TILE, (1 - core) * n_q, core * n_q - n_q) + c * TILE
        for i in range(n_q // TILE):
            k_at = base + lax.broadcasted_iota(jnp.int32, (TILE, TILE), 0)
            q_at = core * n_q + i * TILE + lax.broadcasted_iota(jnp.int32, (TILE, TILE), 1)
            seen = (k_at <= q_at) & (k_at >= q_at - pos[:, pl.ds(i * TILE, TILE)])
            mask[pl.ds(c * TILE, TILE), pl.ds(i * TILE, TILE)] = jnp.where(seen, 1.0, 0.0)


def keys_for(i, n_q):
    return n_q + (i + 1) * TILE


def forward_kernel(ratio, x_ref, cos_ref, sin_ref, pos, in0, in1, in2,
                   wq_out, wo_out, gain_out, normed, inv_rms, q_ref, kv_ref, o_ref, inv_ref,
                   wq, gains, gain_row, mask, v_t, w_scr, p_scr, *sems):
    n_q, dim = x_ref.shape
    bf, f32 = jnp.bfloat16, jnp.float32
    coords, core = place()
    sibling = device(coords, 1 - core)
    greet(coords, core)
    own_sem, swap_send, swap_recv = sems[12:15]
    qkv, out, gain = (Gather(st, src, dst, *sems[4 * g:4 * g + 4]) for g, (st, src, dst) in enumerate(
        ((QKV_IN, in0, wq), (OUT, in1, wo_out), (GAIN, in2, gains))))
    nq = range(len(QKV_IN))
    gain.start(0, 0)
    for s in nq:
        qkv.start(s, 0)
    for s in range(3):
        out.start(s, 0)
    own_out = pltpu.make_async_copy(in1, wo_out.at[coords[0], coords[1], coords[2]], own_sem.at[0])
    own_out.start()
    wq[coords[0], coords[1], coords[2]] = in0[...]
    gains[coords[0], coords[1], coords[2]] = in2[...]

    def stats(i, carry):
        at = pl.ds(i * 64, 64)
        v = x_ref[at, :].astype(f32)
        inv_rms[at, :] = lax.rsqrt(jnp.sum(v * v, axis=1, keepdims=True) * (1.0 / dim) + NORM_EPS)
        return carry
    lax.fori_loop(0, n_q // 64, stats, 0)
    gain.middle(0, 0)
    for s in nq:
        qkv.middle(s, 0)
    gain.finish(0, 0)
    gain.start(0, 1)
    for s in nq:
        qkv.finish(s, 0)
        qkv.start(s, 1)
    for s in range(3):
        out.middle(s, 0)
    gain.middle(0, 1)
    for s in nq:
        qkv.middle(s, 1)
    gain.finish(0, 1)
    gain.start(0, 2)
    for s in range(3):
        out.finish(s, 0)
    own_out.wait()
    for s in nq:
        qkv.finish(s, 1)
        qkv.start(s, 2)
    for s in range(3):
        out.start(s, 1)
    gain.middle(0, 2)
    gain.finish(0, 2)
    for p in range(3):
        gain.drain(0, p)
    for kind in range(2):
        for j in range(16):
            row = sum(gains[j // 4, j % 4, x, pl.ds(0, 1), pl.ds(kind * 128, 128)] for x in range(SIDE))
            gain_row[pl.ds(kind, 1), pl.ds(j * 128, 128)] = row
    gain_out[...] = gain_row[...]
    fill_mask(mask, pos)

    def scale(i, carry):
        at = pl.ds(i * 64, 64)
        normed[at, :] = (x_ref[at, :].astype(f32) * inv_rms[at, :] * (1.0 + gain_row[pl.ds(0, 1), :])).astype(bf)
        return carry
    lax.fori_loop(0, n_q // 64, scale, 0)
    for s in nq:
        qkv.middle(s, 2)
    for s in range(3):
        out.middle(s, 1)
    for s in nq:
        qkv.finish(s, 2)
    for s in range(3):
        out.finish(s, 1)
        out.start(s, 2)
    for s in nq:
        for p in range(3):
            qkv.drain(s, p)
    keep = pltpu.make_async_copy(wq, wq_out, own_sem.at[1])
    keep.start()

    def project(n):
        rhs = wq[:, :, :, :, pl.ds(pl.multiple_of(n * TILE, TILE), TILE)].reshape(dim, TILE)
        return nn(normed[...], rhs).astype(bf)

    def rope(u):
        lo, hi = u[:, :TILE // 2].astype(f32), u[:, TILE // 2:].astype(f32)
        c, s = cos_ref[...], sin_ref[...]
        return jnp.concatenate([lo * c - hi * s, hi * c + lo * s], axis=1).astype(bf)
    n_heads = q_ref.shape[1] // TILE
    mine, other = pl.ds(n_q, n_q), pl.ds(0, n_q)
    kv_ref[mine, pl.ds(0, TILE)] = rope(project(n_heads))
    kv_ref[mine, pl.ds(TILE, TILE)] = project(n_heads + 1)
    swap = pltpu.make_async_remote_copy(kv_ref.at[mine], kv_ref.at[other], swap_send.at[0], swap_recv.at[0],
                                        device_id=sibling, device_id_type=MESH)
    swap.start()

    def project_head(h, carry):
        q_ref[:, pl.ds(pl.multiple_of(h * TILE, TILE), TILE)] = rope(project(h))
        return carry
    lax.fori_loop(0, n_heads, project_head, 0)
    for s in range(3):
        out.middle(s, 2)
    swap.wait_recv()
    k_cols = pl.ds(0, TILE)
    v_t[...] = kv_ref[:, pl.ds(TILE, TILE)].T

    def head(h, carry):
        cols = pl.ds(pl.multiple_of(h * TILE, TILE), TILE)
        for i in range(n_q // TILE):
            qi = q_ref[pl.ds(i * TILE, TILE), cols]
            n_keys = keys_for(i, n_q)
            total = jnp.zeros((8, TILE), f32)
            for c in range(n_keys // TILE):
                t = jnp.tanh(nt(kv_ref[pl.ds(c * TILE, TILE), k_cols], qi) * ratio)
                w = jnp.exp2(t * (SOFT_CAP * LOG2E)) * mask[pl.ds(c * TILE, TILE), pl.ds(i * TILE, TILE)]
                w_scr[i, pl.ds(c * TILE, TILE), :] = w
                total = total + jnp.sum(w.reshape(TILE // 8, 8, TILE), axis=0)
            inv = 1.0 / jnp.sum(total, axis=0, keepdims=True)
            inv_ref[h, :, pl.ds(i * TILE, TILE)] = inv
            p_scr[i, pl.ds(0, n_keys), :] = (w_scr[i, pl.ds(0, n_keys), :] * inv).astype(bf)
            o_t = nn(v_t[:, pl.ds(0, n_keys)], p_scr[i, pl.ds(0, n_keys), :])
            o_ref[pl.ds(i * TILE, TILE), cols] = o_t.T.astype(bf)
        return carry
    lax.fori_loop(0, n_heads, head, 0)
    for s in range(3):
        out.finish(s, 2)
    for s in range(3):
        for p in range(3):
            out.drain(s, p)
    swap.wait_send()
    keep.wait()


def forward(x, cos_t, sin_t, pos, w0, w1, w2, n_heads, ratio):
    n_q, dim = x.shape
    n_k = 2 * n_q
    bf, f32 = jnp.bfloat16, jnp.float32
    dma = pltpu.SemaphoreType.DMA
    vmem, hbm = pl.BlockSpec(memory_space=pltpu.VMEM), pl.BlockSpec(memory_space=pltpu.HBM)
    grid = (SIDE, SIDE, SIDE)
    shape = jax.ShapeDtypeStruct
    tiles = n_q // TILE
    return pl.pallas_call(
        functools.partial(forward_kernel, ratio), name="forward",
        out_shape=[shape(grid + w0.shape, bf), shape(grid + w1.shape, bf), shape((2, dim), f32), shape((n_q, dim), bf),
                   shape((n_q, 1), f32), shape((n_q, n_heads * TILE), bf), shape((n_k, 2 * TILE), bf),
                   shape((n_q, n_heads * TILE), bf), shape((n_heads, 1, n_q), f32)],
        in_specs=[vmem] * 7, out_specs=[hbm] * 2 + [vmem] * 7,
        scratch_shapes=[pltpu.VMEM(grid + w0.shape, bf), pltpu.VMEM(grid + w2.shape, f32), pltpu.VMEM((2, dim), f32),
                        pltpu.VMEM((n_k, n_q), f32), pltpu.VMEM((TILE, n_k), bf),
                        pltpu.VMEM((tiles, n_k, TILE), f32), pltpu.VMEM((tiles, n_k, TILE), bf)]
        + [dma((len(st), 3, 4)) for st in (QKV_IN, OUT, GAIN) for _ in range(4)]
        + [dma((2,)), dma((1,)), dma((1,))],
        compiler_params=pltpu.CompilerParams(collective_id=1, has_side_effects=True, vmem_limit_bytes=VMEM_MAX),
    )(x, cos_t, sin_t, pos, w0, w1, w2)


def attend_back_kernel(ratio, q_ref, do_ref, kv_ref, pos, inv_ref, dz_ref, o_ref,
                       dq_ref, dk_ref, dv_ref, acc0, acc1, acc2,
                       mask, k_t, g_scr, dp_scr, p_scr, ds_scr, dk_acc, dv_acc, dz_t, own, sib_out, sib_in, *scratch):
    n_q = q_ref.shape[0]
    coords, core = place()
    greet(coords, core)
    sbuf, rbuf, sems = scratch[0:3], scratch[3:6], scratch[6:8]
    gift_send, gift_recv = scratch[8:10]
    out = Scatter(OUT, own, sib_in, [[a] for a in (acc0, acc1, acc2)], [[b] for b in sbuf], [[b] for b in rbuf], *sems)
    chunks = own.shape[2] // CHUNK
    transpose_into(dz_t, dz_ref)
    gifts = [chunk_gift(sib_out, sib_in, gift_send, gift_recv, j) for j in range(chunks)]
    for j in range(chunks):
        grad_chunk(dz_t, o_ref, sib_out, 1 - core, j)
        gifts[j].start()
    done = 0
    for s, (_, off, width) in enumerate(OUT):
        while done * CHUNK < off + width:
            grad_chunk(dz_t, o_ref, own, core, done)
            gifts[done].wait_recv()
            done += 1
        out.one(s, 0)
    fill_mask(mask, pos)
    k_cols, v_cols = pl.ds(0, TILE), pl.ds(TILE, TILE)
    k_t[...] = kv_ref[:, k_cols].T
    dk_acc[...] = jnp.zeros_like(dk_acc)
    dv_acc[...] = jnp.zeros_like(dv_acc)

    def head(h, carry):
        cols = pl.ds(pl.multiple_of(h * TILE, TILE), TILE)
        for i in range(n_q // TILE):
            rows = pl.ds(i * TILE, TILE)
            qi, doi = q_ref[rows, cols], do_ref[rows, cols]
            inv = inv_ref[h, :, rows]
            n_keys = keys_for(i, n_q)
            total = jnp.zeros((8, TILE), jnp.float32)
            for c in range(n_keys // TILE):
                at = pl.ds(c * TILE, TILE)
                t = jnp.tanh(nt(kv_ref[at, k_cols], qi) * ratio)
                p = jnp.exp2(t * (SOFT_CAP * LOG2E)) * (mask[at, rows] * inv)
                dp = nt(kv_ref[at, v_cols], doi)
                p_scr[i, at, :] = p.astype(jnp.bfloat16)
                g_scr[i, at, :] = p * ((1.0 - t * t) * (ratio * SOFT_CAP))
                dp_scr[i, at, :] = dp
                total = total + jnp.sum((p * dp).reshape(TILE // 8, 8, TILE), axis=0)
            row_dot = jnp.sum(total, axis=0, keepdims=True)
            seen = pl.ds(0, n_keys)
            ds_scr[i, seen, :] = ((dp_scr[i, seen, :] - row_dot) * g_scr[i, seen, :]).astype(jnp.bfloat16)
            dq_t = nn(k_t[:, seen], ds_scr[i, seen, :])
            dq_ref[rows, cols] = dq_t.T.astype(jnp.bfloat16)
            dk_acc[seen, :] += nn(ds_scr[i, seen, :], qi)
            dv_acc[seen, :] += nn(p_scr[i, seen, :], doi)

        @pl.when(h == 3)
        def _():
            for s in range(3):
                out.two(s, 0)
        return carry
    lax.fori_loop(0, q_ref.shape[1] // TILE, head, 0)
    for s in range(3):
        out.three(s, 0)
    for s in range(3):
        out.drain(s, 0)
    for copy in gifts:
        copy.wait_send()
    dk_ref[...] = dk_acc[...].astype(jnp.bfloat16)
    dv_ref[...] = dv_acc[...].astype(jnp.bfloat16)


def attend_back(q, do, kv, pos, inv_sum, dz, o, ratio):
    n_q, n_k = q.shape[0], kv.shape[0]
    vmem = pl.BlockSpec(memory_space=pltpu.VMEM)
    tiles = n_q // TILE
    bf, f32 = jnp.bfloat16, jnp.float32
    return pl.pallas_call(
        functools.partial(attend_back_kernel, ratio), name="attend_back",
        out_shape=[jax.ShapeDtypeStruct(q.shape, bf)] + [jax.ShapeDtypeStruct((n_k, TILE), bf)] * 2
        + [jax.ShapeDtypeStruct(*a) for a in acc_shapes(OUT, 32, (0,))],
        in_specs=[vmem] * 7, out_specs=[vmem] * 6,
        scratch_shapes=[pltpu.VMEM((n_k, n_q), f32), pltpu.VMEM((TILE, n_k), bf),
                        pltpu.VMEM((tiles, n_k, TILE), f32), pltpu.VMEM((tiles, n_k, TILE), f32),
                        pltpu.VMEM((tiles, n_k, TILE), bf), pltpu.VMEM((tiles, n_k, TILE), bf),
                        pltpu.VMEM((n_k, TILE), f32), pltpu.VMEM((n_k, TILE), f32),
                        pltpu.VMEM((dz.shape[1], n_q), bf), pltpu.VMEM((dz.shape[1] // 32, 32, o.shape[1] // 2), f32)]
        + [pltpu.VMEM((dz.shape[1] // 32, 32, o.shape[1] // 2), bf)] * 2
        + wire_shapes(OUT, bf, 32, (0,)) * 2 + [pltpu.SemaphoreType.DMA((3, 3, 4))] * 2
        + [pltpu.SemaphoreType.DMA((o.shape[1] // 2 // CHUNK,))] * 2,
        compiler_params=pltpu.CompilerParams(collective_id=4, has_side_effects=True, vmem_limit_bytes=VMEM_MAX),
    )(q, do, kv, pos, inv_sum, dz, o)


def rope_tables(pos_ids, head_dim):
    half_dim = head_dim // 2
    inv_freq = ROPE_BASE ** (-2.0 * jnp.arange(half_dim, dtype=jnp.float32) / head_dim)
    angles = pos_ids.astype(jnp.float32)[..., None] * inv_freq
    return jnp.cos(angles)[..., None, :], jnp.sin(angles)[..., None, :]


def rotate(values, cos_t, sin_t):
    half_dim = values.shape[-1] // 2
    first_half = values[..., :half_dim].astype(jnp.float32)
    second_half = values[..., half_dim:].astype(jnp.float32)
    rotated = jnp.concatenate([first_half * cos_t - second_half * sin_t,
                               second_half * cos_t + first_half * sin_t], axis=-1)
    return rotated.astype(jnp.bfloat16)


def norm_forward(values, gain_vec):
    values_f = values.astype(jnp.float32)
    inv_rms = lax.rsqrt(jnp.mean(values_f * values_f, axis=-1, keepdims=True) + NORM_EPS)
    normed = values_f * inv_rms * (1.0 + gain_vec.astype(jnp.float32))
    return normed.astype(jnp.bfloat16), inv_rms


def norm_backward(values, inv_rms, gain_vec, grads):
    values_f = values.astype(jnp.float32)
    grads_f = grads.astype(jnp.float32)
    scaled = grads_f * (1.0 + gain_vec.astype(jnp.float32))
    d_values = inv_rms * scaled - values_f * inv_rms ** 3 * jnp.mean(scaled * values_f, axis=-1, keepdims=True)
    d_gain = jnp.sum(grads_f * values_f * inv_rms, axis=0)
    return d_values, d_gain


def dot(a, b, dims):
    return lax.dot_general(a, b, ((dims[:1], dims[1:]), ((), ())), preferred_element_type=jnp.float32)


def solution(mesh):
    tok_spec = P('fsdp', 'cp', None)
    ids_spec = P('fsdp', 'cp')
    in_spec = P('fsdp', None, None)
    out_spec = P(None, None, 'fsdp')
    gain_spec = P('fsdp')
    bf, f32 = jnp.bfloat16, jnp.float32

    def layer_local(hidden, doc_ids, doc_pos, grad_out, w_query, w_key, w_value, w_out, gain_pre, gain_post):
        _, n_tok, model_dim = hidden.shape
        hidden, grad_out = hidden[0], grad_out[0]
        n_heads, head_dim = w_query.shape[1], w_query.shape[2]
        rows = w_query.shape[0]
        q_cols = n_heads * head_dim
        core = lax.axis_index('cp')
        w0 = jnp.concatenate([w_query.reshape(rows, q_cols), w_key.reshape(rows, head_dim),
                              w_value.reshape(rows, head_dim)], axis=1)
        w1 = w_out.reshape(q_cols, rows).T
        lane = lax.rem(lax.axis_index('fsdp'), SIDE) * rows
        w2 = jnp.zeros((16, 256), f32)
        for kind, g in enumerate((gain_pre, gain_post)):
            w2 = lax.dynamic_update_slice(w2, g.astype(f32)[None], (0, kind * 128 + lane))
        cos_t, sin_t = rope_tables(doc_pos[0], head_dim)
        q_scale = (head_dim if head_dim >= 256 else model_dim // n_heads) ** -0.5
        ratio = q_scale / SOFT_CAP
        wqkv, wo_t, gains, normed, inv_pre, q_flat, kv_all, attn_flat, inv_sum = forward(
            hidden, cos_t[:, 0], sin_t[:, 0], doc_pos, w0, w1, w2, n_heads, ratio)
        pre_full, post_full = gains[0], gains[1]
        wqkv = wqkv.reshape(model_dim, q_cols + 2 * head_dim)
        wo_t = wo_t.reshape(model_dim, q_cols)
        swap = [(0, 1), (1, 0)]
        proj_out = dot(attn_flat, wo_t, (1, 1)).astype(bf)
        post_out, inv_post = norm_forward(proj_out, post_full)
        out_hidden = (hidden.astype(f32) + post_out.astype(f32)).astype(bf)

        d_proj, d_gain_post = norm_backward(proj_out, inv_post, post_full, grad_out)
        d_proj = d_proj.astype(bf)
        d_attn = dot(d_proj, wo_t, (1, 0)).astype(bf)

        d_q_flat, d_k, d_v, *accs = attend_back(q_flat, d_attn, kv_all, doc_pos, inv_sum, d_proj, attn_flat, ratio)
        d_kv = jnp.concatenate([d_k, d_v], axis=1)
        d_kv = (d_kv[n_tok:].astype(f32) + lax.ppermute(d_kv[:n_tok], 'cp', swap).astype(f32)).astype(bf)
        d_k_rot, d_v_proj = d_kv[:, :head_dim], d_kv[:, head_dim:]
        d_q_rot = d_q_flat.reshape(n_tok, n_heads, head_dim)
        d_q_proj = rotate(d_q_rot, cos_t, -sin_t)
        d_k_proj = rotate(d_k_rot[:, None], cos_t, -sin_t)[:, 0]
        d_qkv = jnp.concatenate([d_q_proj.reshape(n_tok, q_cols), d_k_proj, d_v_proj], axis=1)

        d_normed = dot(d_qkv, wqkv, (1, 1)).astype(bf)
        d_hidden, d_gain_pre = norm_backward(hidden, inv_pre, pre_full, d_normed)
        grad_hidden = (grad_out.astype(f32) + d_hidden).astype(bf)
        d_gains = jnp.stack([d_gain_pre, d_gain_post]).reshape(2, model_dim // rows, 1, rows)
        d_gains = jnp.pad(d_gains, ((0, 0), (0, 0), (0, 15), (0, 128 - rows)))
        own_g = lax.dynamic_index_in_dim(d_gains, core, 0, keepdims=False)
        sib_g = lax.dynamic_index_in_dim(d_gains, 1 - core, 0, keepdims=False)
        g0, g1, gg = scatter_grads(normed, d_qkv, own_g, sib_g, accs)
        g0 = jnp.concatenate([g0[0], g0[1]], axis=1)
        g1 = jnp.concatenate([g1[0], g1[1]], axis=1)
        return (out_hidden[None], grad_hidden[None], g0[:, :q_cols].reshape(rows, n_heads, head_dim),
                g0[:, q_cols:q_cols + head_dim].reshape(rows, 1, head_dim),
                g0[:, q_cols + head_dim:].reshape(rows, 1, head_dim),
                g1.T.reshape(n_heads, head_dim, rows), gg[0, 0, :rows], gg[1, 0, :rows])

    return jax.shard_map(layer_local, mesh=mesh,
                         in_specs=(tok_spec, ids_spec, ids_spec, tok_spec, in_spec, in_spec, in_spec, out_spec, gain_spec, gain_spec),
                         out_specs=(tok_spec, tok_spec, in_spec, in_spec, in_spec, out_spec, gain_spec, gain_spec),
                         check_vma=False)
```

```python
import functools

import jax
import jax.numpy as jnp
from jax import lax
from jax.experimental import pallas as pl
from jax.experimental.pallas import tpu as pltpu
from jax.sharding import PartitionSpec as P

SOFT_CAP = 50.0
NORM_EPS = 1e-6
ROPE_BASE = 10000.0
MESH = pl.DeviceIdType.MESH
SIDE = 4
VMEM_MAX = 67_043_328

QKV_IN = ((0, 0, 256), (1, 512, 256), (2, 896, 256), (0, 256, 256), (1, 768, 128), (2, 1152, 128))
QKV = ((0, 0, 256), (0, 256, 256), (1, 512, 256), (1, 768, 128), (2, 896, 256), (2, 1152, 128))
OUT = ((0, 0, 256), (1, 256, 384), (2, 640, 384))
GAIN = ((0, 0, 128),)
CHUNK = 256


def place():
    f = lax.axis_index('fsdp')
    return (f // 16, lax.rem(f // 4, 4), lax.rem(f, 4)), lax.axis_index('cp')


def shifted(coords, dim, delta):
    out = list(coords)
    out[dim] = lax.rem(coords[dim] + delta + SIDE, SIDE)
    return tuple(out)


def device(coords, core):
    return (coords[0] * 16 + coords[1] * 4 + coords[2], core)


def greet(coords, core, steps=(1, -1)):
    barrier = pltpu.get_barrier_semaphore()
    for dim in range(3):
        for delta in steps:
            pl.semaphore_signal(barrier, inc=1, device_id=device(shifted(coords, dim, delta), core), device_id_type=MESH)
    pl.semaphore_signal(barrier, inc=1, device_id=device(coords, 1 - core), device_id_type=MESH)
    pl.semaphore_wait(barrier, 3 * len(steps) + 1)


def order_of(colour):
    return tuple((colour + i) % 3 for i in range(3))


def region(ref, full, coords, rows, cols):
    idx = [pl.ds(0, SIDE) if d in full else coords[d] for d in range(3)]
    return ref.at[idx[0], idx[1], idx[2], pl.ds(*rows), pl.ds(*cols)]


class Gather:
    def __init__(self, streams, src, out, direct, send, recv, sib_send, sib_recv):
        self.streams, self.src, self.out, self.direct = streams, src, out, direct
        self.sems = (send, recv, sib_send, sib_recv)
        self.coords, self.core = place()
        self.rows = out.shape[3]

    def cols(self, s, side):
        _, off, width = self.streams[s]
        return pl.ds(pl.multiple_of(side * (self.out.shape[4] // 2) + off, 128), width)

    def part(self, s, p, kind, at, side):
        full = order_of(self.streams[s][0])[:p]
        idx = [pl.ds(0, SIDE) if d in full else at[d] for d in range(3)]
        half = self.rows // 2
        r0, nr = (0, self.rows) if kind < 2 or p in self.direct else ((kind - 2) * half, half)
        return self.out.at[idx[0], idx[1], idx[2], pl.ds(r0, nr), self.cols(s, side)]

    def hop(self, s, p, kind):
        dim = order_of(self.streams[s][0])[p]
        direct = p in self.direct
        at = shifted(self.coords, dim, 0 if direct else (0, 0, -1, 1)[kind])
        to = shifted(self.coords, dim, (1, -1, 2 if direct else 1, -1)[kind])
        dst = self.part(s, p, kind, at, self.core)
        src = self.src.at[:, self.cols(s, self.core)] if p == 0 and (direct or kind < 2) else dst
        return pltpu.make_async_remote_copy(src, dst, self.sems[0].at[s, p, kind], self.sems[1].at[s, p, kind],
                                            device_id=device(to, self.core), device_id_type=MESH)

    def landed(self, s, p, kind, side):
        dim = order_of(self.streams[s][0])[p]
        return self.part(s, p, kind, shifted(self.coords, dim, (-1, 1, -2, 2)[kind]), side)

    def gift(self, s, p, kind, side):
        here = self.landed(s, p, kind, side)
        return pltpu.make_async_remote_copy(here, here, self.sems[2].at[s, p, kind], self.sems[3].at[s, p, kind],
                                            device_id=device(self.coords, 1 - self.core), device_id_type=MESH)

    def arrive(self, s, p, kind):
        here = self.landed(s, p, kind, self.core)
        pltpu.make_async_remote_copy(here, here, self.sems[0].at[s, p, kind], self.sems[1].at[s, p, kind],
                                     device_id=device(self.coords, 1 - self.core), device_id_type=MESH).wait_recv()

    def start(self, s, p):
        self.hop(s, p, 0).start()
        self.hop(s, p, 1).start()
        if p in self.direct:
            self.hop(s, p, 2).start()

    def middle(self, s, p):
        if p in self.direct:
            for kind in range(3):
                self.arrive(s, p, kind)
                self.gift(s, p, kind, self.core).start()
            return
        for kind in (0, 1):
            self.arrive(s, p, kind)
            self.hop(s, p, kind + 2).start()
            self.gift(s, p, kind, self.core).start()

    def finish(self, s, p):
        for kind in () if p in self.direct else (2, 3):
            self.arrive(s, p, kind)
            self.gift(s, p, kind, self.core).start()

    def drain(self, s, p):
        for kind in range(3 if p in self.direct else 4):
            self.hop(s, p, kind).wait_send()
            self.gift(s, p, kind, self.core).wait_send()
            self.gift(s, p, kind, 1 - self.core).wait_recv()


class Scatter:
    def __init__(self, streams, own, sib, acc, sbuf, rbuf, send, recv):
        self.streams, self.own, self.sib = streams, own, sib
        self.acc, self.sbuf, self.rbuf, self.sems = acc, sbuf, rbuf, (send, recv)
        self.coords, self.core = place()

    def half(self, s):
        return self.acc[s][0].shape[1] // 2

    def dim(self, s, q):
        return order_of(self.streams[s][0])[2 - q]

    def value(self, s, q, at, n, r0):
        colour, off, width = self.streams[s]
        order = order_of(colour)
        nr = self.half(s)
        idx = list(at)
        full = sorted(order[:2 - q])
        for d, digit in zip(full, (n // SIDE, lax.rem(n, SIDE)) if len(full) == 2 else (n,)):
            idx[d] = digit
        if q == 0:
            where = (idx[0] * 16 + idx[1] * 4 + idx[2], pl.ds(r0, nr), pl.ds(off, width))
            return self.own[where] + self.sib[where].astype(jnp.float32)
        m = 0
        for d in sorted(order[:3 - q]):
            m = m * SIDE + idx[d]
        return self.acc[s][q - 1][m, pl.ds(r0, nr), :]

    def hop(self, s, q, kind):
        lo, n = ((0, 2), (2, 2), (4, 1), (5, 1))[kind]
        to = shifted(self.coords, self.dim(s, q), (1, -1, 1, -1)[kind])
        return pltpu.make_async_remote_copy(
            self.sbuf[s][q].at[pl.ds(lo, n)], self.rbuf[s][q].at[pl.ds(lo, n)],
            self.sems[0].at[s, q, kind], self.sems[1].at[s, q, kind],
            device_id=device(to, self.core), device_id_type=MESH)

    def each(self, q, body):
        n = SIDE ** (2 - q)

        def step(i, carry):
            body(i)
            return carry
        lax.fori_loop(0, n, step, 0, unroll=min(n, 2))

    def one(self, s, q):
        dim, half, buf = self.dim(s, q), self.half(s), self.sbuf[s][q]
        far, right, left = (shifted(self.coords, dim, d) for d in (2, 1, -1))

        def to_right(n):
            buf[0, n] = self.value(s, q, far, n, 0).astype(buf.dtype)
            buf[1, n] = self.value(s, q, right, n, half).astype(buf.dtype)

        def to_left(n):
            buf[2, n] = self.value(s, q, far, n, half).astype(buf.dtype)
            buf[3, n] = self.value(s, q, left, n, 0).astype(buf.dtype)
        self.each(q, to_right)
        self.hop(s, q, 0).start()
        self.each(q, to_left)
        self.hop(s, q, 1).start()

    def two(self, s, q):
        dim, half, buf, got = self.dim(s, q), self.half(s), self.sbuf[s][q], self.rbuf[s][q]
        right, left = (shifted(self.coords, dim, d) for d in (1, -1))

        def to_right(n):
            buf[4, n] = (self.value(s, q, right, n, 0) + got[0, n].astype(jnp.float32)).astype(buf.dtype)

        def to_left(n):
            buf[5, n] = (self.value(s, q, left, n, half) + got[2, n].astype(jnp.float32)).astype(buf.dtype)
        self.hop(s, q, 0).wait_recv()
        self.each(q, to_right)
        self.hop(s, q, 2).start()
        self.hop(s, q, 1).wait_recv()
        self.each(q, to_left)
        self.hop(s, q, 3).start()

    def three(self, s, q):
        half, got, acc = self.half(s), self.rbuf[s][q], self.acc[s][q]
        self.hop(s, q, 2).wait_recv()
        self.hop(s, q, 3).wait_recv()

        def keep(n):
            for r0, i, j in ((0, 3, 4), (half, 1, 5)):
                acc[n, pl.ds(r0, half), :] = (self.value(s, q, self.coords, n, r0) + got[i, n].astype(jnp.float32)
                                              + got[j, n].astype(jnp.float32))
        self.each(q, keep)

    def drain(self, s, q):
        for kind in range(4):
            self.hop(s, q, kind).wait_send()


def transpose_into(dst, src):
    def strip(j, carry):
        at = pl.ds(pl.multiple_of(j * CHUNK, CHUNK), CHUNK)
        dst[at, :] = src[:, at].T
        return carry
    lax.fori_loop(0, src.shape[1] // CHUNK, strip, 0)


def grad_chunk(grads_t, acts, dst, side, j):
    half = dst.shape[2]
    rhs = acts[:, pl.ds(pl.multiple_of(side * half + j * CHUNK, CHUNK), CHUNK)]
    n_rows = 512

    def strip(i, carry):
        at = pl.multiple_of(i * n_rows, n_rows)
        out = nn(grads_t[pl.ds(at, n_rows), :], rhs).astype(dst.dtype)
        dst[pl.ds(i * (n_rows // 32), n_rows // 32), :, pl.ds(j * CHUNK, CHUNK)] = out.reshape(n_rows // 32, 32, CHUNK)
        return carry
    lax.fori_loop(0, grads_t.shape[0] // n_rows, strip, 0)


def chunk_gift(src, dst, send, recv, j):
    coords, core = place()
    at = pl.ds(j * CHUNK, CHUNK)
    return pltpu.make_async_remote_copy(src.at[:, :, at], dst.at[:, :, at], send.at[j], recv.at[j],
                                        device_id=device(coords, 1 - core), device_id_type=MESH)


def wire_shapes(streams, dtype, rows, phases):
    return [pltpu.VMEM((6, SIDE ** (2 - q), rows // 2, width), dtype) for _, _, width in streams for q in phases]


def acc_shapes(streams, rows, phases):
    return [((SIDE ** (2 - q), rows, width), jnp.float32) for _, _, width in streams for q in phases]


def scatter_kernel(normed, d_qkv, w_ref, x_ref, dy_ref, inv_rms, gain, post_row, acc_o0, acc_o1, acc_o2,
                   dx_ref, grad_q, grad_k, grad_v, grad_o, out_g, *scratch):
    scratch = list(scratch)

    def take(n):
        head = scratch[:n]
        del scratch[:n]
        return head
    normed_t, own_q, sib_out, sib_q, own_g, sib_g, sib_in_g, out_q, out_o, w_buf, dn, pre_row = take(12)
    nq = len(QKV)
    acc_q, sbuf_q, rbuf_q = take(3 * nq), take(3 * nq), take(3 * nq)
    acc_o, sbuf_o, rbuf_o = take(6), take(6), take(6)
    acc_g, sbuf_g, rbuf_g = take(3), take(3), take(3)
    sems = take(6)
    gift_send, gift_recv, gain_sem, fin_send, fin_recv, w_sem = take(6)
    bf, f32 = jnp.bfloat16, jnp.float32
    n_tok, dim = x_ref.shape
    strips = dim // CHUNK
    coords, core = place()
    sibling = device(coords, 1 - core)
    greet(coords, core)

    def triples(flat):
        return [flat[3 * s:3 * s + 3] for s in range(len(flat) // 3)]

    def tails(flat, heads):
        return [[heads[s]] + flat[2 * s:2 * s + 2] for s in range(3)]
    qkv = Scatter(QKV, own_q, sib_q, triples(acc_q), triples(sbuf_q), triples(rbuf_q), *sems[0:2])
    out = Scatter(OUT, None, None, tails(acc_o, (acc_o0, acc_o1, acc_o2)), tails(sbuf_o, (None,) * 3),
                  tails(rbuf_o, (None,) * 3), *sems[2:4])
    gains = Scatter(GAIN, own_g, sib_in_g, triples(acc_g), triples(sbuf_g), triples(rbuf_g), *sems[4:6])
    gain_gift = pltpu.make_async_remote_copy(sib_g, sib_in_g, gain_sem.at[0], gain_sem.at[1],
                                             device_id=sibling, device_id_type=MESH)
    loads = [pltpu.make_async_copy(w_ref.at[pl.ds(8 * j, 8)], w_buf.at[j % 2], w_sem.at[j]) for j in range(strips)]
    loads[0].start()
    loads[1].start()
    for s in range(3):
        out.one(s, 1)
    own_g[...] = jnp.zeros_like(own_g)
    sib_g[...] = jnp.zeros_like(sib_g)
    transpose_into(normed_t, normed)
    chunks = own_q.shape[2] // CHUNK
    gifts = [chunk_gift(sib_out, sib_q, gift_send, gift_recv, j) for j in range(chunks)]
    for j in range(chunks):
        grad_chunk(normed_t, d_qkv, sib_out, 1 - core, j)
        gifts[j].start()
    for s in range(3):
        out.two(s, 1)
    done = 0
    for s, (_, off, width) in enumerate(QKV):
        while done * CHUNK < off + width:
            grad_chunk(normed_t, d_qkv, own_q, core, done)
            gifts[done].wait_recv()
            done += 1
        qkv.one(s, 0)
        if s == 0:
            for i in range(3):
                out.three(i, 1)
                out.one(i, 2)
    for j in range(strips):
        loads[j].wait()
        dn[:, pl.ds(j * CHUNK, CHUNK)] = nt(d_qkv[...], w_buf[j % 2].reshape(CHUNK, d_qkv.shape[1])).astype(bf)
        if j + 2 < strips:
            loads[j + 2].start()
    work = [(qkv, s) for s in range(nq)]
    for s in range(3):
        out.two(s, 2)
    for scatter, s in work:
        scatter.two(s, 0)
    pre_row[...] = jnp.zeros_like(pre_row)
    one_gain = 1.0 + gain[pl.ds(0, 1), :]

    def back(i, carry):
        at = pl.ds(i * 32, 32)
        xs, g, inv = x_ref[at, :].astype(f32), dn[at, :].astype(f32), inv_rms[at, :]
        scaled = g * one_gain
        mean = jnp.sum(scaled * xs, axis=1, keepdims=True) * (1.0 / dim)
        dx_ref[at, :] = (dy_ref[at, :].astype(f32) + (inv * scaled - xs * (inv * inv * inv * mean))).astype(bf)
        pre_row[...] += jnp.sum((g * (xs * inv)).reshape(4, 8, dim), axis=0)
        return carry
    lax.fori_loop(0, n_tok // 32, back, 0)
    pre, post = jnp.sum(pre_row[...], axis=0, keepdims=True), post_row[...]
    own_row, sib_row = jnp.where(core == 0, pre, post), jnp.where(core == 0, post, pre)
    for j in range(16):
        for x in range(SIDE):
            own_g[SIDE * j + x, pl.ds(0, 1), :] = own_row[:, j * 128:(j + 1) * 128]
            sib_g[SIDE * j + x, pl.ds(0, 1), :] = sib_row[:, j * 128:(j + 1) * 128]
    gain_gift.start()
    for scatter, s in work:
        scatter.three(s, 0)
        scatter.one(s, 1)
    for s in range(3):
        out.three(s, 2)
    gain_gift.wait_recv()
    gains.one(0, 0)
    work = work + [(gains, 0)]
    for q in range(3):
        for scatter, s in work:
            if q > 0 or scatter is gains:
                scatter.two(s, q)
        for scatter, s in work:
            if q == 0 and scatter is not gains:
                continue
            scatter.three(s, q)
            if q < 2:
                scatter.one(s, q + 1)
    fins = []
    k = 0
    for scatter, ref in ((qkv, out_q), (out, out_o), (gains, out_g)):
        for s, (_, off, width) in enumerate(scatter.streams):
            part = scatter.acc[s][2].at[0]
            ref[core, :, pl.ds(off, width)] = scatter.acc[s][2][0]
            here, there = (ref.at[side, :, pl.ds(off, width)] for side in (core, 1 - core))
            pair = [pltpu.make_async_remote_copy(part, side, fin_send.at[k], fin_recv.at[k],
                                                 device_id=sibling, device_id_type=MESH) for side in (here, there)]
            pair[0].start()
            fins.append(pair)
            k += 1
    for mine, theirs in fins:
        mine.wait_send()
        theirs.wait_recv()
    n_heads = grad_q.shape[1]
    per = out_q.shape[2] // TILE
    for h in range(n_heads + 2):
        part = out_q[h // per, :, pl.ds(h % per * TILE, TILE)]
        if h < n_heads:
            grad_q[:, h, :] = part
        else:
            (grad_k, grad_v)[h - n_heads][...] = part
    for side in range(2):
        grad_o[pl.ds(side * out_o.shape[2], out_o.shape[2]), :] = out_o[side].T
    for copy in gifts + [gain_gift]:
        copy.wait_send()
    for scatter, phases in ((qkv, (0, 1, 2)), (out, (1, 2)), (gains, (0, 1, 2))):
        for s in range(len(scatter.streams)):
            for q in phases:
                scatter.drain(s, q)


def scatter_grads(normed, d_qkv, w, x, dy, inv_rms, gain, post_row, accs, n_heads):
    bf, f32 = jnp.bfloat16, jnp.float32
    n_tok, model_dim = normed.shape
    half, rows = d_qkv.shape[1] // 2, 32
    blocks = model_dim // rows
    dma = pltpu.SemaphoreType.DMA
    vmem = pl.BlockSpec(memory_space=pltpu.VMEM)
    scratch = [pltpu.VMEM((model_dim, n_tok), bf), pltpu.VMEM((blocks, rows, half), f32),
               pltpu.VMEM((blocks, rows, half), bf), pltpu.VMEM((blocks, rows, half), bf)]
    scratch += [pltpu.VMEM((blocks, 16, 128), f32)] * 3
    scratch += [pltpu.VMEM((2, rows, half), f32), pltpu.VMEM((2, rows, 1024), f32),
                pltpu.VMEM((2, CHUNK // rows, rows, 2 * half), bf), pltpu.VMEM((n_tok, model_dim), bf),
                pltpu.VMEM((8, model_dim), f32)]
    for streams, dtype, n_rows, phases in ((QKV, bf, rows, (0, 1, 2)), (OUT, bf, rows, (1, 2)), (GAIN, f32, 16, (0, 1, 2))):
        scratch += [pltpu.VMEM(*a) for a in acc_shapes(streams, n_rows, phases)]
        scratch += wire_shapes(streams, dtype, n_rows, phases) * 2
    scratch += [dma((len(st), 3, 4)) for st in (QKV, OUT, GAIN) for _ in range(2)]
    scratch += [dma((half // CHUNK,))] * 2 + [dma((2,))] + [dma((len(QKV) + 4,))] * 2 + [dma((model_dim // CHUNK,))]
    return pl.pallas_call(
        scatter_kernel, name="scatter_grads",
        out_shape=[jax.ShapeDtypeStruct((n_tok, model_dim), bf), jax.ShapeDtypeStruct((rows, n_heads, TILE), f32),
                   jax.ShapeDtypeStruct((rows, TILE), f32), jax.ShapeDtypeStruct((rows, TILE), f32),
                   jax.ShapeDtypeStruct((n_heads * TILE, rows), f32), jax.ShapeDtypeStruct((2, 16, 128), f32)],
        in_specs=[vmem] * 2 + [pl.BlockSpec(memory_space=pltpu.HBM)] + [vmem] * 8, out_specs=[vmem] * 6,
        scratch_shapes=scratch,
        compiler_params=pltpu.CompilerParams(collective_id=2, has_side_effects=True, vmem_limit_bytes=VMEM_MAX),
    )(normed, d_qkv, w, x, dy, inv_rms, gain, post_row, *accs)


LOG2E = 1.4426950408889634
TILE = 256


def nt(a, b):
    return lax.dot_general(a, b, (((1,), (1,)), ((), ())), preferred_element_type=jnp.float32)


def nn(a, b):
    return lax.dot_general(a, b, (((1,), (0,)), ((), ())), preferred_element_type=jnp.float32)


def fill_mask(mask, pos):
    n_keys, n_q = mask.shape
    core = lax.axis_index('cp')
    for c in range(n_keys // TILE):
        base = jnp.where(c < n_q // TILE, (1 - core) * n_q, core * n_q - n_q) + c * TILE
        for i in range(n_q // TILE):
            k_at = base + lax.broadcasted_iota(jnp.int32, (TILE, TILE), 0)
            q_at = core * n_q + i * TILE + lax.broadcasted_iota(jnp.int32, (TILE, TILE), 1)
            seen = (k_at <= q_at) & (k_at >= q_at - pos[:, pl.ds(i * TILE, TILE)])
            mask[pl.ds(c * TILE, TILE), pl.ds(i * TILE, TILE)] = jnp.where(seen, 1.0, 0.0)


def keys_for(i, n_q):
    return n_q + (i + 1) * TILE


def forward_kernel(ratio, x_ref, cos_ref, sin_ref, pos, in0, in1, in2,
                   wq_out, wo_out, gain_out, normed, inv_rms, q_ref, kv_ref, o_ref, inv_ref,
                   wq, gains, gain_row, mask, v_t, w_scr, p_scr, *sems):
    n_q, dim = x_ref.shape
    bf, f32 = jnp.bfloat16, jnp.float32
    coords, core = place()
    sibling = device(coords, 1 - core)
    greet(coords, core, (1, -1, 2))
    own_sem, swap_send, swap_recv = sems[12:15]
    qkv, out, gain = (Gather(st, src, dst, direct, *sems[4 * g:4 * g + 4]) for g, (st, src, dst, direct) in enumerate(
        ((QKV_IN, in0, wq, (0,)), (OUT, in1, wo_out, (0,)), (GAIN, in2, gains, (0, 1, 2)))))
    nq = range(len(QKV_IN))
    gain.start(0, 0)
    for s in nq:
        qkv.start(s, 0)
    for s in range(3):
        out.start(s, 0)
    own_out = pltpu.make_async_copy(in1, wo_out.at[coords[0], coords[1], coords[2]], own_sem.at[0])
    own_out.start()
    wq[coords[0], coords[1], coords[2]] = in0[...]
    gains[coords[0], coords[1], coords[2]] = in2[...]

    def stats(i, carry):
        at = pl.ds(i * 64, 64)
        v = x_ref[at, :].astype(f32)
        inv_rms[at, :] = lax.rsqrt(jnp.sum(v * v, axis=1, keepdims=True) * (1.0 / dim) + NORM_EPS)
        return carry
    lax.fori_loop(0, n_q // 64, stats, 0)
    gain.middle(0, 0)
    gain.start(0, 1)
    for s in nq:
        qkv.middle(s, 0)
        qkv.start(s, 1)
    gain.middle(0, 1)
    gain.start(0, 2)
    for s in range(3):
        out.middle(s, 0)
    own_out.wait()
    for s in nq:
        qkv.middle(s, 1)
    for s in range(3):
        out.start(s, 1)
    gain.middle(0, 2)
    for s in nq:
        qkv.finish(s, 1)
        qkv.start(s, 2)
    for p in range(3):
        gain.drain(0, p)
    for kind in range(2):
        for j in range(16):
            row = sum(gains[j // 4, j % 4, x, pl.ds(0, 1), pl.ds(kind * 128, 128)] for x in range(SIDE))
            gain_row[pl.ds(kind, 1), pl.ds(j * 128, 128)] = row
    gain_out[...] = gain_row[...]
    fill_mask(mask, pos)

    def scale(i, carry):
        at = pl.ds(i * 64, 64)
        normed[at, :] = (x_ref[at, :].astype(f32) * inv_rms[at, :] * (1.0 + gain_row[pl.ds(0, 1), :])).astype(bf)
        return carry
    lax.fori_loop(0, n_q // 64, scale, 0)
    for s in nq:
        qkv.middle(s, 2)
    for s in range(3):
        out.middle(s, 1)
    for s in nq:
        qkv.finish(s, 2)
    for s in range(3):
        out.finish(s, 1)
        out.start(s, 2)
    for s in nq:
        for p in range(3):
            qkv.drain(s, p)
    keep = pltpu.make_async_copy(wq, wq_out, own_sem.at[1])
    keep.start()

    def project(n):
        rhs = wq[:, :, :, :, pl.ds(pl.multiple_of(n * TILE, TILE), TILE)].reshape(dim, TILE)
        return nn(normed[...], rhs).astype(bf)

    def rope(u):
        lo, hi = u[:, :TILE // 2].astype(f32), u[:, TILE // 2:].astype(f32)
        c, s = cos_ref[...], sin_ref[...]
        return jnp.concatenate([lo * c - hi * s, hi * c + lo * s], axis=1).astype(bf)
    n_heads = q_ref.shape[1] // TILE
    mine, other = pl.ds(n_q, n_q), pl.ds(0, n_q)
    kv_ref[mine, pl.ds(0, TILE)] = rope(project(n_heads))
    kv_ref[mine, pl.ds(TILE, TILE)] = project(n_heads + 1)
    swap = pltpu.make_async_remote_copy(kv_ref.at[mine], kv_ref.at[other], swap_send.at[0], swap_recv.at[0],
                                        device_id=sibling, device_id_type=MESH)
    swap.start()

    def project_head(h, carry):
        q_ref[:, pl.ds(pl.multiple_of(h * TILE, TILE), TILE)] = rope(project(h))
        return carry
    lax.fori_loop(0, n_heads, project_head, 0)
    for s in range(3):
        out.middle(s, 2)
    swap.wait_recv()
    k_cols = pl.ds(0, TILE)
    v_t[...] = kv_ref[:, pl.ds(TILE, TILE)].T

    def head(h, carry):
        cols = pl.ds(pl.multiple_of(h * TILE, TILE), TILE)
        for i in range(n_q // TILE):
            qi = q_ref[pl.ds(i * TILE, TILE), cols]
            n_keys = keys_for(i, n_q)
            total = jnp.zeros((8, TILE), f32)
            for c in range(n_keys // TILE):
                t = jnp.tanh(nt(kv_ref[pl.ds(c * TILE, TILE), k_cols], qi) * ratio)
                w = jnp.exp2(t * (SOFT_CAP * LOG2E)) * mask[pl.ds(c * TILE, TILE), pl.ds(i * TILE, TILE)]
                w_scr[i, pl.ds(c * TILE, TILE), :] = w
                total = total + jnp.sum(w.reshape(TILE // 8, 8, TILE), axis=0)
            inv = 1.0 / jnp.sum(total, axis=0, keepdims=True)
            inv_ref[h, :, pl.ds(i * TILE, TILE)] = inv
            p_scr[i, pl.ds(0, n_keys), :] = (w_scr[i, pl.ds(0, n_keys), :] * inv).astype(bf)
            o_t = nn(v_t[:, pl.ds(0, n_keys)], p_scr[i, pl.ds(0, n_keys), :])
            o_ref[pl.ds(i * TILE, TILE), cols] = o_t.T.astype(bf)
        return carry
    lax.fori_loop(0, n_heads, head, 0)
    for s in range(3):
        out.finish(s, 2)
    for s in range(3):
        for p in range(3):
            out.drain(s, p)
    swap.wait_send()
    keep.wait()


def forward(x, cos_t, sin_t, pos, w0, w1, w2, n_heads, ratio):
    n_q, dim = x.shape
    n_k = 2 * n_q
    bf, f32 = jnp.bfloat16, jnp.float32
    dma = pltpu.SemaphoreType.DMA
    vmem, hbm = pl.BlockSpec(memory_space=pltpu.VMEM), pl.BlockSpec(memory_space=pltpu.HBM)
    grid = (SIDE, SIDE, SIDE)
    shape = jax.ShapeDtypeStruct
    tiles = n_q // TILE
    return pl.pallas_call(
        functools.partial(forward_kernel, ratio), name="forward",
        out_shape=[shape(grid + w0.shape, bf), shape(grid + w1.shape, bf), shape((2, dim), f32), shape((n_q, dim), bf),
                   shape((n_q, 1), f32), shape((n_q, n_heads * TILE), bf), shape((n_k, 2 * TILE), bf),
                   shape((n_q, n_heads * TILE), bf), shape((n_heads, 1, n_q), f32)],
        in_specs=[vmem] * 7, out_specs=[hbm] * 2 + [vmem] * 7,
        scratch_shapes=[pltpu.VMEM(grid + w0.shape, bf), pltpu.VMEM(grid + w2.shape, f32), pltpu.VMEM((2, dim), f32),
                        pltpu.VMEM((n_k, n_q), f32), pltpu.VMEM((TILE, n_k), bf),
                        pltpu.VMEM((tiles, n_k, TILE), f32), pltpu.VMEM((tiles, n_k, TILE), bf)]
        + [dma((len(st), 3, 4)) for st in (QKV_IN, OUT, GAIN) for _ in range(4)]
        + [dma((2,)), dma((1,)), dma((1,))],
        compiler_params=pltpu.CompilerParams(collective_id=1, has_side_effects=True, vmem_limit_bytes=VMEM_MAX),
    )(x, cos_t, sin_t, pos, w0, w1, w2)


def attend_back_kernel(ratio, q_ref, do_ref, kv_ref, pos, inv_ref, dz_ref, o_ref, cos_ref, sin_ref,
                       dqkv_ref, acc0, acc1, acc2,
                       mask, k_t, g_scr, dp_scr, p_scr, ds_scr, dk_acc, dv_acc, dkv_out, dkv_in, dz_t, own, sib_out, sib_in,
                       *scratch):
    n_q = q_ref.shape[0]
    coords, core = place()
    greet(coords, core)
    sbuf, rbuf, sems = scratch[0:3], scratch[3:6], scratch[6:8]
    gift_send, gift_recv, swap_sem = scratch[8:11]
    bf, f32 = jnp.bfloat16, jnp.float32
    swap = pltpu.make_async_remote_copy(dkv_out, dkv_in, swap_sem.at[0], swap_sem.at[1],
                                        device_id=device(coords, 1 - core), device_id_type=MESH)

    def rope_back(u):
        lo, hi = u[:, :TILE // 2].astype(f32), u[:, TILE // 2:].astype(f32)
        c, s = cos_ref[pl.ds(0, u.shape[0]), :], sin_ref[pl.ds(0, u.shape[0]), :]
        return jnp.concatenate([lo * c + hi * s, hi * c - lo * s], axis=1).astype(bf)
    out = Scatter(OUT, own, sib_in, [[a] for a in (acc0, acc1, acc2)], [[b] for b in sbuf], [[b] for b in rbuf], *sems)
    chunks = own.shape[2] // CHUNK
    transpose_into(dz_t, dz_ref)
    gifts = [chunk_gift(sib_out, sib_in, gift_send, gift_recv, j) for j in range(chunks)]
    for j in range(chunks):
        grad_chunk(dz_t, o_ref, sib_out, 1 - core, j)
        gifts[j].start()
    done = 0
    for s, (_, off, width) in enumerate(OUT):
        while done * CHUNK < off + width:
            grad_chunk(dz_t, o_ref, own, core, done)
            gifts[done].wait_recv()
            done += 1
        out.one(s, 0)
    fill_mask(mask, pos)
    k_cols, v_cols = pl.ds(0, TILE), pl.ds(TILE, TILE)
    k_t[...] = kv_ref[:, k_cols].T
    dk_acc[...] = jnp.zeros_like(dk_acc)
    dv_acc[...] = jnp.zeros_like(dv_acc)

    def head(h, carry):
        cols = pl.ds(pl.multiple_of(h * TILE, TILE), TILE)
        for i in range(n_q // TILE):
            rows = pl.ds(i * TILE, TILE)
            qi, doi = q_ref[rows, cols], do_ref[rows, cols]
            inv = inv_ref[h, :, rows]
            n_keys = keys_for(i, n_q)
            total = jnp.zeros((8, TILE), jnp.float32)
            for c in range(n_keys // TILE):
                at = pl.ds(c * TILE, TILE)
                t = jnp.tanh(nt(kv_ref[at, k_cols], qi) * ratio)
                p = jnp.exp2(t * (SOFT_CAP * LOG2E)) * (mask[at, rows] * inv)
                dp = nt(kv_ref[at, v_cols], doi)
                p_scr[i, at, :] = p.astype(jnp.bfloat16)
                g_scr[i, at, :] = p * ((1.0 - t * t) * (ratio * SOFT_CAP))
                dp_scr[i, at, :] = dp
                total = total + jnp.sum((p * dp).reshape(TILE // 8, 8, TILE), axis=0)
            row_dot = jnp.sum(total, axis=0, keepdims=True)
            seen = pl.ds(0, n_keys)
            ds_scr[i, seen, :] = ((dp_scr[i, seen, :] - row_dot) * g_scr[i, seen, :]).astype(jnp.bfloat16)
            dq_t = nn(k_t[:, seen], ds_scr[i, seen, :])
            dq = dq_t.T.astype(bf)
            lo, hi = dq[:, :TILE // 2].astype(f32), dq[:, TILE // 2:].astype(f32)
            cos, sin = cos_ref[rows, :], sin_ref[rows, :]
            dqkv_ref[rows, cols] = jnp.concatenate([lo * cos + hi * sin, hi * cos - lo * sin], axis=1).astype(bf)
            dk_acc[seen, :] += nn(ds_scr[i, seen, :], qi)
            dv_acc[seen, :] += nn(p_scr[i, seen, :], doi)

        @pl.when(h == 3)
        def _():
            for s in range(3):
                out.two(s, 0)
        return carry
    lax.fori_loop(0, q_ref.shape[1] // TILE, head, 0)
    mine, other = pl.ds(n_q, n_q), pl.ds(0, n_q)
    dkv_out[:, k_cols] = dk_acc[other, :].astype(bf)
    dkv_out[:, v_cols] = dv_acc[other, :].astype(bf)
    swap.start()
    for s in range(3):
        out.three(s, 0)
    swap.wait_recv()
    q_cols = q_ref.shape[1]
    dqkv_ref[:, pl.ds(q_cols, TILE)] = rope_back((dk_acc[mine, :] + dkv_in[:, k_cols].astype(f32)).astype(bf))
    dqkv_ref[:, pl.ds(q_cols + TILE, TILE)] = (dv_acc[mine, :] + dkv_in[:, v_cols].astype(f32)).astype(bf)
    for s in range(3):
        out.drain(s, 0)
    for copy in gifts + [swap]:
        copy.wait_send()


def attend_back(q, do, kv, pos, inv_sum, dz, o, cos_t, sin_t, ratio):
    n_q, n_k = q.shape[0], kv.shape[0]
    vmem = pl.BlockSpec(memory_space=pltpu.VMEM)
    tiles = n_q // TILE
    bf, f32 = jnp.bfloat16, jnp.float32
    return pl.pallas_call(
        functools.partial(attend_back_kernel, ratio), name="attend_back",
        out_shape=[jax.ShapeDtypeStruct((n_q, q.shape[1] + 2 * TILE), bf)]
        + [jax.ShapeDtypeStruct(*a) for a in acc_shapes(OUT, 32, (0,))],
        in_specs=[vmem] * 9, out_specs=[vmem] * 4,
        scratch_shapes=[pltpu.VMEM((n_k, n_q), f32), pltpu.VMEM((TILE, n_k), bf),
                        pltpu.VMEM((tiles, n_k, TILE), f32), pltpu.VMEM((tiles, n_k, TILE), f32),
                        pltpu.VMEM((tiles, n_k, TILE), bf), pltpu.VMEM((tiles, n_k, TILE), bf),
                        pltpu.VMEM((n_k, TILE), f32), pltpu.VMEM((n_k, TILE), f32),
                        pltpu.VMEM((n_q, 2 * TILE), bf), pltpu.VMEM((n_q, 2 * TILE), bf),
                        pltpu.VMEM((dz.shape[1], n_q), bf), pltpu.VMEM((dz.shape[1] // 32, 32, o.shape[1] // 2), f32)]
        + [pltpu.VMEM((dz.shape[1] // 32, 32, o.shape[1] // 2), bf)] * 2
        + wire_shapes(OUT, bf, 32, (0,)) * 2 + [pltpu.SemaphoreType.DMA((3, 3, 4))] * 2
        + [pltpu.SemaphoreType.DMA((o.shape[1] // 2 // CHUNK,))] * 2 + [pltpu.SemaphoreType.DMA((2,))],
        compiler_params=pltpu.CompilerParams(collective_id=4, has_side_effects=True, vmem_limit_bytes=VMEM_MAX),
    )(q, do, kv, pos, inv_sum, dz, o, cos_t, sin_t)


def rope_tables(pos_ids, head_dim):
    half_dim = head_dim // 2
    inv_freq = ROPE_BASE ** (-2.0 * jnp.arange(half_dim, dtype=jnp.float32) / head_dim)
    angles = pos_ids.astype(jnp.float32)[..., None] * inv_freq
    return jnp.cos(angles)[..., None, :], jnp.sin(angles)[..., None, :]


def rotate(values, cos_t, sin_t):
    half_dim = values.shape[-1] // 2
    first_half = values[..., :half_dim].astype(jnp.float32)
    second_half = values[..., half_dim:].astype(jnp.float32)
    rotated = jnp.concatenate([first_half * cos_t - second_half * sin_t,
                               second_half * cos_t + first_half * sin_t], axis=-1)
    return rotated.astype(jnp.bfloat16)


def norm_forward(values, gain_vec):
    values_f = values.astype(jnp.float32)
    inv_rms = lax.rsqrt(jnp.mean(values_f * values_f, axis=-1, keepdims=True) + NORM_EPS)
    normed = values_f * inv_rms * (1.0 + gain_vec.astype(jnp.float32))
    return normed.astype(jnp.bfloat16), inv_rms


def norm_backward(values, inv_rms, gain_vec, grads):
    values_f = values.astype(jnp.float32)
    grads_f = grads.astype(jnp.float32)
    scaled = grads_f * (1.0 + gain_vec.astype(jnp.float32))
    d_values = inv_rms * scaled - values_f * inv_rms ** 3 * jnp.mean(scaled * values_f, axis=-1, keepdims=True)
    d_gain = jnp.sum(grads_f * values_f * inv_rms, axis=0)
    return d_values, d_gain


def dot(a, b, dims):
    return lax.dot_general(a, b, ((dims[:1], dims[1:]), ((), ())), preferred_element_type=jnp.float32)


def solution(mesh):
    tok_spec = P('fsdp', 'cp', None)
    ids_spec = P('fsdp', 'cp')
    in_spec = P('fsdp', None, None)
    out_spec = P(None, None, 'fsdp')
    gain_spec = P('fsdp')
    bf, f32 = jnp.bfloat16, jnp.float32

    def layer_local(hidden, doc_ids, doc_pos, grad_out, w_query, w_key, w_value, w_out, gain_pre, gain_post):
        _, n_tok, model_dim = hidden.shape
        hidden, grad_out = hidden[0], grad_out[0]
        n_heads, head_dim = w_query.shape[1], w_query.shape[2]
        rows = w_query.shape[0]
        q_cols = n_heads * head_dim
        w0 = jnp.concatenate([w_query.reshape(rows, q_cols), w_key.reshape(rows, head_dim),
                              w_value.reshape(rows, head_dim)], axis=1)
        w1 = w_out.reshape(q_cols, rows).T
        lane = lax.rem(lax.axis_index('fsdp'), SIDE) * rows
        w2 = jnp.zeros((8, 256), f32)
        for kind, g in enumerate((gain_pre, gain_post)):
            w2 = lax.dynamic_update_slice(w2, g.astype(f32)[None], (0, kind * 128 + lane))
        cos_t, sin_t = rope_tables(doc_pos[0], head_dim)
        q_scale = (head_dim if head_dim >= 256 else model_dim // n_heads) ** -0.5
        ratio = q_scale / SOFT_CAP
        wqkv, wo_t, gains, normed, inv_pre, q_flat, kv_all, attn_flat, inv_sum = forward(
            hidden, cos_t[:, 0], sin_t[:, 0], doc_pos, w0, w1, w2, n_heads, ratio)
        post_full = gains[1]
        wqkv = wqkv.reshape(model_dim // rows, rows, q_cols + 2 * head_dim)
        wo_t = wo_t.reshape(model_dim, q_cols)
        proj_out = dot(attn_flat, wo_t, (1, 1)).astype(bf)
        post_out, inv_post = norm_forward(proj_out, post_full)
        out_hidden = (hidden.astype(f32) + post_out.astype(f32)).astype(bf)

        d_proj, d_gain_post = norm_backward(proj_out, inv_post, post_full, grad_out)
        d_proj = d_proj.astype(bf)
        d_attn = dot(d_proj, wo_t, (1, 0)).astype(bf)

        d_qkv, *accs = attend_back(q_flat, d_attn, kv_all, doc_pos, inv_sum, d_proj, attn_flat, cos_t[:, 0], sin_t[:, 0], ratio)
        dx, g_q, g_k, g_v, g_o, g_g = scatter_grads(normed, d_qkv, wqkv, hidden, grad_out, inv_pre, gains,
                                                    d_gain_post[None], accs, n_heads)
        g_g = lax.dynamic_slice(g_g, (0, 0, lane), (2, 1, rows))[:, 0]
        return (out_hidden[None], dx[None], g_q, g_k[:, None], g_v[:, None], g_o.reshape(n_heads, head_dim, rows),
                g_g[0], g_g[1])

    return jax.shard_map(layer_local, mesh=mesh,
                         in_specs=(tok_spec, ids_spec, ids_spec, tok_spec, in_spec, in_spec, in_spec, out_spec, gain_spec, gain_spec),
                         out_specs=(tok_spec, tok_spec, in_spec, in_spec, in_spec, out_spec, gain_spec, gain_spec),
                         check_vma=False)
```

```python
import functools

import jax
import jax.numpy as jnp
from jax import lax
from jax.experimental import pallas as pl
from jax.experimental.pallas import tpu as pltpu
from jax.sharding import PartitionSpec as P

SOFT_CAP = 50.0
NORM_EPS = 1e-6
ROPE_BASE = 10000.0
MESH = pl.DeviceIdType.MESH
SIDE = 4
VMEM_MAX = 67_043_328

QKV = ((0, 0, 256), (1, 256, 256), (2, 512, 256), (0, 768, 256), (1, 1024, 128), (2, 1152, 128))
OUT = ((0, 0, 256), (1, 256, 256), (2, 512, 256), (1, 768, 128), (2, 896, 128))
GAIN = ((0, 0, 128),)
CHUNK = 256


def place():
    f = lax.axis_index('fsdp')
    return (f // 16, lax.rem(f // 4, 4), lax.rem(f, 4)), lax.axis_index('cp')


def shifted(coords, dim, delta):
    out = list(coords)
    out[dim] = lax.rem(coords[dim] + delta + SIDE, SIDE)
    return tuple(out)


def device(coords, core):
    return (coords[0] * 16 + coords[1] * 4 + coords[2], core)


def greet(coords, core, steps=(1, -1)):
    barrier = pltpu.get_barrier_semaphore()
    for dim in range(3):
        for delta in steps:
            pl.semaphore_signal(barrier, inc=1, device_id=device(shifted(coords, dim, delta), core), device_id_type=MESH)
    pl.semaphore_signal(barrier, inc=1, device_id=device(coords, 1 - core), device_id_type=MESH)
    pl.semaphore_wait(barrier, 3 * len(steps) + 1)


def order_of(colour):
    return tuple((colour + i) % 3 for i in range(3))


def region(ref, full, coords, rows, cols):
    idx = [pl.ds(0, SIDE) if d in full else coords[d] for d in range(3)]
    return ref.at[idx[0], idx[1], idx[2], pl.ds(*rows), pl.ds(*cols)]


class Gather:
    def __init__(self, streams, src, out, direct, send, recv, sib_send, sib_recv):
        self.streams, self.src, self.out, self.direct = streams, src, out, direct
        self.sems = (send, recv, sib_send, sib_recv)
        self.coords, self.core = place()
        self.rows = out.shape[3]

    def cols(self, s, side):
        _, off, width = self.streams[s]
        return pl.ds(pl.multiple_of(side * (self.out.shape[4] // 2) + off, 128), width)

    def part(self, s, p, kind, at, side):
        full = order_of(self.streams[s][0])[:p]
        idx = [pl.ds(0, SIDE) if d in full else at[d] for d in range(3)]
        half = self.rows // 2
        r0, nr = (0, self.rows) if kind < 2 or p in self.direct else ((kind - 2) * half, half)
        return self.out.at[idx[0], idx[1], idx[2], pl.ds(r0, nr), self.cols(s, side)]

    def hop(self, s, p, kind):
        dim = order_of(self.streams[s][0])[p]
        direct = p in self.direct
        at = shifted(self.coords, dim, 0 if direct else (0, 0, -1, 1)[kind])
        to = shifted(self.coords, dim, (1, -1, 2 if direct else 1, -1)[kind])
        dst = self.part(s, p, kind, at, self.core)
        src = self.src.at[:, self.cols(s, self.core)] if p == 0 and (direct or kind < 2) else dst
        return pltpu.make_async_remote_copy(src, dst, self.sems[0].at[s, p, kind], self.sems[1].at[s, p, kind],
                                            device_id=device(to, self.core), device_id_type=MESH)

    def landed(self, s, p, kind, side):
        dim = order_of(self.streams[s][0])[p]
        return self.part(s, p, kind, shifted(self.coords, dim, (-1, 1, -2, 2)[kind]), side)

    def gift(self, s, p, kind, side):
        here = self.landed(s, p, kind, side)
        return pltpu.make_async_remote_copy(here, here, self.sems[2].at[s, p, kind], self.sems[3].at[s, p, kind],
                                            device_id=device(self.coords, 1 - self.core), device_id_type=MESH)

    def arrive(self, s, p, kind):
        here = self.landed(s, p, kind, self.core)
        pltpu.make_async_remote_copy(here, here, self.sems[0].at[s, p, kind], self.sems[1].at[s, p, kind],
                                     device_id=device(self.coords, 1 - self.core), device_id_type=MESH).wait_recv()

    def start(self, s, p):
        self.hop(s, p, 0).start()
        self.hop(s, p, 1).start()
        if p in self.direct:
            self.hop(s, p, 2).start()

    def middle(self, s, p):
        if p in self.direct:
            for kind in range(3):
                self.arrive(s, p, kind)
                self.gift(s, p, kind, self.core).start()
            return
        for kind in (0, 1):
            self.arrive(s, p, kind)
            self.hop(s, p, kind + 2).start()
            self.gift(s, p, kind, self.core).start()

    def finish(self, s, p):
        for kind in () if p in self.direct else (2, 3):
            self.arrive(s, p, kind)
            self.gift(s, p, kind, self.core).start()

    def drain(self, s, p):
        for kind in range(3 if p in self.direct else 4):
            self.hop(s, p, kind).wait_send()
            self.gift(s, p, kind, self.core).wait_send()
            self.gift(s, p, kind, 1 - self.core).wait_recv()


class Scatter:
    def __init__(self, streams, own, sib, acc, sbuf, rbuf, send, recv):
        self.streams, self.own, self.sib = streams, own, sib
        self.acc, self.sbuf, self.rbuf, self.sems = acc, sbuf, rbuf, (send, recv)
        self.coords, self.core = place()

    def half(self, s):
        return self.acc[s][0].shape[1] // 2

    def dim(self, s, q):
        return order_of(self.streams[s][0])[2 - q]

    def value(self, s, q, at, n, r0):
        colour, off, width = self.streams[s]
        order = order_of(colour)
        nr = self.half(s)
        idx = list(at)
        full = sorted(order[:2 - q])
        for d, digit in zip(full, (n // SIDE, lax.rem(n, SIDE)) if len(full) == 2 else (n,)):
            idx[d] = digit
        if q == 0:
            where = (idx[0] * 16 + idx[1] * 4 + idx[2], pl.ds(r0, nr), pl.ds(off, width))
            return self.own[where] + self.sib[where].astype(jnp.float32)
        m = 0
        for d in sorted(order[:3 - q]):
            m = m * SIDE + idx[d]
        return self.acc[s][q - 1][m, pl.ds(r0, nr), :]

    def hop(self, s, q, kind):
        lo, n = ((0, 2), (2, 2), (4, 1), (5, 1))[kind]
        to = shifted(self.coords, self.dim(s, q), (1, -1, 1, -1)[kind])
        return pltpu.make_async_remote_copy(
            self.sbuf[s][q].at[pl.ds(lo, n)], self.rbuf[s][q].at[pl.ds(lo, n)],
            self.sems[0].at[s, q, kind], self.sems[1].at[s, q, kind],
            device_id=device(to, self.core), device_id_type=MESH)

    def each(self, q, body):
        n = SIDE ** (2 - q)

        def step(i, carry):
            body(i)
            return carry
        lax.fori_loop(0, n, step, 0, unroll=min(n, 4))

    def one(self, s, q):
        dim, half, buf = self.dim(s, q), self.half(s), self.sbuf[s][q]
        far, right, left = (shifted(self.coords, dim, d) for d in (2, 1, -1))

        def to_right(n):
            buf[0, n] = self.value(s, q, far, n, 0).astype(buf.dtype)
            buf[1, n] = self.value(s, q, right, n, half).astype(buf.dtype)

        def to_left(n):
            buf[2, n] = self.value(s, q, far, n, half).astype(buf.dtype)
            buf[3, n] = self.value(s, q, left, n, 0).astype(buf.dtype)
        self.each(q, to_right)
        self.hop(s, q, 0).start()
        self.each(q, to_left)
        self.hop(s, q, 1).start()

    def two(self, s, q):
        dim, half, buf, got = self.dim(s, q), self.half(s), self.sbuf[s][q], self.rbuf[s][q]
        right, left = (shifted(self.coords, dim, d) for d in (1, -1))

        def to_right(n):
            buf[4, n] = (self.value(s, q, right, n, 0) + got[0, n].astype(jnp.float32)).astype(buf.dtype)

        def to_left(n):
            buf[5, n] = (self.value(s, q, left, n, half) + got[2, n].astype(jnp.float32)).astype(buf.dtype)
        self.hop(s, q, 0).wait_recv()
        self.each(q, to_right)
        self.hop(s, q, 2).start()
        self.hop(s, q, 1).wait_recv()
        self.each(q, to_left)
        self.hop(s, q, 3).start()

    def three(self, s, q):
        half, got, acc = self.half(s), self.rbuf[s][q], self.acc[s][q]
        self.hop(s, q, 2).wait_recv()
        self.hop(s, q, 3).wait_recv()

        def keep(n):
            for r0, i, j in ((0, 3, 4), (half, 1, 5)):
                acc[n, pl.ds(r0, half), :] = (self.value(s, q, self.coords, n, r0) + got[i, n].astype(jnp.float32)
                                              + got[j, n].astype(jnp.float32))
        self.each(q, keep)

    def drain(self, s, q):
        for kind in range(4):
            self.hop(s, q, kind).wait_send()


def transpose_into(dst, src):
    def strip(j, carry):
        at = pl.ds(pl.multiple_of(j * CHUNK, CHUNK), CHUNK)
        dst[at, :] = src[:, at].T
        return carry
    lax.fori_loop(0, src.shape[1] // CHUNK, strip, 0)


def grad_chunk(grads_t, acts, dst, side, j):
    half = dst.shape[2]
    rhs = acts[:, pl.ds(pl.multiple_of(side * half + j * CHUNK, CHUNK), CHUNK)]
    n_rows = 512

    def strip(i, carry):
        at = pl.multiple_of(i * n_rows, n_rows)
        out = nn(grads_t[pl.ds(at, n_rows), :], rhs).astype(dst.dtype)
        dst[pl.ds(i * (n_rows // 32), n_rows // 32), :, pl.ds(j * CHUNK, CHUNK)] = out.reshape(n_rows // 32, 32, CHUNK)
        return carry
    lax.fori_loop(0, grads_t.shape[0] // n_rows, strip, 0)


def chunk_gift(src, dst, send, recv, j):
    coords, core = place()
    at = pl.ds(j * CHUNK, CHUNK)
    return pltpu.make_async_remote_copy(src.at[:, :, at], dst.at[:, :, at], send.at[j], recv.at[j],
                                        device_id=device(coords, 1 - core), device_id_type=MESH)


def wire_shapes(streams, dtype, rows, phases):
    return [pltpu.VMEM((6, SIDE ** (2 - q), rows // 2, width), dtype) for _, _, width in streams for q in phases]


def acc_shapes(streams, rows, phases):
    return [((SIDE ** (2 - q), rows, width), jnp.float32) for _, _, width in streams for q in phases]


def scatter_kernel(normed, d_qkv, w_ref, x_ref, dy_ref, inv_rms, gain, post_row, *refs):
    no = len(OUT)
    acc_in, scratch = refs[:no], refs[no + 6:]
    dx_ref, grad_q, grad_k, grad_v, grad_o, out_g = refs[no:no + 6]
    scratch = list(scratch)

    def take(n):
        head = scratch[:n]
        del scratch[:n]
        return head
    normed_t, own_q, sib_out, sib_q, own_g, sib_g, sib_in_g, out_q, out_o, w_buf, dn, pre_row = take(12)
    nq = len(QKV)
    acc_q, sbuf_q, rbuf_q = take(3 * nq), take(3 * nq), take(3 * nq)
    acc_o, sbuf_o, rbuf_o = take(2 * no), take(2 * no), take(2 * no)
    acc_g, sbuf_g, rbuf_g = take(3), take(3), take(3)
    sems = take(6)
    gift_send, gift_recv, gain_sem, fin_send, fin_recv, w_sem = take(6)
    bf, f32 = jnp.bfloat16, jnp.float32
    n_tok, dim = x_ref.shape
    strips = dim // CHUNK
    coords, core = place()
    sibling = device(coords, 1 - core)
    greet(coords, core)

    def triples(flat):
        return [flat[3 * s:3 * s + 3] for s in range(len(flat) // 3)]

    def tails(flat, heads):
        return [[heads[s]] + flat[2 * s:2 * s + 2] for s in range(no)]
    qkv = Scatter(QKV, own_q, sib_q, triples(acc_q), triples(sbuf_q), triples(rbuf_q), *sems[0:2])
    out = Scatter(OUT, None, None, tails(acc_o, acc_in), tails(sbuf_o, (None,) * no),
                  tails(rbuf_o, (None,) * no), *sems[2:4])
    gains = Scatter(GAIN, own_g, sib_in_g, triples(acc_g), triples(sbuf_g), triples(rbuf_g), *sems[4:6])
    gain_gift = pltpu.make_async_remote_copy(sib_g, sib_in_g, gain_sem.at[0], gain_sem.at[1],
                                             device_id=sibling, device_id_type=MESH)
    loads = [pltpu.make_async_copy(w_ref.at[pl.ds(8 * j, 8)], w_buf.at[j % 2], w_sem.at[j]) for j in range(strips)]
    loads[0].start()
    loads[1].start()
    for s in range(len(OUT)):
        out.one(s, 1)
    own_g[...] = jnp.zeros_like(own_g)
    sib_g[...] = jnp.zeros_like(sib_g)
    transpose_into(normed_t, normed)
    chunks = own_q.shape[2] // CHUNK
    gifts = [chunk_gift(sib_out, sib_q, gift_send, gift_recv, j) for j in range(chunks)]
    grad_chunk(normed_t, d_qkv, sib_out, 1 - core, 0)
    gifts[0].start()
    ready = 0
    for j in range(chunks):
        if j + 1 < chunks:
            grad_chunk(normed_t, d_qkv, sib_out, 1 - core, j + 1)
            gifts[j + 1].start()
        grad_chunk(normed_t, d_qkv, own_q, core, j)
        gifts[j].wait_recv()
        while ready < nq and QKV[ready][1] + QKV[ready][2] <= (j + 1) * CHUNK:
            qkv.one(ready, 0)
            ready += 1
        if j == 1:
            for s in range(no):
                out.two(s, 1)
        if j == 3:
            for s in range(no):
                out.three(s, 1)
                out.one(s, 2)
    for j in range(strips):
        loads[j].wait()
        dn[:, pl.ds(j * CHUNK, CHUNK)] = nt(d_qkv[...], w_buf[j % 2].reshape(CHUNK, d_qkv.shape[1])).astype(bf)
        if j + 2 < strips:
            loads[j + 2].start()
    work = [(qkv, s) for s in range(nq)]
    for s in range(len(OUT)):
        out.two(s, 2)
    for scatter, s in work:
        scatter.two(s, 0)
    pre_row[...] = jnp.zeros_like(pre_row)
    one_gain = 1.0 + gain[pl.ds(0, 1), :]

    def back(i, carry):
        at = pl.ds(i * 32, 32)
        xs, g, inv = x_ref[at, :].astype(f32), dn[at, :].astype(f32), inv_rms[at, :]
        scaled = g * one_gain
        mean = jnp.sum(scaled * xs, axis=1, keepdims=True) * (1.0 / dim)
        dx_ref[at, :] = (dy_ref[at, :].astype(f32) + (inv * scaled - xs * (inv * inv * inv * mean))).astype(bf)
        pre_row[...] += jnp.sum((g * (xs * inv)).reshape(4, 8, dim), axis=0)
        return carry
    lax.fori_loop(0, n_tok // 32, back, 0)
    pre, post = jnp.sum(pre_row[...], axis=0, keepdims=True), post_row[...]
    own_row, sib_row = jnp.where(core == 0, pre, post), jnp.where(core == 0, post, pre)
    for j in range(16):
        for x in range(SIDE):
            own_g[SIDE * j + x, pl.ds(0, 1), :] = own_row[:, j * 128:(j + 1) * 128]
            sib_g[SIDE * j + x, pl.ds(0, 1), :] = sib_row[:, j * 128:(j + 1) * 128]
    gain_gift.start()
    for scatter, s in work:
        scatter.three(s, 0)
        scatter.one(s, 1)
    for s in range(len(OUT)):
        out.three(s, 2)
    gain_gift.wait_recv()
    gains.one(0, 0)
    work = work + [(gains, 0)]
    for q in range(3):
        for scatter, s in work:
            if q > 0 or scatter is gains:
                scatter.two(s, q)
        for scatter, s in work:
            if q == 0 and scatter is not gains:
                continue
            scatter.three(s, q)
            if q < 2:
                scatter.one(s, q + 1)
    fins = []
    k = 0
    for scatter, ref in ((qkv, out_q), (out, out_o), (gains, out_g)):
        for s, (_, off, width) in enumerate(scatter.streams):
            part = scatter.acc[s][2].at[0]
            ref[core, :, pl.ds(off, width)] = scatter.acc[s][2][0]
            here, there = (ref.at[side, :, pl.ds(off, width)] for side in (core, 1 - core))
            pair = [pltpu.make_async_remote_copy(part, side, fin_send.at[k], fin_recv.at[k],
                                                 device_id=sibling, device_id_type=MESH) for side in (here, there)]
            pair[0].start()
            fins.append(pair)
            k += 1
    for mine, theirs in fins:
        mine.wait_send()
        theirs.wait_recv()
    n_heads = grad_q.shape[1]
    per = out_q.shape[2] // TILE
    for h in range(n_heads + 2):
        part = out_q[h // per, :, pl.ds(h % per * TILE, TILE)]
        if h < n_heads:
            grad_q[:, h, :] = part
        else:
            (grad_k, grad_v)[h - n_heads][:, 0, :] = part
    for h in range(n_heads):
        grad_o[h] = out_o[h // 4, :, pl.ds(h % 4 * TILE, TILE)]
    for copy in gifts + [gain_gift]:
        copy.wait_send()
    for scatter, phases in ((qkv, (0, 1, 2)), (out, (1, 2)), (gains, (0, 1, 2))):
        for s in range(len(scatter.streams)):
            for q in phases:
                scatter.drain(s, q)


def scatter_grads(normed, d_qkv, w, x, dy, inv_rms, gain, post_row, accs, n_heads):
    bf, f32 = jnp.bfloat16, jnp.float32
    n_tok, model_dim = normed.shape
    half, rows = d_qkv.shape[1] // 2, 32
    blocks = model_dim // rows
    dma = pltpu.SemaphoreType.DMA
    vmem = pl.BlockSpec(memory_space=pltpu.VMEM)
    scratch = [pltpu.VMEM((model_dim, n_tok), bf), pltpu.VMEM((blocks, rows, half), f32),
               pltpu.VMEM((blocks, rows, half), bf), pltpu.VMEM((blocks, rows, half), bf)]
    scratch += [pltpu.VMEM((blocks, 16, 128), f32)] * 3
    scratch += [pltpu.VMEM((2, rows, half), f32), pltpu.VMEM((2, rows, 1024), f32),
                pltpu.VMEM((2, CHUNK // rows, rows, 2 * half), bf), pltpu.VMEM((n_tok, model_dim), bf),
                pltpu.VMEM((8, model_dim), f32)]
    for streams, dtype, n_rows, phases in ((QKV, bf, rows, (0, 1, 2)), (OUT, bf, rows, (1, 2)), (GAIN, f32, 16, (0, 1, 2))):
        scratch += [pltpu.VMEM(*a) for a in acc_shapes(streams, n_rows, phases)]
        scratch += wire_shapes(streams, dtype, n_rows, phases) * 2
    scratch += [dma((len(st), 3, 4)) for st in (QKV, OUT, GAIN) for _ in range(2)]
    scratch += [dma((half // CHUNK,))] * 2 + [dma((2,))] + [dma((len(QKV) + len(OUT) + 1,))] * 2 + [dma((model_dim // CHUNK,))]
    return pl.pallas_call(
        scatter_kernel, name="scatter_grads",
        out_shape=[jax.ShapeDtypeStruct((n_tok, model_dim), bf), jax.ShapeDtypeStruct((rows, n_heads, TILE), f32),
                   jax.ShapeDtypeStruct((rows, 1, TILE), f32), jax.ShapeDtypeStruct((rows, 1, TILE), f32),
                   jax.ShapeDtypeStruct((n_heads, rows, TILE), f32), jax.ShapeDtypeStruct((2, 16, 128), f32)],
        in_specs=[vmem] * 2 + [pl.BlockSpec(memory_space=pltpu.HBM)] + [vmem] * (5 + len(OUT)), out_specs=[vmem] * 6,
        scratch_shapes=scratch,
        compiler_params=pltpu.CompilerParams(collective_id=2, has_side_effects=True, vmem_limit_bytes=VMEM_MAX),
    )(normed, d_qkv, w, x, dy, inv_rms, gain, post_row, *accs)


LOG2E = 1.4426950408889634
TILE = 256


def nt(a, b):
    return lax.dot_general(a, b, (((1,), (1,)), ((), ())), preferred_element_type=jnp.float32)


def nn(a, b):
    return lax.dot_general(a, b, (((1,), (0,)), ((), ())), preferred_element_type=jnp.float32)


def fill_mask(mask, pos):
    n_keys, n_q = mask.shape
    core = lax.axis_index('cp')
    for c in range(n_keys // TILE):
        base = jnp.where(c < n_q // TILE, (1 - core) * n_q, core * n_q - n_q) + c * TILE
        for i in range(n_q // TILE):
            k_at = base + lax.broadcasted_iota(jnp.int32, (TILE, TILE), 0)
            q_at = core * n_q + i * TILE + lax.broadcasted_iota(jnp.int32, (TILE, TILE), 1)
            seen = (k_at <= q_at) & (k_at >= q_at - pos[:, pl.ds(i * TILE, TILE)])
            mask[pl.ds(c * TILE, TILE), pl.ds(i * TILE, TILE)] = jnp.where(seen, 1.0, 0.0)


def keys_for(i, n_q):
    return n_q + (i + 1) * TILE


def forward_kernel(ratio, x_ref, cos_ref, sin_ref, pos, in0, in1, in2,
                   wq_out, wo_out, gain_out, normed, inv_rms, q_ref, kv_ref, o_ref, inv_ref,
                   wq, gains, gain_row, mask, v_t, w_scr, p_scr, *sems):
    n_q, dim = x_ref.shape
    bf, f32 = jnp.bfloat16, jnp.float32
    coords, core = place()
    sibling = device(coords, 1 - core)
    greet(coords, core, (1, -1, 2))
    own_sem, swap_send, swap_recv = sems[12:15]
    qkv, out, gain = (Gather(st, src, dst, direct, *sems[4 * g:4 * g + 4]) for g, (st, src, dst, direct) in enumerate(
        ((QKV, in0, wq, (0,)), (OUT, in1, wo_out, (0,)), (GAIN, in2, gains, (0, 1, 2)))))
    nq = range(len(QKV))
    gain.start(0, 0)
    for s in nq:
        qkv.start(s, 0)
    for s in range(len(OUT)):
        out.start(s, 0)
    own_out = pltpu.make_async_copy(in1, wo_out.at[coords[0], coords[1], coords[2]], own_sem.at[0])
    own_out.start()
    wq[coords[0], coords[1], coords[2]] = in0[...]
    gains[coords[0], coords[1], coords[2]] = in2[...]

    def stats(i, carry):
        at = pl.ds(i * 64, 64)
        v = x_ref[at, :].astype(f32)
        inv_rms[at, :] = lax.rsqrt(jnp.sum(v * v, axis=1, keepdims=True) * (1.0 / dim) + NORM_EPS)
        return carry
    lax.fori_loop(0, n_q // 64, stats, 0)
    gain.middle(0, 0)
    gain.start(0, 1)
    for s in nq:
        qkv.middle(s, 0)
        qkv.start(s, 1)
    gain.middle(0, 1)
    gain.start(0, 2)
    for s in range(len(OUT)):
        out.middle(s, 0)
    own_out.wait()
    for s in nq:
        qkv.middle(s, 1)
    for s in range(len(OUT)):
        out.start(s, 1)
    gain.middle(0, 2)
    for s in nq:
        qkv.finish(s, 1)
        qkv.start(s, 2)
    for p in range(3):
        gain.drain(0, p)
    for kind in range(2):
        for j in range(16):
            row = sum(gains[j // 4, j % 4, x, pl.ds(0, 1), pl.ds(kind * 128, 128)] for x in range(SIDE))
            gain_row[pl.ds(kind, 1), pl.ds(j * 128, 128)] = row
    gain_out[...] = gain_row[...]
    fill_mask(mask, pos)

    def scale(i, carry):
        at = pl.ds(i * 64, 64)
        normed[at, :] = (x_ref[at, :].astype(f32) * inv_rms[at, :] * (1.0 + gain_row[pl.ds(0, 1), :])).astype(bf)
        return carry
    lax.fori_loop(0, n_q // 64, scale, 0)
    for s in nq:
        qkv.middle(s, 2)
    for s in range(len(OUT)):
        out.middle(s, 1)
    for s in nq:
        qkv.finish(s, 2)
    for s in range(len(OUT)):
        out.finish(s, 1)
        out.start(s, 2)
    for s in nq:
        for p in range(3):
            qkv.drain(s, p)
    keep = pltpu.make_async_copy(wq, wq_out, own_sem.at[1])
    keep.start()

    def project(n):
        rhs = wq[:, :, :, :, pl.ds(pl.multiple_of(n * TILE, TILE), TILE)].reshape(dim, TILE)
        return nn(normed[...], rhs).astype(bf)

    def rope(u):
        lo, hi = u[:, :TILE // 2].astype(f32), u[:, TILE // 2:].astype(f32)
        c, s = cos_ref[...], sin_ref[...]
        return jnp.concatenate([lo * c - hi * s, hi * c + lo * s], axis=1).astype(bf)
    n_heads = q_ref.shape[1] // TILE
    mine, other = pl.ds(n_q, n_q), pl.ds(0, n_q)
    kv_ref[mine, pl.ds(0, TILE)] = rope(project(n_heads))
    kv_ref[mine, pl.ds(TILE, TILE)] = project(n_heads + 1)
    swap = pltpu.make_async_remote_copy(kv_ref.at[mine], kv_ref.at[other], swap_send.at[0], swap_recv.at[0],
                                        device_id=sibling, device_id_type=MESH)
    swap.start()

    def project_head(h, carry):
        q_ref[:, pl.ds(pl.multiple_of(h * TILE, TILE), TILE)] = rope(project(h))
        return carry
    lax.fori_loop(0, n_heads, project_head, 0)
    for s in range(len(OUT)):
        out.middle(s, 2)
    swap.wait_recv()
    k_cols = pl.ds(0, TILE)
    v_t[...] = kv_ref[:, pl.ds(TILE, TILE)].T

    def head(h, carry):
        cols = pl.ds(pl.multiple_of(h * TILE, TILE), TILE)
        for i in range(n_q // TILE):
            qi = q_ref[pl.ds(i * TILE, TILE), cols]
            n_keys = keys_for(i, n_q)
            total = jnp.zeros((8, TILE), f32)
            for c in range(n_keys // TILE):
                t = jnp.tanh(nt(kv_ref[pl.ds(c * TILE, TILE), k_cols], qi) * ratio)
                w = jnp.exp2(t * (SOFT_CAP * LOG2E)) * mask[pl.ds(c * TILE, TILE), pl.ds(i * TILE, TILE)]
                w_scr[i, pl.ds(c * TILE, TILE), :] = w
                total = total + jnp.sum(w.reshape(TILE // 8, 8, TILE), axis=0)
            inv = 1.0 / jnp.sum(total, axis=0, keepdims=True)
            inv_ref[h, :, pl.ds(i * TILE, TILE)] = inv
            p_scr[i, pl.ds(0, n_keys), :] = (w_scr[i, pl.ds(0, n_keys), :] * inv).astype(bf)
            o_t = nn(v_t[:, pl.ds(0, n_keys)], p_scr[i, pl.ds(0, n_keys), :])
            o_ref[pl.ds(i * TILE, TILE), cols] = o_t.T.astype(bf)
        return carry
    lax.fori_loop(0, n_heads, head, 0)
    for s in range(len(OUT)):
        out.finish(s, 2)
    for s in range(len(OUT)):
        for p in range(3):
            out.drain(s, p)
    swap.wait_send()
    keep.wait()


def forward(x, cos_t, sin_t, pos, w0, w1, w2, n_heads, ratio):
    n_q, dim = x.shape
    n_k = 2 * n_q
    bf, f32 = jnp.bfloat16, jnp.float32
    dma = pltpu.SemaphoreType.DMA
    vmem, hbm = pl.BlockSpec(memory_space=pltpu.VMEM), pl.BlockSpec(memory_space=pltpu.HBM)
    grid = (SIDE, SIDE, SIDE)
    shape = jax.ShapeDtypeStruct
    tiles = n_q // TILE
    return pl.pallas_call(
        functools.partial(forward_kernel, ratio), name="forward",
        out_shape=[shape(grid + w0.shape, bf), shape(grid + w1.shape, bf), shape((2, dim), f32), shape((n_q, dim), bf),
                   shape((n_q, 1), f32), shape((n_q, n_heads * TILE), bf), shape((n_k, 2 * TILE), bf),
                   shape((n_q, n_heads * TILE), bf), shape((n_heads, 1, n_q), f32)],
        in_specs=[vmem] * 7, out_specs=[hbm] * 2 + [vmem] * 7,
        scratch_shapes=[pltpu.VMEM(grid + w0.shape, bf), pltpu.VMEM(grid + w2.shape, f32), pltpu.VMEM((2, dim), f32),
                        pltpu.VMEM((n_k, n_q), f32), pltpu.VMEM((TILE, n_k), bf),
                        pltpu.VMEM((tiles, n_k, TILE), f32), pltpu.VMEM((tiles, n_k, TILE), bf)]
        + [dma((len(st), 3, 4)) for st in (QKV, OUT, GAIN) for _ in range(4)]
        + [dma((2,)), dma((1,)), dma((1,))],
        compiler_params=pltpu.CompilerParams(collective_id=1, has_side_effects=True, vmem_limit_bytes=VMEM_MAX),
    )(x, cos_t, sin_t, pos, w0, w1, w2)


def attend_back_kernel(ratio, q_ref, do_ref, kv_ref, pos, inv_ref, dz_ref, o_ref, cos_ref, sin_ref,
                       dqkv_ref, *refs):
    no = len(OUT)
    accs = refs[:no]
    (mask, k_t, g_scr, dp_scr, p_scr, ds_scr, dk_acc, dv_acc, dkv_out, dkv_in, dz_t, own, sib_out, sib_in,
     *scratch) = refs[no:]
    n_q = q_ref.shape[0]
    coords, core = place()
    greet(coords, core)
    sbuf, rbuf, sems = scratch[:no], scratch[no:2 * no], scratch[2 * no:2 * no + 2]
    gift_send, gift_recv, swap_sem = scratch[2 * no + 2:]
    bf, f32 = jnp.bfloat16, jnp.float32
    swap = pltpu.make_async_remote_copy(dkv_out, dkv_in, swap_sem.at[0], swap_sem.at[1],
                                        device_id=device(coords, 1 - core), device_id_type=MESH)

    def rope_back(u):
        lo, hi = u[:, :TILE // 2].astype(f32), u[:, TILE // 2:].astype(f32)
        c, s = cos_ref[pl.ds(0, u.shape[0]), :], sin_ref[pl.ds(0, u.shape[0]), :]
        return jnp.concatenate([lo * c + hi * s, hi * c - lo * s], axis=1).astype(bf)
    out = Scatter(OUT, own, sib_in, [[a] for a in accs], [[b] for b in sbuf], [[b] for b in rbuf], *sems)
    chunks = own.shape[2] // CHUNK
    transpose_into(dz_t, dz_ref)
    gifts = [chunk_gift(sib_out, sib_in, gift_send, gift_recv, j) for j in range(chunks)]
    grad_chunk(dz_t, o_ref, sib_out, 1 - core, 0)
    gifts[0].start()
    ready = 0
    for j in range(chunks):
        if j + 1 < chunks:
            grad_chunk(dz_t, o_ref, sib_out, 1 - core, j + 1)
            gifts[j + 1].start()
        grad_chunk(dz_t, o_ref, own, core, j)
        gifts[j].wait_recv()
        while ready < no and OUT[ready][1] + OUT[ready][2] <= (j + 1) * CHUNK:
            out.one(ready, 0)
            ready += 1
    fill_mask(mask, pos)
    k_cols, v_cols = pl.ds(0, TILE), pl.ds(TILE, TILE)
    k_t[...] = kv_ref[:, k_cols].T
    dk_acc[...] = jnp.zeros_like(dk_acc)
    dv_acc[...] = jnp.zeros_like(dv_acc)

    def head(h, carry):
        cols = pl.ds(pl.multiple_of(h * TILE, TILE), TILE)
        for i in range(n_q // TILE):
            rows = pl.ds(i * TILE, TILE)
            qi, doi = q_ref[rows, cols], do_ref[rows, cols]
            inv = inv_ref[h, :, rows]
            n_keys = keys_for(i, n_q)
            total = jnp.zeros((8, TILE), jnp.float32)
            for c in range(n_keys // TILE):
                at = pl.ds(c * TILE, TILE)
                t = jnp.tanh(nt(kv_ref[at, k_cols], qi) * ratio)
                p = jnp.exp2(t * (SOFT_CAP * LOG2E)) * (mask[at, rows] * inv)
                dp = nt(kv_ref[at, v_cols], doi)
                p_scr[i, at, :] = p.astype(jnp.bfloat16)
                g_scr[i, at, :] = p * ((1.0 - t * t) * (ratio * SOFT_CAP))
                dp_scr[i, at, :] = dp
                total = total + jnp.sum((p * dp).reshape(TILE // 8, 8, TILE), axis=0)
            row_dot = jnp.sum(total, axis=0, keepdims=True)
            seen = pl.ds(0, n_keys)
            ds_scr[i, seen, :] = ((dp_scr[i, seen, :] - row_dot) * g_scr[i, seen, :]).astype(jnp.bfloat16)
            dq_t = nn(k_t[:, seen], ds_scr[i, seen, :])
            dq = dq_t.T.astype(bf)
            lo, hi = dq[:, :TILE // 2].astype(f32), dq[:, TILE // 2:].astype(f32)
            cos, sin = cos_ref[rows, :], sin_ref[rows, :]
            dqkv_ref[rows, cols] = jnp.concatenate([lo * cos + hi * sin, hi * cos - lo * sin], axis=1).astype(bf)
            dk_acc[seen, :] += nn(ds_scr[i, seen, :], qi)
            dv_acc[seen, :] += nn(p_scr[i, seen, :], doi)

        @pl.when(h == 3)
        def _():
            for s in range(no):
                out.two(s, 0)

        @pl.when(h == 6)
        def _():
            for s in range(no):
                out.three(s, 0)
        return carry
    lax.fori_loop(0, q_ref.shape[1] // TILE, head, 0)
    mine, other = pl.ds(n_q, n_q), pl.ds(0, n_q)
    dkv_out[:, k_cols] = dk_acc[other, :].astype(bf)
    dkv_out[:, v_cols] = dv_acc[other, :].astype(bf)
    swap.start()
    swap.wait_recv()
    q_cols = q_ref.shape[1]
    dqkv_ref[:, pl.ds(q_cols, TILE)] = rope_back((dk_acc[mine, :] + dkv_in[:, k_cols].astype(f32)).astype(bf))
    dqkv_ref[:, pl.ds(q_cols + TILE, TILE)] = (dv_acc[mine, :] + dkv_in[:, v_cols].astype(f32)).astype(bf)
    for s in range(len(OUT)):
        out.drain(s, 0)
    for copy in gifts + [swap]:
        copy.wait_send()


def attend_back(q, do, kv, pos, inv_sum, dz, o, cos_t, sin_t, ratio):
    n_q, n_k = q.shape[0], kv.shape[0]
    vmem = pl.BlockSpec(memory_space=pltpu.VMEM)
    tiles = n_q // TILE
    bf, f32 = jnp.bfloat16, jnp.float32
    return pl.pallas_call(
        functools.partial(attend_back_kernel, ratio), name="attend_back",
        out_shape=[jax.ShapeDtypeStruct((n_q, q.shape[1] + 2 * TILE), bf)]
        + [jax.ShapeDtypeStruct(*a) for a in acc_shapes(OUT, 32, (0,))],
        in_specs=[vmem] * 9, out_specs=[vmem] * (1 + len(OUT)),
        scratch_shapes=[pltpu.VMEM((n_k, n_q), f32), pltpu.VMEM((TILE, n_k), bf),
                        pltpu.VMEM((tiles, n_k, TILE), f32), pltpu.VMEM((tiles, n_k, TILE), f32),
                        pltpu.VMEM((tiles, n_k, TILE), bf), pltpu.VMEM((tiles, n_k, TILE), bf),
                        pltpu.VMEM((n_k, TILE), f32), pltpu.VMEM((n_k, TILE), f32),
                        pltpu.VMEM((n_q, 2 * TILE), bf), pltpu.VMEM((n_q, 2 * TILE), bf),
                        pltpu.VMEM((dz.shape[1], n_q), bf), pltpu.VMEM((dz.shape[1] // 32, 32, o.shape[1] // 2), f32)]
        + [pltpu.VMEM((dz.shape[1] // 32, 32, o.shape[1] // 2), bf)] * 2
        + wire_shapes(OUT, bf, 32, (0,)) * 2 + [pltpu.SemaphoreType.DMA((len(OUT), 3, 4))] * 2
        + [pltpu.SemaphoreType.DMA((o.shape[1] // 2 // CHUNK,))] * 2 + [pltpu.SemaphoreType.DMA((2,))],
        compiler_params=pltpu.CompilerParams(collective_id=4, has_side_effects=True, vmem_limit_bytes=VMEM_MAX),
    )(q, do, kv, pos, inv_sum, dz, o, cos_t, sin_t)


def rope_tables(pos_ids, head_dim):
    half_dim = head_dim // 2
    inv_freq = ROPE_BASE ** (-2.0 * jnp.arange(half_dim, dtype=jnp.float32) / head_dim)
    angles = pos_ids.astype(jnp.float32)[..., None] * inv_freq
    return jnp.cos(angles)[..., None, :], jnp.sin(angles)[..., None, :]


def rotate(values, cos_t, sin_t):
    half_dim = values.shape[-1] // 2
    first_half = values[..., :half_dim].astype(jnp.float32)
    second_half = values[..., half_dim:].astype(jnp.float32)
    rotated = jnp.concatenate([first_half * cos_t - second_half * sin_t,
                               second_half * cos_t + first_half * sin_t], axis=-1)
    return rotated.astype(jnp.bfloat16)


def norm_forward(values, gain_vec):
    values_f = values.astype(jnp.float32)
    inv_rms = lax.rsqrt(jnp.mean(values_f * values_f, axis=-1, keepdims=True) + NORM_EPS)
    normed = values_f * inv_rms * (1.0 + gain_vec.astype(jnp.float32))
    return normed.astype(jnp.bfloat16), inv_rms


def norm_backward(values, inv_rms, gain_vec, grads):
    values_f = values.astype(jnp.float32)
    grads_f = grads.astype(jnp.float32)
    scaled = grads_f * (1.0 + gain_vec.astype(jnp.float32))
    d_values = inv_rms * scaled - values_f * inv_rms ** 3 * jnp.mean(scaled * values_f, axis=-1, keepdims=True)
    d_gain = jnp.sum(grads_f * values_f * inv_rms, axis=0)
    return d_values, d_gain


def dot(a, b, dims):
    return lax.dot_general(a, b, ((dims[:1], dims[1:]), ((), ())), preferred_element_type=jnp.float32)


def solution(mesh):
    tok_spec = P('fsdp', 'cp', None)
    ids_spec = P('fsdp', 'cp')
    in_spec = P('fsdp', None, None)
    out_spec = P(None, None, 'fsdp')
    gain_spec = P('fsdp')
    bf, f32 = jnp.bfloat16, jnp.float32

    def layer_local(hidden, doc_ids, doc_pos, grad_out, w_query, w_key, w_value, w_out, gain_pre, gain_post):
        _, n_tok, model_dim = hidden.shape
        hidden, grad_out = hidden[0], grad_out[0]
        n_heads, head_dim = w_query.shape[1], w_query.shape[2]
        rows = w_query.shape[0]
        q_cols = n_heads * head_dim
        w0 = jnp.concatenate([w_query.reshape(rows, q_cols), w_key.reshape(rows, head_dim),
                              w_value.reshape(rows, head_dim)], axis=1)
        w1 = w_out.reshape(q_cols, rows).T
        lane = lax.rem(lax.axis_index('fsdp'), SIDE) * rows
        w2 = jnp.zeros((8, 256), f32)
        for kind, g in enumerate((gain_pre, gain_post)):
            w2 = lax.dynamic_update_slice(w2, g.astype(f32)[None], (0, kind * 128 + lane))
        cos_t, sin_t = rope_tables(doc_pos[0], head_dim)
        q_scale = (head_dim if head_dim >= 256 else model_dim // n_heads) ** -0.5
        ratio = q_scale / SOFT_CAP
        wqkv, wo_t, gains, normed, inv_pre, q_flat, kv_all, attn_flat, inv_sum = forward(
            hidden, cos_t[:, 0], sin_t[:, 0], doc_pos, w0, w1, w2, n_heads, ratio)
        post_full = gains[1]
        wqkv = wqkv.reshape(model_dim // rows, rows, q_cols + 2 * head_dim)
        wo_t = wo_t.reshape(model_dim, q_cols)
        proj_out = dot(attn_flat, wo_t, (1, 1)).astype(bf)
        post_out, inv_post = norm_forward(proj_out, post_full)
        out_hidden = (hidden.astype(f32) + post_out.astype(f32)).astype(bf)

        d_proj, d_gain_post = norm_backward(proj_out, inv_post, post_full, grad_out)
        d_proj = d_proj.astype(bf)
        d_attn = dot(d_proj, wo_t, (1, 0)).astype(bf)

        d_qkv, *accs = attend_back(q_flat, d_attn, kv_all, doc_pos, inv_sum, d_proj, attn_flat, cos_t[:, 0], sin_t[:, 0], ratio)
        dx, g_q, g_k, g_v, g_o, g_g = scatter_grads(normed, d_qkv, wqkv, hidden, grad_out, inv_pre, gains,
                                                    d_gain_post[None], accs, n_heads)
        g_g = lax.dynamic_slice(g_g, (0, 0, lane), (2, 1, rows))[:, 0]
        return (out_hidden[None], dx[None], g_q, g_k, g_v, g_o.transpose(0, 2, 1),
                g_g[0], g_g[1])

    return jax.shard_map(layer_local, mesh=mesh,
                         in_specs=(tok_spec, ids_spec, ids_spec, tok_spec, in_spec, in_spec, in_spec, out_spec, gain_spec, gain_spec),
                         out_specs=(tok_spec, tok_spec, in_spec, in_spec, in_spec, out_spec, gain_spec, gain_spec),
                         check_vma=False)
```

```python
import functools

import jax
import jax.numpy as jnp
from jax import lax
from jax.experimental import pallas as pl
from jax.experimental.pallas import tpu as pltpu
from jax.sharding import PartitionSpec as P

SOFT_CAP = 50.0
NORM_EPS = 1e-6
ROPE_BASE = 10000.0
MESH = pl.DeviceIdType.MESH
SIDE = 4

QKV = ((0, 0, 256), (1, 256, 256), (2, 512, 256), (0, 768, 256), (1, 1024, 128), (2, 1152, 128))
OUT = ((0, 0, 256), (1, 256, 256), (2, 512, 256), (1, 768, 128), (2, 896, 128))
GAIN = ((0, 0, 128),)
CHUNK = 256


def place():
    f = lax.axis_index('fsdp')
    return (f // 16, lax.rem(f // 4, 4), lax.rem(f, 4)), lax.axis_index('cp')


def shifted(coords, dim, delta):
    out = list(coords)
    out[dim] = lax.rem(coords[dim] + delta + SIDE, SIDE)
    return tuple(out)


def device(coords, core):
    return (coords[0] * 16 + coords[1] * 4 + coords[2], core)


def greet(coords, core, steps=(1, -1)):
    barrier = pltpu.get_barrier_semaphore()
    for dim in range(3):
        for delta in steps:
            pl.semaphore_signal(barrier, inc=1, device_id=device(shifted(coords, dim, delta), core), device_id_type=MESH)
    pl.semaphore_signal(barrier, inc=1, device_id=device(coords, 1 - core), device_id_type=MESH)


def greeted(steps=(1, -1)):
    pl.semaphore_wait(pltpu.get_barrier_semaphore(), 3 * len(steps) + 1)


def order_of(colour):
    return tuple((colour + i) % 3 for i in range(3))


def region(ref, full, coords, rows, cols):
    idx = [pl.ds(0, SIDE) if d in full else coords[d] for d in range(3)]
    return ref.at[idx[0], idx[1], idx[2], pl.ds(*rows), pl.ds(*cols)]


class Gather:
    def __init__(self, streams, src, out, direct, send, recv, sib_send, sib_recv):
        self.streams, self.src, self.out, self.direct = streams, src, out, direct
        self.sems = (send, recv, sib_send, sib_recv)
        self.coords, self.core = place()
        self.rows = out.shape[3]

    def cols(self, s, side):
        _, off, width = self.streams[s]
        return pl.ds(pl.multiple_of(side * (self.out.shape[4] // 2) + off, 128), width)

    def part(self, s, p, kind, at, side):
        full = order_of(self.streams[s][0])[:p]
        idx = [pl.ds(0, SIDE) if d in full else at[d] for d in range(3)]
        half = self.rows // 2
        r0, nr = (0, self.rows) if kind < 2 or p in self.direct else ((kind - 2) * half, half)
        return self.out.at[idx[0], idx[1], idx[2], pl.ds(r0, nr), self.cols(s, side)]

    def hop(self, s, p, kind):
        dim = order_of(self.streams[s][0])[p]
        direct = p in self.direct
        at = shifted(self.coords, dim, 0 if direct else (0, 0, -1, 1)[kind])
        to = shifted(self.coords, dim, (1, -1, 2 if direct else 1, -1)[kind])
        dst = self.part(s, p, kind, at, self.core)
        src = self.src.at[:, self.cols(s, self.core)] if p == 0 and (direct or kind < 2) else dst
        return pltpu.make_async_remote_copy(src, dst, self.sems[0].at[s, p, kind], self.sems[1].at[s, p, kind],
                                            device_id=device(to, self.core), device_id_type=MESH)

    def landed(self, s, p, kind, side):
        dim = order_of(self.streams[s][0])[p]
        return self.part(s, p, kind, shifted(self.coords, dim, (-1, 1, -2, 2)[kind]), side)

    def gift(self, s, p, kind, side):
        here = self.landed(s, p, kind, side)
        return pltpu.make_async_remote_copy(here, here, self.sems[2].at[s, p, kind], self.sems[3].at[s, p, kind],
                                            device_id=device(self.coords, 1 - self.core), device_id_type=MESH)

    def arrive(self, s, p, kind):
        here = self.landed(s, p, kind, self.core)
        pltpu.make_async_remote_copy(here, here, self.sems[0].at[s, p, kind], self.sems[1].at[s, p, kind],
                                     device_id=device(self.coords, 1 - self.core), device_id_type=MESH).wait_recv()

    def start(self, s, p):
        self.hop(s, p, 0).start()
        self.hop(s, p, 1).start()
        if p in self.direct:
            self.hop(s, p, 2).start()

    def middle(self, s, p):
        if p in self.direct:
            for kind in range(3):
                self.arrive(s, p, kind)
                self.gift(s, p, kind, self.core).start()
            return
        for kind in (0, 1):
            self.arrive(s, p, kind)
            self.hop(s, p, kind + 2).start()
            self.gift(s, p, kind, self.core).start()

    def finish(self, s, p):
        for kind in () if p in self.direct else (2, 3):
            self.arrive(s, p, kind)
            self.gift(s, p, kind, self.core).start()

    def drain(self, s, p):
        for kind in range(3 if p in self.direct else 4):
            self.hop(s, p, kind).wait_send()
            self.gift(s, p, kind, self.core).wait_send()
            self.gift(s, p, kind, 1 - self.core).wait_recv()


class Scatter:
    def __init__(self, streams, own, sib, acc, sbuf, rbuf, direct, send, recv):
        self.direct = direct
        self.streams, self.own, self.sib = streams, own, sib
        self.acc, self.sbuf, self.rbuf, self.sems = acc, sbuf, rbuf, (send, recv)
        self.coords, self.core = place()

    def half(self, s):
        return self.acc[s][0].shape[1] // 2

    def dim(self, s, q):
        return order_of(self.streams[s][0])[2 - q]

    def value(self, s, q, at, n, r0):
        colour, off, width = self.streams[s]
        order = order_of(colour)
        nr = self.half(s)
        idx = list(at)
        full = sorted(order[:2 - q])
        for d, digit in zip(full, (n // SIDE, lax.rem(n, SIDE)) if len(full) == 2 else (n,)):
            idx[d] = digit
        if q == 0:
            where = (idx[0] * 16 + idx[1] * 4 + idx[2], pl.ds(r0, nr), pl.ds(off, width))
            return self.own[where] + self.sib[where].astype(jnp.float32)
        m = 0
        for d in sorted(order[:3 - q]):
            m = m * SIDE + idx[d]
        return self.acc[s][q - 1][m, pl.ds(r0, nr), :]

    def hop(self, s, q, kind):
        if q in self.direct:
            lo, n, step = ((0, 2, 1), (2, 2, 2), (4, 2, -1))[kind]
        else:
            lo, n, step = ((0, 2, 1), (2, 2, -1), (4, 1, 1), (5, 1, -1))[kind]
        to = shifted(self.coords, self.dim(s, q), step)
        return pltpu.make_async_remote_copy(
            self.sbuf[s][q].at[pl.ds(lo, n)], self.rbuf[s][q].at[pl.ds(lo, n)],
            self.sems[0].at[s, q, kind], self.sems[1].at[s, q, kind],
            device_id=device(to, self.core), device_id_type=MESH)

    def each(self, q, body):
        n = SIDE ** (2 - q)

        def step(i, carry):
            body(i)
            return carry
        lax.fori_loop(0, n, step, 0, unroll=min(n, 4))

    def one(self, s, q):
        dim, half, buf = self.dim(s, q), self.half(s), self.sbuf[s][q]
        far, right, left = (shifted(self.coords, dim, d) for d in (2, 1, -1))

        def to_right(n):
            buf[0, n] = self.value(s, q, far, n, 0).astype(buf.dtype)
            buf[1, n] = self.value(s, q, right, n, half).astype(buf.dtype)

        def to_left(n):
            buf[2, n] = self.value(s, q, far, n, half).astype(buf.dtype)
            buf[3, n] = self.value(s, q, left, n, 0).astype(buf.dtype)

        def straight(n):
            for i, at in enumerate((right, far, left)):
                for j in range(2):
                    buf[2 * i + j, n] = self.value(s, q, at, n, j * half).astype(buf.dtype)
        if q in self.direct:
            self.each(q, straight)
            for kind in range(3):
                self.hop(s, q, kind).start()
            return
        self.each(q, to_right)
        self.hop(s, q, 0).start()
        self.each(q, to_left)
        self.hop(s, q, 1).start()

    def two(self, s, q):
        if q in self.direct:
            return
        dim, half, buf, got = self.dim(s, q), self.half(s), self.sbuf[s][q], self.rbuf[s][q]
        right, left = (shifted(self.coords, dim, d) for d in (1, -1))

        def to_right(n):
            buf[4, n] = (self.value(s, q, right, n, 0) + got[0, n].astype(jnp.float32)).astype(buf.dtype)

        def to_left(n):
            buf[5, n] = (self.value(s, q, left, n, half) + got[2, n].astype(jnp.float32)).astype(buf.dtype)
        self.hop(s, q, 0).wait_recv()
        self.each(q, to_right)
        self.hop(s, q, 2).start()
        self.hop(s, q, 1).wait_recv()
        self.each(q, to_left)
        self.hop(s, q, 3).start()

    def three(self, s, q):
        half, got, acc = self.half(s), self.rbuf[s][q], self.acc[s][q]
        direct = q in self.direct
        for kind in (0, 1, 2) if direct else (2, 3):
            self.hop(s, q, kind).wait_recv()

        def keep(n):
            for r0, parts in ((0, (0, 2, 4) if direct else (3, 4)), (half, (1, 3, 5) if direct else (1, 5))):
                total = self.value(s, q, self.coords, n, r0)
                for i in parts:
                    total = total + got[i, n].astype(jnp.float32)
                acc[n, pl.ds(r0, half), :] = total
        self.each(q, keep)

    def drain(self, s, q):
        for kind in range(3 if q in self.direct else 4):
            self.hop(s, q, kind).wait_send()


def transpose_into(dst, src):
    def strip(j, carry):
        at = pl.ds(pl.multiple_of(j * CHUNK, CHUNK), CHUNK)
        dst[at, :] = src[:, at].T
        return carry
    lax.fori_loop(0, src.shape[1] // CHUNK, strip, 0)


def grad_chunk(grads_t, acts, dst, side, j):
    half = dst.shape[2]
    rhs = acts[:, pl.ds(pl.multiple_of(side * half + j * CHUNK, CHUNK), CHUNK)]
    n_rows = 512

    def strip(i, carry):
        at = pl.multiple_of(i * n_rows, n_rows)
        out = nn(grads_t[pl.ds(at, n_rows), :], rhs).astype(dst.dtype)
        dst[pl.ds(i * (n_rows // 32), n_rows // 32), :, pl.ds(j * CHUNK, CHUNK)] = out.reshape(n_rows // 32, 32, CHUNK)
        return carry
    lax.fori_loop(0, grads_t.shape[0] // n_rows, strip, 0)


def chunk_gift(src, dst, send, recv, j):
    coords, core = place()
    at = pl.ds(j * CHUNK, CHUNK)
    return pltpu.make_async_remote_copy(src.at[:, :, at], dst.at[:, :, at], send.at[j], recv.at[j],
                                        device_id=device(coords, 1 - core), device_id_type=MESH)


def wire_shapes(streams, dtype, rows, phases):
    return [pltpu.VMEM((6, SIDE ** (2 - q), rows // 2, width), dtype) for _, _, width in streams for q in phases]


def acc_shapes(streams, rows, phases):
    return [((SIDE ** (2 - q), rows, width), jnp.float32) for _, _, width in streams for q in phases]


def scatter_kernel(normed, d_qkv, w_ref, x_ref, dy_ref, inv_rms, gain, post_row, *refs):
    no = len(OUT)
    acc_in, scratch = refs[:no], refs[no + 6:]
    dx_ref, grad_q, grad_k, grad_v, grad_o, out_g = refs[no:no + 6]
    scratch = list(scratch)

    def take(n):
        head = scratch[:n]
        del scratch[:n]
        return head
    normed_t, own_q, sib_out, sib_q, own_g, sib_g, sib_in_g, out_q, out_o, w_buf, dn, pre_row = take(12)
    nq = len(QKV)
    acc_q, sbuf_q, rbuf_q = take(3 * nq), take(3 * nq), take(3 * nq)
    acc_o, sbuf_o, rbuf_o = take(2 * no), take(2 * no), take(2 * no)
    acc_g, sbuf_g, rbuf_g = take(3), take(3), take(3)
    sems = take(6)
    gift_send, gift_recv, gain_sem, fin_send, fin_recv, w_sem = take(6)
    bf, f32 = jnp.bfloat16, jnp.float32
    n_tok, dim = x_ref.shape
    strips = dim // CHUNK
    coords, core = place()
    sibling = device(coords, 1 - core)
    greet(coords, core, (1, -1, 2))

    def triples(flat):
        return [flat[3 * s:3 * s + 3] for s in range(len(flat) // 3)]

    def tails(flat, heads):
        return [[heads[s]] + flat[2 * s:2 * s + 2] for s in range(no)]
    qkv = Scatter(QKV, own_q, sib_q, triples(acc_q), triples(sbuf_q), triples(rbuf_q), (2,), *sems[0:2])
    out = Scatter(OUT, None, None, tails(acc_o, acc_in), tails(sbuf_o, (None,) * no),
                  tails(rbuf_o, (None,) * no), (2,), *sems[2:4])
    gains = Scatter(GAIN, own_g, sib_in_g, triples(acc_g), triples(sbuf_g), triples(rbuf_g), (0, 1, 2), *sems[4:6])
    gain_gift = pltpu.make_async_remote_copy(sib_g, sib_in_g, gain_sem.at[0], gain_sem.at[1],
                                             device_id=sibling, device_id_type=MESH)
    loads = [pltpu.make_async_copy(w_ref.at[pl.ds(8 * j, 8)], w_buf.at[j % 2], w_sem.at[j]) for j in range(strips)]
    loads[0].start()
    loads[1].start()
    transpose_into(normed_t, normed)
    own_g[...] = jnp.zeros_like(own_g)
    sib_g[...] = jnp.zeros_like(sib_g)
    chunks = own_q.shape[2] // CHUNK
    gifts = [chunk_gift(sib_out, sib_q, gift_send, gift_recv, j) for j in range(chunks)]
    grad_chunk(normed_t, d_qkv, sib_out, 1 - core, 0)
    greeted((1, -1, 2))
    gifts[0].start()
    for s in range(no):
        out.one(s, 1)
    ready = 0
    for j in range(chunks):
        if j + 1 < chunks:
            grad_chunk(normed_t, d_qkv, sib_out, 1 - core, j + 1)
            gifts[j + 1].start()
        grad_chunk(normed_t, d_qkv, own_q, core, j)
        gifts[j].wait_recv()
        while ready < nq and QKV[ready][1] + QKV[ready][2] <= (j + 1) * CHUNK:
            qkv.one(ready, 0)
            ready += 1
        if j == 1:
            for s in range(no):
                out.two(s, 1)
        if j == 3:
            for s in range(no):
                out.three(s, 1)
                out.one(s, 2)
    for j in range(strips):
        loads[j].wait()
        dn[:, pl.ds(j * CHUNK, CHUNK)] = nt(d_qkv[...], w_buf[j % 2].reshape(CHUNK, d_qkv.shape[1])).astype(bf)
        if j + 2 < strips:
            loads[j + 2].start()
    work = [(qkv, s) for s in range(nq)]
    for s in range(len(OUT)):
        out.two(s, 2)
    for scatter, s in work:
        scatter.two(s, 0)
    pre_row[...] = jnp.zeros_like(pre_row)
    one_gain = 1.0 + gain[pl.ds(0, 1), :]

    def back(i, carry):
        at = pl.ds(i * 32, 32)
        xs, g, inv = x_ref[at, :].astype(f32), dn[at, :].astype(f32), inv_rms[at, :]
        scaled = g * one_gain
        mean = jnp.sum(scaled * xs, axis=1, keepdims=True) * (1.0 / dim)
        dx_ref[at, :] = (dy_ref[at, :].astype(f32) + (inv * scaled - xs * (inv * inv * inv * mean))).astype(bf)
        pre_row[...] += jnp.sum((g * (xs * inv)).reshape(4, 8, dim), axis=0)
        return carry
    lax.fori_loop(0, n_tok // 32, back, 0)
    pre, post = jnp.sum(pre_row[...], axis=0, keepdims=True), post_row[...]
    own_row, sib_row = jnp.where(core == 0, pre, post), jnp.where(core == 0, post, pre)
    for j in range(16):
        for x in range(SIDE):
            own_g[SIDE * j + x, pl.ds(0, 1), :] = own_row[:, j * 128:(j + 1) * 128]
            sib_g[SIDE * j + x, pl.ds(0, 1), :] = sib_row[:, j * 128:(j + 1) * 128]
    gain_gift.start()
    for s in range(nq):
        qkv.three(s, 0)
        qkv.one(s, 1)
    gain_gift.wait_recv()
    gains.one(0, 0)
    for s in range(no):
        out.three(s, 2)
    for s in range(nq):
        qkv.two(s, 1)
    gains.three(0, 0)
    gains.one(0, 1)
    for s in range(nq):
        qkv.three(s, 1)
        qkv.one(s, 2)
    gains.three(0, 1)
    gains.one(0, 2)
    for s in range(nq):
        qkv.three(s, 2)
    gains.three(0, 2)
    fins = []
    k = 0
    for scatter, ref in ((qkv, out_q), (out, out_o), (gains, out_g)):
        for s, (_, off, width) in enumerate(scatter.streams):
            part = scatter.acc[s][2].at[0]
            ref[core, :, pl.ds(off, width)] = scatter.acc[s][2][0]
            here, there = (ref.at[side, :, pl.ds(off, width)] for side in (core, 1 - core))
            pair = [pltpu.make_async_remote_copy(part, side, fin_send.at[k], fin_recv.at[k],
                                                 device_id=sibling, device_id_type=MESH) for side in (here, there)]
            pair[0].start()
            fins.append(pair)
            k += 1
    for mine, theirs in fins:
        mine.wait_send()
        theirs.wait_recv()
    n_heads = grad_q.shape[1]
    per = out_q.shape[2] // TILE
    for h in range(n_heads + 2):
        part = out_q[h // per, :, pl.ds(h % per * TILE, TILE)]
        if h < n_heads:
            grad_q[:, h, :] = part
        else:
            (grad_k, grad_v)[h - n_heads][:, 0, :] = part
    for h in range(n_heads):
        grad_o[h] = out_o[h // 4, :, pl.ds(h % 4 * TILE, TILE)]
    for copy in gifts + [gain_gift]:
        copy.wait_send()
    for scatter, phases in ((qkv, (0, 1, 2)), (out, (1, 2)), (gains, (0, 1, 2))):
        for s in range(len(scatter.streams)):
            for q in phases:
                scatter.drain(s, q)


def scatter_grads(normed, d_qkv, w, x, dy, inv_rms, gain, post_row, accs, n_heads):
    bf, f32 = jnp.bfloat16, jnp.float32
    n_tok, model_dim = normed.shape
    half, rows = d_qkv.shape[1] // 2, 32
    blocks = model_dim // rows
    dma = pltpu.SemaphoreType.DMA
    vmem = pl.BlockSpec(memory_space=pltpu.VMEM)
    scratch = [pltpu.VMEM((model_dim, n_tok), bf), pltpu.VMEM((blocks, rows, half), f32),
               pltpu.VMEM((blocks, rows, half), bf), pltpu.VMEM((blocks, rows, half), bf)]
    scratch += [pltpu.VMEM((blocks, 16, 128), f32)] * 3
    scratch += [pltpu.VMEM((2, rows, half), f32), pltpu.VMEM((2, rows, 1024), f32),
                pltpu.VMEM((2, CHUNK // rows, rows, 2 * half), bf), pltpu.VMEM((n_tok, model_dim), bf),
                pltpu.VMEM((8, model_dim), f32)]
    for streams, dtype, n_rows, phases in ((QKV, bf, rows, (0, 1, 2)), (OUT, bf, rows, (1, 2)), (GAIN, f32, 16, (0, 1, 2))):
        scratch += [pltpu.VMEM(*a) for a in acc_shapes(streams, n_rows, phases)]
        scratch += wire_shapes(streams, dtype, n_rows, phases) * 2
    scratch += [dma((len(st), 3, 4)) for st in (QKV, OUT, GAIN) for _ in range(2)]
    scratch += [dma((half // CHUNK,))] * 2 + [dma((2,))] + [dma((len(QKV) + len(OUT) + 1,))] * 2 + [dma((model_dim // CHUNK,))]
    return pl.pallas_call(
        scatter_kernel, name="scatter_grads",
        out_shape=[jax.ShapeDtypeStruct((n_tok, model_dim), bf), jax.ShapeDtypeStruct((rows, n_heads, TILE), f32),
                   jax.ShapeDtypeStruct((rows, 1, TILE), f32), jax.ShapeDtypeStruct((rows, 1, TILE), f32),
                   jax.ShapeDtypeStruct((n_heads, rows, TILE), f32), jax.ShapeDtypeStruct((2, 16, 128), f32)],
        in_specs=[vmem] * 2 + [pl.BlockSpec(memory_space=pltpu.HBM)] + [vmem] * (5 + len(OUT)), out_specs=[vmem] * 6,
        scratch_shapes=scratch,
        compiler_params=pltpu.CompilerParams(collective_id=2, has_side_effects=True, vmem_limit_bytes=62914560),
    )(normed, d_qkv, w, x, dy, inv_rms, gain, post_row, *accs)


LOG2E = 1.4426950408889634
TILE = 256


def nt(a, b):
    return lax.dot_general(a, b, (((1,), (1,)), ((), ())), preferred_element_type=jnp.float32)


def nn(a, b):
    return lax.dot_general(a, b, (((1,), (0,)), ((), ())), preferred_element_type=jnp.float32)


def fill_mask(mask, pos):
    n_keys, n_q = mask.shape
    core = lax.axis_index('cp')
    for c in range(n_keys // TILE):
        base = jnp.where(c < n_q // TILE, (1 - core) * n_q, core * n_q - n_q) + c * TILE
        for i in range(n_q // TILE):
            k_at = base + lax.broadcasted_iota(jnp.int32, (TILE, TILE), 0)
            q_at = core * n_q + i * TILE + lax.broadcasted_iota(jnp.int32, (TILE, TILE), 1)
            seen = (k_at <= q_at) & (k_at >= q_at - pos[:, pl.ds(i * TILE, TILE)])
            mask[pl.ds(c * TILE, TILE), pl.ds(i * TILE, TILE)] = jnp.where(seen, 1.0, 0.0)


def keys_for(i, n_q):
    return n_q + (i + 1) * TILE


def forward_kernel(ratio, x_ref, cos_ref, sin_ref, pos, in0, in1, in2,
                   wq_out, wo_out, gain_out, normed, inv_rms, q_ref, kv_ref, o_ref, inv_ref,
                   wq, gains, gain_row, mask, v_t, w_scr, p_scr, *sems):
    n_q, dim = x_ref.shape
    bf, f32 = jnp.bfloat16, jnp.float32
    coords, core = place()
    sibling = device(coords, 1 - core)
    greet(coords, core, (1, -1, 2))
    own_sem, swap_send, swap_recv = sems[12:15]
    qkv, out, gain = (Gather(st, src, dst, direct, *sems[4 * g:4 * g + 4]) for g, (st, src, dst, direct) in enumerate(
        ((QKV, in0, wq, (0,)), (OUT, in1, wo_out, (0,)), (GAIN, in2, gains, (0, 1, 2)))))
    nq = range(len(QKV))
    wq[coords[0], coords[1], coords[2]] = in0[...]
    gains[coords[0], coords[1], coords[2]] = in2[...]
    greeted((1, -1, 2))
    gain.start(0, 0)
    for s in nq:
        qkv.start(s, 0)
    for s in range(len(OUT)):
        out.start(s, 0)
    own_out = pltpu.make_async_copy(in1, wo_out.at[coords[0], coords[1], coords[2]], own_sem.at[0])
    own_out.start()

    def stats(i, carry):
        at = pl.ds(i * 64, 64)
        v = x_ref[at, :].astype(f32)
        inv_rms[at, :] = lax.rsqrt(jnp.sum(v * v, axis=1, keepdims=True) * (1.0 / dim) + NORM_EPS)
        return carry
    lax.fori_loop(0, n_q // 64, stats, 0)
    gain.middle(0, 0)
    gain.start(0, 1)
    for s in nq:
        qkv.middle(s, 0)
        qkv.start(s, 1)
    gain.middle(0, 1)
    gain.start(0, 2)
    for s in range(len(OUT)):
        out.middle(s, 0)
    own_out.wait()
    for s in nq:
        qkv.middle(s, 1)
    for s in range(len(OUT)):
        out.start(s, 1)
    gain.middle(0, 2)
    for s in nq:
        qkv.finish(s, 1)
        qkv.start(s, 2)
    for p in range(3):
        gain.drain(0, p)
    for kind in range(2):
        for j in range(16):
            row = sum(gains[j // 4, j % 4, x, pl.ds(0, 1), pl.ds(kind * 128, 128)] for x in range(SIDE))
            gain_row[pl.ds(kind, 1), pl.ds(j * 128, 128)] = row
    gain_out[...] = gain_row[...]
    fill_mask(mask, pos)

    def scale(i, carry):
        at = pl.ds(i * 64, 64)
        normed[at, :] = (x_ref[at, :].astype(f32) * inv_rms[at, :] * (1.0 + gain_row[pl.ds(0, 1), :])).astype(bf)
        return carry
    lax.fori_loop(0, n_q // 64, scale, 0)
    for s in nq:
        qkv.middle(s, 2)
    for s in range(len(OUT)):
        out.middle(s, 1)
    for s in nq:
        qkv.finish(s, 2)
    for s in range(len(OUT)):
        out.finish(s, 1)
        out.start(s, 2)
    for s in nq:
        for p in range(3):
            qkv.drain(s, p)
    keep = pltpu.make_async_copy(wq, wq_out, own_sem.at[1])
    keep.start()

    def project(n):
        rhs = wq[:, :, :, :, pl.ds(pl.multiple_of(n * TILE, TILE), TILE)].reshape(dim, TILE)
        return nn(normed[...], rhs).astype(bf)

    def rope(u):
        lo, hi = u[:, :TILE // 2].astype(f32), u[:, TILE // 2:].astype(f32)
        c, s = cos_ref[...], sin_ref[...]
        return jnp.concatenate([lo * c - hi * s, hi * c + lo * s], axis=1).astype(bf)
    n_heads = q_ref.shape[1] // TILE
    mine, other = pl.ds(n_q, n_q), pl.ds(0, n_q)
    kv_ref[mine, pl.ds(0, TILE)] = rope(project(n_heads))
    kv_ref[mine, pl.ds(TILE, TILE)] = project(n_heads + 1)
    swap = pltpu.make_async_remote_copy(kv_ref.at[mine], kv_ref.at[other], swap_send.at[0], swap_recv.at[0],
                                        device_id=sibling, device_id_type=MESH)
    swap.start()

    def project_head(h, carry):
        q_ref[:, pl.ds(pl.multiple_of(h * TILE, TILE), TILE)] = rope(project(h))
        return carry
    lax.fori_loop(0, n_heads, project_head, 0)
    for s in range(len(OUT)):
        out.middle(s, 2)
    swap.wait_recv()
    k_cols = pl.ds(0, TILE)
    v_t[...] = kv_ref[:, pl.ds(TILE, TILE)].T

    def head(h, carry):
        cols = pl.ds(pl.multiple_of(h * TILE, TILE), TILE)
        for i in range(n_q // TILE):
            qi = q_ref[pl.ds(i * TILE, TILE), cols]
            n_keys = keys_for(i, n_q)
            total = jnp.zeros((8, TILE), f32)
            for c in range(n_keys // TILE):
                t = jnp.tanh(nt(kv_ref[pl.ds(c * TILE, TILE), k_cols], qi) * ratio)
                w = jnp.exp2(t * (SOFT_CAP * LOG2E)) * mask[pl.ds(c * TILE, TILE), pl.ds(i * TILE, TILE)]
                w_scr[i, pl.ds(c * TILE, TILE), :] = w
                total = total + jnp.sum(w.reshape(TILE // 8, 8, TILE), axis=0)
            inv = 1.0 / jnp.sum(total, axis=0, keepdims=True)
            inv_ref[h, :, pl.ds(i * TILE, TILE)] = inv
            p_scr[i, pl.ds(0, n_keys), :] = (w_scr[i, pl.ds(0, n_keys), :] * inv).astype(bf)
            o_t = nn(v_t[:, pl.ds(0, n_keys)], p_scr[i, pl.ds(0, n_keys), :])
            o_ref[pl.ds(i * TILE, TILE), cols] = o_t.T.astype(bf)
        return carry
    lax.fori_loop(0, n_heads, head, 0)
    for s in range(len(OUT)):
        out.finish(s, 2)
    for s in range(len(OUT)):
        for p in range(3):
            out.drain(s, p)
    swap.wait_send()
    keep.wait()


def forward(x, cos_t, sin_t, pos, w0, w1, w2, n_heads, ratio):
    n_q, dim = x.shape
    n_k = 2 * n_q
    bf, f32 = jnp.bfloat16, jnp.float32
    dma = pltpu.SemaphoreType.DMA
    vmem, hbm = pl.BlockSpec(memory_space=pltpu.VMEM), pl.BlockSpec(memory_space=pltpu.HBM)
    grid = (SIDE, SIDE, SIDE)
    shape = jax.ShapeDtypeStruct
    tiles = n_q // TILE
    return pl.pallas_call(
        functools.partial(forward_kernel, ratio), name="forward",
        out_shape=[shape(grid + w0.shape, bf), shape(grid + w1.shape, bf), shape((2, dim), f32), shape((n_q, dim), bf),
                   shape((n_q, 1), f32), shape((n_q, n_heads * TILE), bf), shape((n_k, 2 * TILE), bf),
                   shape((n_q, n_heads * TILE), bf), shape((n_heads, 1, n_q), f32)],
        in_specs=[vmem] * 7, out_specs=[hbm] * 2 + [vmem] * 7,
        scratch_shapes=[pltpu.VMEM(grid + w0.shape, bf), pltpu.VMEM(grid + w2.shape, f32), pltpu.VMEM((2, dim), f32),
                        pltpu.VMEM((n_k, n_q), f32), pltpu.VMEM((TILE, n_k), bf),
                        pltpu.VMEM((tiles, n_k, TILE), f32), pltpu.VMEM((tiles, n_k, TILE), bf)]
        + [dma((len(st), 3, 4)) for st in (QKV, OUT, GAIN) for _ in range(4)]
        + [dma((2,)), dma((1,)), dma((1,))],
        compiler_params=pltpu.CompilerParams(collective_id=1, has_side_effects=True, vmem_limit_bytes=35651584),
    )(x, cos_t, sin_t, pos, w0, w1, w2)


def attend_back_kernel(ratio, q_ref, do_ref, kv_ref, pos, inv_ref, dz_ref, o_ref, cos_ref, sin_ref,
                       dqkv_ref, *refs):
    no = len(OUT)
    accs = refs[:no]
    (mask, k_t, g_scr, dp_scr, p_scr, ds_scr, dk_acc, dv_acc, dkv_out, dkv_in, dz_t, own, sib_out, sib_in,
     *scratch) = refs[no:]
    n_q = q_ref.shape[0]
    coords, core = place()
    greet(coords, core)
    sbuf, rbuf, sems = scratch[:no], scratch[no:2 * no], scratch[2 * no:2 * no + 2]
    gift_send, gift_recv, swap_sem = scratch[2 * no + 2:]
    bf, f32 = jnp.bfloat16, jnp.float32
    swap = pltpu.make_async_remote_copy(dkv_out, dkv_in, swap_sem.at[0], swap_sem.at[1],
                                        device_id=device(coords, 1 - core), device_id_type=MESH)

    def rope_back(u):
        lo, hi = u[:, :TILE // 2].astype(f32), u[:, TILE // 2:].astype(f32)
        c, s = cos_ref[pl.ds(0, u.shape[0]), :], sin_ref[pl.ds(0, u.shape[0]), :]
        return jnp.concatenate([lo * c + hi * s, hi * c - lo * s], axis=1).astype(bf)
    out = Scatter(OUT, own, sib_in, [[a] for a in accs], [[b] for b in sbuf], [[b] for b in rbuf], (), *sems)
    chunks = own.shape[2] // CHUNK
    transpose_into(dz_t, dz_ref)
    gifts = [chunk_gift(sib_out, sib_in, gift_send, gift_recv, j) for j in range(chunks)]
    grad_chunk(dz_t, o_ref, sib_out, 1 - core, 0)
    greeted()
    gifts[0].start()
    ready = 0
    for j in range(chunks):
        if j + 1 < chunks:
            grad_chunk(dz_t, o_ref, sib_out, 1 - core, j + 1)
            gifts[j + 1].start()
        grad_chunk(dz_t, o_ref, own, core, j)
        gifts[j].wait_recv()
        while ready < no and OUT[ready][1] + OUT[ready][2] <= (j + 1) * CHUNK:
            out.one(ready, 0)
            ready += 1
    fill_mask(mask, pos)
    k_cols, v_cols = pl.ds(0, TILE), pl.ds(TILE, TILE)
    k_t[...] = kv_ref[:, k_cols].T
    dk_acc[...] = jnp.zeros_like(dk_acc)
    dv_acc[...] = jnp.zeros_like(dv_acc)

    def head(h, carry):
        cols = pl.ds(pl.multiple_of(h * TILE, TILE), TILE)
        for i in range(n_q // TILE):
            rows = pl.ds(i * TILE, TILE)
            qi, doi = q_ref[rows, cols], do_ref[rows, cols]
            inv = inv_ref[h, :, rows]
            n_keys = keys_for(i, n_q)
            total = jnp.zeros((8, TILE), jnp.float32)
            for c in range(n_keys // TILE):
                at = pl.ds(c * TILE, TILE)
                t = jnp.tanh(nt(kv_ref[at, k_cols], qi) * ratio)
                p = jnp.exp2(t * (SOFT_CAP * LOG2E)) * (mask[at, rows] * inv)
                dp = nt(kv_ref[at, v_cols], doi)
                p_scr[i, at, :] = p.astype(jnp.bfloat16)
                g_scr[i, at, :] = p * ((1.0 - t * t) * (ratio * SOFT_CAP))
                dp_scr[i, at, :] = dp
                total = total + jnp.sum((p * dp).reshape(TILE // 8, 8, TILE), axis=0)
            row_dot = jnp.sum(total, axis=0, keepdims=True)
            seen = pl.ds(0, n_keys)
            ds_scr[i, seen, :] = ((dp_scr[i, seen, :] - row_dot) * g_scr[i, seen, :]).astype(jnp.bfloat16)
            dq_t = nn(k_t[:, seen], ds_scr[i, seen, :])
            dq = dq_t.T.astype(bf)
            lo, hi = dq[:, :TILE // 2].astype(f32), dq[:, TILE // 2:].astype(f32)
            cos, sin = cos_ref[rows, :], sin_ref[rows, :]
            dqkv_ref[rows, cols] = jnp.concatenate([lo * cos + hi * sin, hi * cos - lo * sin], axis=1).astype(bf)
            dk_acc[seen, :] += nn(ds_scr[i, seen, :], qi)
            dv_acc[seen, :] += nn(p_scr[i, seen, :], doi)

        @pl.when(h == 3)
        def _():
            for s in range(no):
                out.two(s, 0)

        @pl.when(h == 6)
        def _():
            for s in range(no):
                out.three(s, 0)
        return carry
    lax.fori_loop(0, q_ref.shape[1] // TILE, head, 0)
    mine, other = pl.ds(n_q, n_q), pl.ds(0, n_q)
    dkv_out[:, k_cols] = dk_acc[other, :].astype(bf)
    dkv_out[:, v_cols] = dv_acc[other, :].astype(bf)
    swap.start()
    swap.wait_recv()
    q_cols = q_ref.shape[1]
    dqkv_ref[:, pl.ds(q_cols, TILE)] = rope_back((dk_acc[mine, :] + dkv_in[:, k_cols].astype(f32)).astype(bf))
    dqkv_ref[:, pl.ds(q_cols + TILE, TILE)] = (dv_acc[mine, :] + dkv_in[:, v_cols].astype(f32)).astype(bf)
    for s in range(len(OUT)):
        out.drain(s, 0)
    for copy in gifts + [swap]:
        copy.wait_send()


def attend_back(q, do, kv, pos, inv_sum, dz, o, cos_t, sin_t, ratio):
    n_q, n_k = q.shape[0], kv.shape[0]
    vmem = pl.BlockSpec(memory_space=pltpu.VMEM)
    tiles = n_q // TILE
    bf, f32 = jnp.bfloat16, jnp.float32
    return pl.pallas_call(
        functools.partial(attend_back_kernel, ratio), name="attend_back",
        out_shape=[jax.ShapeDtypeStruct((n_q, q.shape[1] + 2 * TILE), bf)]
        + [jax.ShapeDtypeStruct(*a) for a in acc_shapes(OUT, 32, (0,))],
        in_specs=[vmem] * 9, out_specs=[vmem] * (1 + len(OUT)),
        scratch_shapes=[pltpu.VMEM((n_k, n_q), f32), pltpu.VMEM((TILE, n_k), bf),
                        pltpu.VMEM((tiles, n_k, TILE), f32), pltpu.VMEM((tiles, n_k, TILE), f32),
                        pltpu.VMEM((tiles, n_k, TILE), bf), pltpu.VMEM((tiles, n_k, TILE), bf),
                        pltpu.VMEM((n_k, TILE), f32), pltpu.VMEM((n_k, TILE), f32),
                        pltpu.VMEM((n_q, 2 * TILE), bf), pltpu.VMEM((n_q, 2 * TILE), bf),
                        pltpu.VMEM((dz.shape[1], n_q), bf), pltpu.VMEM((dz.shape[1] // 32, 32, o.shape[1] // 2), f32)]
        + [pltpu.VMEM((dz.shape[1] // 32, 32, o.shape[1] // 2), bf)] * 2
        + wire_shapes(OUT, bf, 32, (0,)) * 2 + [pltpu.SemaphoreType.DMA((len(OUT), 3, 4))] * 2
        + [pltpu.SemaphoreType.DMA((o.shape[1] // 2 // CHUNK,))] * 2 + [pltpu.SemaphoreType.DMA((2,))],
        compiler_params=pltpu.CompilerParams(collective_id=4, has_side_effects=True, vmem_limit_bytes=50331648),
    )(q, do, kv, pos, inv_sum, dz, o, cos_t, sin_t)


def rope_tables(pos_ids, head_dim):
    half_dim = head_dim // 2
    inv_freq = ROPE_BASE ** (-2.0 * jnp.arange(half_dim, dtype=jnp.float32) / head_dim)
    angles = pos_ids.astype(jnp.float32)[..., None] * inv_freq
    return jnp.cos(angles)[..., None, :], jnp.sin(angles)[..., None, :]


def rotate(values, cos_t, sin_t):
    half_dim = values.shape[-1] // 2
    first_half = values[..., :half_dim].astype(jnp.float32)
    second_half = values[..., half_dim:].astype(jnp.float32)
    rotated = jnp.concatenate([first_half * cos_t - second_half * sin_t,
                               second_half * cos_t + first_half * sin_t], axis=-1)
    return rotated.astype(jnp.bfloat16)


def norm_forward(values, gain_vec):
    values_f = values.astype(jnp.float32)
    inv_rms = lax.rsqrt(jnp.mean(values_f * values_f, axis=-1, keepdims=True) + NORM_EPS)
    normed = values_f * inv_rms * (1.0 + gain_vec.astype(jnp.float32))
    return normed.astype(jnp.bfloat16), inv_rms


def norm_backward(values, inv_rms, gain_vec, grads):
    values_f = values.astype(jnp.float32)
    grads_f = grads.astype(jnp.float32)
    scaled = grads_f * (1.0 + gain_vec.astype(jnp.float32))
    d_values = inv_rms * scaled - values_f * inv_rms ** 3 * jnp.mean(scaled * values_f, axis=-1, keepdims=True)
    d_gain = jnp.sum(grads_f * values_f * inv_rms, axis=0)
    return d_values, d_gain


def dot(a, b, dims):
    return lax.dot_general(a, b, ((dims[:1], dims[1:]), ((), ())), preferred_element_type=jnp.float32)


def solution(mesh):
    tok_spec = P('fsdp', 'cp', None)
    ids_spec = P('fsdp', 'cp')
    in_spec = P('fsdp', None, None)
    out_spec = P(None, None, 'fsdp')
    gain_spec = P('fsdp')
    bf, f32 = jnp.bfloat16, jnp.float32

    def layer_local(hidden, doc_ids, doc_pos, grad_out, w_query, w_key, w_value, w_out, gain_pre, gain_post):
        _, n_tok, model_dim = hidden.shape
        hidden, grad_out = hidden[0], grad_out[0]
        n_heads, head_dim = w_query.shape[1], w_query.shape[2]
        rows = w_query.shape[0]
        q_cols = n_heads * head_dim
        w0 = jnp.concatenate([w_query.reshape(rows, q_cols), w_key.reshape(rows, head_dim),
                              w_value.reshape(rows, head_dim)], axis=1)
        w1 = w_out.reshape(q_cols, rows).T
        lane = lax.rem(lax.axis_index('fsdp'), SIDE) * rows
        w2 = jnp.zeros((8, 256), f32)
        for kind, g in enumerate((gain_pre, gain_post)):
            w2 = lax.dynamic_update_slice(w2, g.astype(f32)[None], (0, kind * 128 + lane))
        cos_t, sin_t = rope_tables(doc_pos[0], head_dim)
        q_scale = (head_dim if head_dim >= 256 else model_dim // n_heads) ** -0.5
        ratio = q_scale / SOFT_CAP
        wqkv, wo_t, gains, normed, inv_pre, q_flat, kv_all, attn_flat, inv_sum = forward(
            hidden, cos_t[:, 0], sin_t[:, 0], doc_pos, w0, w1, w2, n_heads, ratio)
        post_full = gains[1]
        wqkv = wqkv.reshape(model_dim // rows, rows, q_cols + 2 * head_dim)
        wo_t = wo_t.reshape(model_dim, q_cols)
        proj_out = dot(attn_flat, wo_t, (1, 1)).astype(bf)
        post_out, inv_post = norm_forward(proj_out, post_full)
        out_hidden = (hidden.astype(f32) + post_out.astype(f32)).astype(bf)

        d_proj, d_gain_post = norm_backward(proj_out, inv_post, post_full, grad_out)
        d_proj = d_proj.astype(bf)
        d_attn = dot(d_proj, wo_t, (1, 0)).astype(bf)

        d_qkv, *accs = attend_back(q_flat, d_attn, kv_all, doc_pos, inv_sum, d_proj, attn_flat, cos_t[:, 0], sin_t[:, 0], ratio)
        dx, g_q, g_k, g_v, g_o, g_g = scatter_grads(normed, d_qkv, wqkv, hidden, grad_out, inv_pre, gains,
                                                    d_gain_post[None], accs, n_heads)
        g_g = lax.dynamic_slice(g_g, (0, 0, lane), (2, 1, rows))[:, 0]
        return (out_hidden[None], dx[None], g_q, g_k, g_v, g_o.transpose(0, 2, 1),
                g_g[0], g_g[1])

    return jax.shard_map(layer_local, mesh=mesh,
                         in_specs=(tok_spec, ids_spec, ids_spec, tok_spec, in_spec, in_spec, in_spec, out_spec, gain_spec, gain_spec),
                         out_specs=(tok_spec, tok_spec, in_spec, in_spec, in_spec, out_spec, gain_spec, gain_spec),
                         check_vma=False)
```

```python
import functools

import jax
import jax.numpy as jnp
from jax import lax
from jax.experimental import pallas as pl
from jax.experimental.pallas import tpu as pltpu
from jax.sharding import PartitionSpec as P

SOFT_CAP = 50.0
NORM_EPS = 1e-6
ROPE_BASE = 10000.0
MESH = pl.DeviceIdType.MESH
SIDE = 4

QKV = ((0, 0, 256), (1, 256, 256), (2, 512, 256), (0, 768, 256), (1, 1024, 128), (2, 1152, 128))
OUT = ((0, 0, 256), (1, 256, 256), (2, 512, 256), (1, 768, 128), (2, 896, 128))
GAIN = ((0, 0, 128),)
CHUNK = 256


def place():
    f = lax.axis_index('fsdp')
    return (f // 16, lax.rem(f // 4, 4), lax.rem(f, 4)), lax.axis_index('cp')


def shifted(coords, dim, delta):
    out = list(coords)
    out[dim] = lax.rem(coords[dim] + delta + SIDE, SIDE)
    return tuple(out)


def device(coords, core):
    return (coords[0] * 16 + coords[1] * 4 + coords[2], core)


def greet(coords, core, steps=(1, -1)):
    barrier = pltpu.get_barrier_semaphore()
    for dim in range(3):
        for delta in steps:
            pl.semaphore_signal(barrier, inc=1, device_id=device(shifted(coords, dim, delta), core), device_id_type=MESH)
    pl.semaphore_signal(barrier, inc=1, device_id=device(coords, 1 - core), device_id_type=MESH)


def greeted(steps=(1, -1)):
    pl.semaphore_wait(pltpu.get_barrier_semaphore(), 3 * len(steps) + 1)


def order_of(colour):
    return tuple((colour + i) % 3 for i in range(3))


def region(ref, full, coords, rows, cols):
    idx = [pl.ds(0, SIDE) if d in full else coords[d] for d in range(3)]
    return ref.at[idx[0], idx[1], idx[2], pl.ds(*rows), pl.ds(*cols)]


class Gather:
    def __init__(self, streams, src, out, direct, send, recv, sib_send, sib_recv):
        self.streams, self.src, self.out, self.direct = streams, src, out, direct
        self.sems = (send, recv, sib_send, sib_recv)
        self.coords, self.core = place()
        self.rows = out.shape[3]

    def cols(self, s, side):
        _, off, width = self.streams[s]
        return pl.ds(pl.multiple_of(side * (self.out.shape[4] // 2) + off, 128), width)

    def part(self, s, p, kind, at, side):
        full = order_of(self.streams[s][0])[:p]
        idx = [pl.ds(0, SIDE) if d in full else at[d] for d in range(3)]
        half = self.rows // 2
        r0, nr = (0, self.rows) if kind < 2 or p in self.direct else ((kind - 2) * half, half)
        return self.out.at[idx[0], idx[1], idx[2], pl.ds(r0, nr), self.cols(s, side)]

    def hop(self, s, p, kind):
        dim = order_of(self.streams[s][0])[p]
        direct = p in self.direct
        at = shifted(self.coords, dim, 0 if direct else (0, 0, -1, 1)[kind])
        to = shifted(self.coords, dim, (1, -1, 2 if direct else 1, -1)[kind])
        dst = self.part(s, p, kind, at, self.core)
        src = self.src.at[:, self.cols(s, self.core)] if p == 0 and (direct or kind < 2) else dst
        return pltpu.make_async_remote_copy(src, dst, self.sems[0].at[s, p, kind], self.sems[1].at[s, p, kind],
                                            device_id=device(to, self.core), device_id_type=MESH)

    def landed(self, s, p, kind, side):
        dim = order_of(self.streams[s][0])[p]
        return self.part(s, p, kind, shifted(self.coords, dim, (-1, 1, -2, 2)[kind]), side)

    def gift(self, s, p, kind, side):
        here = self.landed(s, p, kind, side)
        return pltpu.make_async_remote_copy(here, here, self.sems[2].at[s, p, kind], self.sems[3].at[s, p, kind],
                                            device_id=device(self.coords, 1 - self.core), device_id_type=MESH)

    def arrive(self, s, p, kind):
        here = self.landed(s, p, kind, self.core)
        pltpu.make_async_remote_copy(here, here, self.sems[0].at[s, p, kind], self.sems[1].at[s, p, kind],
                                     device_id=device(self.coords, 1 - self.core), device_id_type=MESH).wait_recv()

    def start(self, s, p):
        self.hop(s, p, 0).start()
        self.hop(s, p, 1).start()
        if p in self.direct:
            self.hop(s, p, 2).start()

    def middle(self, s, p):
        if p in self.direct:
            for kind in range(3):
                self.arrive(s, p, kind)
                self.gift(s, p, kind, self.core).start()
            return
        for kind in (0, 1):
            self.arrive(s, p, kind)
            self.hop(s, p, kind + 2).start()
            self.gift(s, p, kind, self.core).start()

    def finish(self, s, p):
        for kind in () if p in self.direct else (2, 3):
            self.arrive(s, p, kind)
            self.gift(s, p, kind, self.core).start()

    def drain(self, s, p):
        for kind in range(3 if p in self.direct else 4):
            self.hop(s, p, kind).wait_send()
            self.gift(s, p, kind, self.core).wait_send()
            self.gift(s, p, kind, 1 - self.core).wait_recv()


class Scatter:
    def __init__(self, streams, own, sib, acc, sbuf, rbuf, direct, send, recv):
        self.direct = direct
        self.streams, self.own, self.sib = streams, own, sib
        self.acc, self.sbuf, self.rbuf, self.sems = acc, sbuf, rbuf, (send, recv)
        self.coords, self.core = place()

    def half(self, s):
        return self.acc[s][0].shape[1] // 2

    def dim(self, s, q):
        return order_of(self.streams[s][0])[2 - q]

    def value(self, s, q, at, n, r0):
        colour, off, width = self.streams[s]
        order = order_of(colour)
        nr = self.half(s)
        idx = list(at)
        full = sorted(order[:2 - q])
        for d, digit in zip(full, (n // SIDE, lax.rem(n, SIDE)) if len(full) == 2 else (n,)):
            idx[d] = digit
        if q == 0:
            where = (idx[0] * 16 + idx[1] * 4 + idx[2], pl.ds(r0, nr), pl.ds(off, width))
            return self.own[where] + self.sib[where].astype(jnp.float32)
        m = 0
        for d in sorted(order[:3 - q]):
            m = m * SIDE + idx[d]
        return self.acc[s][q - 1][m, pl.ds(r0, nr), :]

    def hop(self, s, q, kind):
        if q in self.direct:
            lo, n, step = ((0, 2, 1), (2, 2, 2), (4, 2, -1))[kind]
        else:
            lo, n, step = ((0, 2, 1), (2, 2, -1), (4, 1, 1), (5, 1, -1))[kind]
        to = shifted(self.coords, self.dim(s, q), step)
        return pltpu.make_async_remote_copy(
            self.sbuf[s][q].at[pl.ds(lo, n)], self.rbuf[s][q].at[pl.ds(lo, n)],
            self.sems[0].at[s, q, kind], self.sems[1].at[s, q, kind],
            device_id=device(to, self.core), device_id_type=MESH)

    def each(self, q, body):
        n = SIDE ** (2 - q)

        def step(i, carry):
            body(i)
            return carry
        lax.fori_loop(0, n, step, 0, unroll=min(n, 4))

    def one(self, s, q):
        dim, half, buf = self.dim(s, q), self.half(s), self.sbuf[s][q]
        far, right, left = (shifted(self.coords, dim, d) for d in (2, 1, -1))

        def to_right(n):
            buf[0, n] = self.value(s, q, far, n, 0).astype(buf.dtype)
            buf[1, n] = self.value(s, q, right, n, half).astype(buf.dtype)

        def to_left(n):
            buf[2, n] = self.value(s, q, far, n, half).astype(buf.dtype)
            buf[3, n] = self.value(s, q, left, n, 0).astype(buf.dtype)

        def straight(n):
            for i, at in enumerate((right, far, left)):
                for j in range(2):
                    buf[2 * i + j, n] = self.value(s, q, at, n, j * half).astype(buf.dtype)
        if q in self.direct:
            self.each(q, straight)
            for kind in range(3):
                self.hop(s, q, kind).start()
            return
        self.each(q, to_right)
        self.hop(s, q, 0).start()
        self.each(q, to_left)
        self.hop(s, q, 1).start()

    def two(self, s, q):
        if q in self.direct:
            return
        dim, half, buf, got = self.dim(s, q), self.half(s), self.sbuf[s][q], self.rbuf[s][q]
        right, left = (shifted(self.coords, dim, d) for d in (1, -1))

        def to_right(n):
            buf[4, n] = (self.value(s, q, right, n, 0) + got[0, n].astype(jnp.float32)).astype(buf.dtype)

        def to_left(n):
            buf[5, n] = (self.value(s, q, left, n, half) + got[2, n].astype(jnp.float32)).astype(buf.dtype)
        self.hop(s, q, 0).wait_recv()
        self.each(q, to_right)
        self.hop(s, q, 2).start()
        self.hop(s, q, 1).wait_recv()
        self.each(q, to_left)
        self.hop(s, q, 3).start()

    def three(self, s, q):
        half, got, acc = self.half(s), self.rbuf[s][q], self.acc[s][q]
        direct = q in self.direct
        for kind in (0, 1, 2) if direct else (2, 3):
            self.hop(s, q, kind).wait_recv()

        def keep(n):
            for r0, parts in ((0, (0, 2, 4) if direct else (3, 4)), (half, (1, 3, 5) if direct else (1, 5))):
                total = self.value(s, q, self.coords, n, r0)
                for i in parts:
                    total = total + got[i, n].astype(jnp.float32)
                acc[n, pl.ds(r0, half), :] = total
        self.each(q, keep)

    def drain(self, s, q):
        for kind in range(3 if q in self.direct else 4):
            self.hop(s, q, kind).wait_send()


def transpose_into(dst, src):
    def strip(j, carry):
        at = pl.ds(pl.multiple_of(j * CHUNK, CHUNK), CHUNK)
        dst[at, :] = src[:, at].T
        return carry
    lax.fori_loop(0, src.shape[1] // CHUNK, strip, 0)


def grad_chunk(grads_t, acts, dst, side, j):
    half = dst.shape[2]
    rhs = acts[:, pl.ds(pl.multiple_of(side * half + j * CHUNK, CHUNK), CHUNK)]
    n_rows = 512

    def strip(i, carry):
        at = pl.multiple_of(i * n_rows, n_rows)
        out = nn(grads_t[pl.ds(at, n_rows), :], rhs).astype(dst.dtype)
        dst[pl.ds(i * (n_rows // 32), n_rows // 32), :, pl.ds(j * CHUNK, CHUNK)] = out.reshape(n_rows // 32, 32, CHUNK)
        return carry
    lax.fori_loop(0, grads_t.shape[0] // n_rows, strip, 0)


def chunk_gift(src, dst, send, recv, j):
    coords, core = place()
    at = pl.ds(j * CHUNK, CHUNK)
    return pltpu.make_async_remote_copy(src.at[:, :, at], dst.at[:, :, at], send.at[j], recv.at[j],
                                        device_id=device(coords, 1 - core), device_id_type=MESH)


def wire_shapes(streams, dtype, rows, phases):
    return [pltpu.VMEM((6, SIDE ** (2 - q), rows // 2, width), dtype) for _, _, width in streams for q in phases]


def acc_shapes(streams, rows, phases):
    return [((SIDE ** (2 - q), rows, width), jnp.float32) for _, _, width in streams for q in phases]


def scatter_kernel(normed, d_qkv, w_ref, x_ref, dy_ref, inv_rms, gain, post_row, *refs):
    no = len(OUT)
    acc_in, scratch = refs[:no], refs[no + 6:]
    dx_ref, grad_q, grad_k, grad_v, grad_o, out_g = refs[no:no + 6]
    scratch = list(scratch)

    def take(n):
        head = scratch[:n]
        del scratch[:n]
        return head
    normed_t, own_q, sib_out, sib_q, own_g, sib_g, sib_in_g, out_q, out_o, w_buf, dn, pre_row = take(12)
    nq = len(QKV)
    acc_q, sbuf_q, rbuf_q = take(3 * nq), take(3 * nq), take(3 * nq)
    acc_o, sbuf_o, rbuf_o = take(2 * no), take(2 * no), take(2 * no)
    acc_g, sbuf_g, rbuf_g = take(3), take(3), take(3)
    sems = take(6)
    gift_send, gift_recv, gain_sem, fin_send, fin_recv, w_sem = take(6)
    bf, f32 = jnp.bfloat16, jnp.float32
    n_tok, dim = x_ref.shape
    strips = dim // CHUNK
    coords, core = place()
    sibling = device(coords, 1 - core)
    greet(coords, core, (1, -1, 2))

    def triples(flat):
        return [flat[3 * s:3 * s + 3] for s in range(len(flat) // 3)]

    def tails(flat, heads):
        return [[heads[s]] + flat[2 * s:2 * s + 2] for s in range(no)]
    qkv = Scatter(QKV, own_q, sib_q, triples(acc_q), triples(sbuf_q), triples(rbuf_q), (2,), *sems[0:2])
    out = Scatter(OUT, None, None, tails(acc_o, acc_in), tails(sbuf_o, (None,) * no),
                  tails(rbuf_o, (None,) * no), (2,), *sems[2:4])
    gains = Scatter(GAIN, own_g, sib_in_g, triples(acc_g), triples(sbuf_g), triples(rbuf_g), (0, 1, 2), *sems[4:6])
    gain_gift = pltpu.make_async_remote_copy(sib_g, sib_in_g, gain_sem.at[0], gain_sem.at[1],
                                             device_id=sibling, device_id_type=MESH)
    loads = [pltpu.make_async_copy(w_ref.at[pl.ds(8 * j, 8)], w_buf.at[j % 2], w_sem.at[j]) for j in range(strips)]
    loads[0].start()
    loads[1].start()
    transpose_into(normed_t, normed)
    own_g[...] = jnp.zeros_like(own_g)
    sib_g[...] = jnp.zeros_like(sib_g)
    chunks = own_q.shape[2] // CHUNK
    gifts = [chunk_gift(sib_out, sib_q, gift_send, gift_recv, j) for j in range(chunks)]
    grad_chunk(normed_t, d_qkv, sib_out, 1 - core, 0)
    greeted((1, -1, 2))
    gifts[0].start()
    for s in range(no):
        out.one(s, 1)
    ready = 0
    for j in range(chunks):
        if j + 1 < chunks:
            grad_chunk(normed_t, d_qkv, sib_out, 1 - core, j + 1)
            gifts[j + 1].start()
        grad_chunk(normed_t, d_qkv, own_q, core, j)
        gifts[j].wait_recv()
        while ready < nq and QKV[ready][1] + QKV[ready][2] <= (j + 1) * CHUNK:
            qkv.one(ready, 0)
            ready += 1
        if j == 1:
            for s in range(no):
                out.two(s, 1)
        if j == 3:
            for s in range(no):
                out.three(s, 1)
                out.one(s, 2)

    def strip(j):
        loads[j].wait()
        dn[:, pl.ds(j * CHUNK, CHUNK)] = nt(d_qkv[...], w_buf[j % 2].reshape(CHUNK, d_qkv.shape[1])).astype(bf)
        if j + 2 < strips:
            loads[j + 2].start()
    for j in range(strips // 2):
        strip(j)
    for s in range(nq):
        qkv.two(s, 0)
    for j in range(strips // 2, strips):
        strip(j)
    for s in range(nq):
        qkv.three(s, 0)
        qkv.one(s, 1)
    pre_row[...] = jnp.zeros_like(pre_row)
    one_gain = 1.0 + gain[pl.ds(0, 1), :]

    def back(i, carry):
        at = pl.ds(i * 32, 32)
        xs, g, inv = x_ref[at, :].astype(f32), dn[at, :].astype(f32), inv_rms[at, :]
        scaled = g * one_gain
        mean = jnp.sum(scaled * xs, axis=1, keepdims=True) * (1.0 / dim)
        dx_ref[at, :] = (dy_ref[at, :].astype(f32) + (inv * scaled - xs * (inv * inv * inv * mean))).astype(bf)
        pre_row[...] += jnp.sum((g * (xs * inv)).reshape(4, 8, dim), axis=0)
        return carry
    lax.fori_loop(0, n_tok // 32, back, 0)
    pre, post = jnp.sum(pre_row[...], axis=0, keepdims=True), post_row[...]
    own_row, sib_row = jnp.where(core == 0, pre, post), jnp.where(core == 0, post, pre)
    for j in range(16):
        for x in range(SIDE):
            own_g[SIDE * j + x, pl.ds(0, 1), :] = own_row[:, j * 128:(j + 1) * 128]
            sib_g[SIDE * j + x, pl.ds(0, 1), :] = sib_row[:, j * 128:(j + 1) * 128]
    gain_gift.start()
    for s in range(nq):
        qkv.two(s, 1)
    gain_gift.wait_recv()
    gains.one(0, 0)
    for s in range(no):
        out.three(s, 2)
    for s in range(nq):
        qkv.three(s, 1)
        qkv.one(s, 2)
    gains.three(0, 0)
    gains.one(0, 1)
    fins = []

    def give(scatter, ref):
        for s, (_, off, width) in enumerate(scatter.streams):
            k = len(fins)
            part = scatter.acc[s][2].at[0]
            ref[core, :, pl.ds(off, width)] = scatter.acc[s][2][0]
            here, there = (ref.at[side, :, pl.ds(off, width)] for side in (core, 1 - core))
            pair = [pltpu.make_async_remote_copy(part, side, fin_send.at[k], fin_recv.at[k],
                                                 device_id=sibling, device_id_type=MESH) for side in (here, there)]
            pair[0].start()
            fins.append(pair)
    give(out, out_o)
    for s in range(nq):
        qkv.three(s, 2)
    give(qkv, out_q)
    gains.three(0, 1)
    gains.one(0, 2)
    gains.three(0, 2)
    give(gains, out_g)
    for mine, theirs in fins:
        mine.wait_send()
        theirs.wait_recv()
    n_heads = grad_q.shape[1]
    per = out_q.shape[2] // TILE
    for h in range(n_heads + 2):
        part = out_q[h // per, :, pl.ds(h % per * TILE, TILE)]
        if h < n_heads:
            grad_q[:, h, :] = part
        else:
            (grad_k, grad_v)[h - n_heads][:, 0, :] = part
    for h in range(n_heads):
        grad_o[h] = out_o[h // 4, :, pl.ds(h % 4 * TILE, TILE)]
    for copy in gifts + [gain_gift]:
        copy.wait_send()
    for scatter, phases in ((qkv, (0, 1, 2)), (out, (1, 2)), (gains, (0, 1, 2))):
        for s in range(len(scatter.streams)):
            for q in phases:
                scatter.drain(s, q)


def scatter_grads(normed, d_qkv, w, x, dy, inv_rms, gain, post_row, accs, n_heads):
    bf, f32 = jnp.bfloat16, jnp.float32
    n_tok, model_dim = normed.shape
    half, rows = d_qkv.shape[1] // 2, 32
    blocks = model_dim // rows
    dma = pltpu.SemaphoreType.DMA
    vmem = pl.BlockSpec(memory_space=pltpu.VMEM)
    scratch = [pltpu.VMEM((model_dim, n_tok), bf), pltpu.VMEM((blocks, rows, half), f32),
               pltpu.VMEM((blocks, rows, half), bf), pltpu.VMEM((blocks, rows, half), bf)]
    scratch += [pltpu.VMEM((blocks, 16, 128), f32)] * 3
    scratch += [pltpu.VMEM((2, rows, half), f32), pltpu.VMEM((2, rows, 1024), f32),
                pltpu.VMEM((2, CHUNK // rows, rows, 2 * half), bf), pltpu.VMEM((n_tok, model_dim), bf),
                pltpu.VMEM((8, model_dim), f32)]
    for streams, dtype, n_rows, phases in ((QKV, bf, rows, (0, 1, 2)), (OUT, bf, rows, (1, 2)), (GAIN, f32, 16, (0, 1, 2))):
        scratch += [pltpu.VMEM(*a) for a in acc_shapes(streams, n_rows, phases)]
        scratch += wire_shapes(streams, dtype, n_rows, phases) * 2
    scratch += [dma((len(st), 3, 4)) for st in (QKV, OUT, GAIN) for _ in range(2)]
    scratch += [dma((half // CHUNK,))] * 2 + [dma((2,))] + [dma((len(QKV) + len(OUT) + 1,))] * 2 + [dma((model_dim // CHUNK,))]
    return pl.pallas_call(
        scatter_kernel, name="scatter_grads",
        out_shape=[jax.ShapeDtypeStruct((n_tok, model_dim), bf), jax.ShapeDtypeStruct((rows, n_heads, TILE), f32),
                   jax.ShapeDtypeStruct((rows, 1, TILE), f32), jax.ShapeDtypeStruct((rows, 1, TILE), f32),
                   jax.ShapeDtypeStruct((n_heads, rows, TILE), f32), jax.ShapeDtypeStruct((2, 16, 128), f32)],
        in_specs=[vmem] * 2 + [pl.BlockSpec(memory_space=pltpu.HBM)] + [vmem] * (5 + len(OUT)), out_specs=[vmem] * 6,
        scratch_shapes=scratch,
        compiler_params=pltpu.CompilerParams(collective_id=2, has_side_effects=True, vmem_limit_bytes=62914560),
    )(normed, d_qkv, w, x, dy, inv_rms, gain, post_row, *accs)


LOG2E = 1.4426950408889634
TILE = 256


def nt(a, b):
    return lax.dot_general(a, b, (((1,), (1,)), ((), ())), preferred_element_type=jnp.float32)


def nn(a, b):
    return lax.dot_general(a, b, (((1,), (0,)), ((), ())), preferred_element_type=jnp.float32)


def fill_mask(mask, pos):
    n_keys, n_q = mask.shape
    core = lax.axis_index('cp')
    for c in range(n_keys // TILE):
        base = jnp.where(c < n_q // TILE, (1 - core) * n_q, core * n_q - n_q) + c * TILE
        for i in range(n_q // TILE):
            k_at = base + lax.broadcasted_iota(jnp.int32, (TILE, TILE), 0)
            q_at = core * n_q + i * TILE + lax.broadcasted_iota(jnp.int32, (TILE, TILE), 1)
            seen = (k_at <= q_at) & (k_at >= q_at - pos[:, pl.ds(i * TILE, TILE)])
            mask[pl.ds(c * TILE, TILE), pl.ds(i * TILE, TILE)] = jnp.where(seen, 1.0, 0.0)


def keys_for(i, n_q):
    return n_q + (i + 1) * TILE


def forward_kernel(ratio, x_ref, cos_ref, sin_ref, pos, in0, in1, in2,
                   wq_out, wo_out, gain_out, normed, inv_rms, q_ref, kv_ref, o_ref, inv_ref,
                   wq, gains, gain_row, mask, v_t, w_scr, p_scr, *sems):
    n_q, dim = x_ref.shape
    bf, f32 = jnp.bfloat16, jnp.float32
    coords, core = place()
    sibling = device(coords, 1 - core)
    greet(coords, core, (1, -1, 2))
    own_sem, swap_send, swap_recv = sems[12:15]
    qkv, out, gain = (Gather(st, src, dst, direct, *sems[4 * g:4 * g + 4]) for g, (st, src, dst, direct) in enumerate(
        ((QKV, in0, wq, (0,)), (OUT, in1, wo_out, (0,)), (GAIN, in2, gains, (0, 1, 2)))))
    nq = range(len(QKV))
    wq[coords[0], coords[1], coords[2]] = in0[...]
    gains[coords[0], coords[1], coords[2]] = in2[...]
    greeted((1, -1, 2))
    gain.start(0, 0)
    for s in nq:
        qkv.start(s, 0)
    for s in range(len(OUT)):
        out.start(s, 0)
    own_out = pltpu.make_async_copy(in1, wo_out.at[coords[0], coords[1], coords[2]], own_sem.at[0])
    own_out.start()

    def stats(i, carry):
        at = pl.ds(i * 64, 64)
        v = x_ref[at, :].astype(f32)
        inv_rms[at, :] = lax.rsqrt(jnp.sum(v * v, axis=1, keepdims=True) * (1.0 / dim) + NORM_EPS)
        return carry
    lax.fori_loop(0, n_q // 64, stats, 0)
    gain.middle(0, 0)
    gain.start(0, 1)
    for s in nq:
        qkv.middle(s, 0)
        qkv.start(s, 1)
    gain.middle(0, 1)
    gain.start(0, 2)
    for s in range(len(OUT)):
        out.middle(s, 0)
    own_out.wait()
    for s in nq:
        qkv.middle(s, 1)
    for s in range(len(OUT)):
        out.start(s, 1)
    gain.middle(0, 2)
    for s in nq:
        qkv.finish(s, 1)
        qkv.start(s, 2)
    for p in range(3):
        gain.drain(0, p)
    for kind in range(2):
        for j in range(16):
            row = sum(gains[j // 4, j % 4, x, pl.ds(0, 1), pl.ds(kind * 128, 128)] for x in range(SIDE))
            gain_row[pl.ds(kind, 1), pl.ds(j * 128, 128)] = row
    gain_out[...] = gain_row[...]
    fill_mask(mask, pos)

    def scale(i, carry):
        at = pl.ds(i * 64, 64)
        normed[at, :] = (x_ref[at, :].astype(f32) * inv_rms[at, :] * (1.0 + gain_row[pl.ds(0, 1), :])).astype(bf)
        return carry
    lax.fori_loop(0, n_q // 64, scale, 0)
    for s in nq:
        qkv.middle(s, 2)
    for s in range(len(OUT)):
        out.middle(s, 1)
    for s in nq:
        qkv.finish(s, 2)
    for s in range(len(OUT)):
        out.finish(s, 1)
        out.start(s, 2)
    for s in nq:
        for p in range(3):
            qkv.drain(s, p)
    keep = pltpu.make_async_copy(wq, wq_out, own_sem.at[1])
    keep.start()

    def project(n):
        rhs = wq[:, :, :, :, pl.ds(pl.multiple_of(n * TILE, TILE), TILE)].reshape(dim, TILE)
        return nn(normed[...], rhs).astype(bf)

    def rope(u):
        lo, hi = u[:, :TILE // 2].astype(f32), u[:, TILE // 2:].astype(f32)
        c, s = cos_ref[...], sin_ref[...]
        return jnp.concatenate([lo * c - hi * s, hi * c + lo * s], axis=1).astype(bf)
    n_heads = q_ref.shape[1] // TILE
    mine, other = pl.ds(n_q, n_q), pl.ds(0, n_q)
    kv_ref[mine, pl.ds(0, TILE)] = rope(project(n_heads))
    kv_ref[mine, pl.ds(TILE, TILE)] = project(n_heads + 1)
    swap = pltpu.make_async_remote_copy(kv_ref.at[mine], kv_ref.at[other], swap_send.at[0], swap_recv.at[0],
                                        device_id=sibling, device_id_type=MESH)
    swap.start()

    def project_head(h, carry):
        q_ref[:, pl.ds(pl.multiple_of(h * TILE, TILE), TILE)] = rope(project(h))
        return carry
    lax.fori_loop(0, n_heads, project_head, 0)
    for s in range(len(OUT)):
        out.middle(s, 2)
    swap.wait_recv()
    k_cols = pl.ds(0, TILE)
    v_t[...] = kv_ref[:, pl.ds(TILE, TILE)].T

    def head(h, carry):
        cols = pl.ds(pl.multiple_of(h * TILE, TILE), TILE)
        for i in range(n_q // TILE):
            qi = q_ref[pl.ds(i * TILE, TILE), cols]
            n_keys = keys_for(i, n_q)
            total = jnp.zeros((8, TILE), f32)
            for c in range(n_keys // TILE):
                t = jnp.tanh(nt(kv_ref[pl.ds(c * TILE, TILE), k_cols], qi) * ratio)
                w = jnp.exp2(t * (SOFT_CAP * LOG2E)) * mask[pl.ds(c * TILE, TILE), pl.ds(i * TILE, TILE)]
                w_scr[i, pl.ds(c * TILE, TILE), :] = w
                total = total + jnp.sum(w.reshape(TILE // 8, 8, TILE), axis=0)
            inv = 1.0 / jnp.sum(total, axis=0, keepdims=True)
            inv_ref[h, :, pl.ds(i * TILE, TILE)] = inv
            p_scr[i, pl.ds(0, n_keys), :] = (w_scr[i, pl.ds(0, n_keys), :] * inv).astype(bf)
            o_t = nn(v_t[:, pl.ds(0, n_keys)], p_scr[i, pl.ds(0, n_keys), :])
            o_ref[pl.ds(i * TILE, TILE), cols] = o_t.T.astype(bf)
        return carry
    lax.fori_loop(0, n_heads, head, 0)
    for s in range(len(OUT)):
        out.finish(s, 2)
    for s in range(len(OUT)):
        for p in range(3):
            out.drain(s, p)
    swap.wait_send()
    keep.wait()


def forward(x, cos_t, sin_t, pos, w0, w1, w2, n_heads, ratio):
    n_q, dim = x.shape
    n_k = 2 * n_q
    bf, f32 = jnp.bfloat16, jnp.float32
    dma = pltpu.SemaphoreType.DMA
    vmem, hbm = pl.BlockSpec(memory_space=pltpu.VMEM), pl.BlockSpec(memory_space=pltpu.HBM)
    grid = (SIDE, SIDE, SIDE)
    shape = jax.ShapeDtypeStruct
    tiles = n_q // TILE
    return pl.pallas_call(
        functools.partial(forward_kernel, ratio), name="forward",
        out_shape=[shape(grid + w0.shape, bf), shape(grid + w1.shape, bf), shape((2, dim), f32), shape((n_q, dim), bf),
                   shape((n_q, 1), f32), shape((n_q, n_heads * TILE), bf), shape((n_k, 2 * TILE), bf),
                   shape((n_q, n_heads * TILE), bf), shape((n_heads, 1, n_q), f32)],
        in_specs=[vmem] * 7, out_specs=[hbm] * 2 + [vmem] * 7,
        scratch_shapes=[pltpu.VMEM(grid + w0.shape, bf), pltpu.VMEM(grid + w2.shape, f32), pltpu.VMEM((2, dim), f32),
                        pltpu.VMEM((n_k, n_q), f32), pltpu.VMEM((TILE, n_k), bf),
                        pltpu.VMEM((tiles, n_k, TILE), f32), pltpu.VMEM((tiles, n_k, TILE), bf)]
        + [dma((len(st), 3, 4)) for st in (QKV, OUT, GAIN) for _ in range(4)]
        + [dma((2,)), dma((1,)), dma((1,))],
        compiler_params=pltpu.CompilerParams(collective_id=1, has_side_effects=True, vmem_limit_bytes=48234496),
    )(x, cos_t, sin_t, pos, w0, w1, w2)


def attend_back_kernel(ratio, q_ref, do_ref, kv_ref, pos, inv_ref, dz_ref, o_ref, cos_ref, sin_ref,
                       dqkv_ref, *refs):
    no = len(OUT)
    accs = refs[:no]
    (mask, k_t, g_scr, dp_scr, p_scr, ds_scr, dk_acc, dv_acc, dkv_out, dkv_in, dz_t, own, sib_out, sib_in,
     *scratch) = refs[no:]
    n_q = q_ref.shape[0]
    coords, core = place()
    greet(coords, core)
    sbuf, rbuf, sems = scratch[:no], scratch[no:2 * no], scratch[2 * no:2 * no + 2]
    gift_send, gift_recv, swap_sem = scratch[2 * no + 2:]
    bf, f32 = jnp.bfloat16, jnp.float32
    swap = pltpu.make_async_remote_copy(dkv_out, dkv_in, swap_sem.at[0], swap_sem.at[1],
                                        device_id=device(coords, 1 - core), device_id_type=MESH)

    def rope_back(u):
        lo, hi = u[:, :TILE // 2].astype(f32), u[:, TILE // 2:].astype(f32)
        c, s = cos_ref[pl.ds(0, u.shape[0]), :], sin_ref[pl.ds(0, u.shape[0]), :]
        return jnp.concatenate([lo * c + hi * s, hi * c - lo * s], axis=1).astype(bf)
    out = Scatter(OUT, own, sib_in, [[a] for a in accs], [[b] for b in sbuf], [[b] for b in rbuf], (), *sems)
    chunks = own.shape[2] // CHUNK
    transpose_into(dz_t, dz_ref)
    gifts = [chunk_gift(sib_out, sib_in, gift_send, gift_recv, j) for j in range(chunks)]
    grad_chunk(dz_t, o_ref, sib_out, 1 - core, 0)
    greeted()
    gifts[0].start()
    ready = 0
    for j in range(chunks):
        if j + 1 < chunks:
            grad_chunk(dz_t, o_ref, sib_out, 1 - core, j + 1)
            gifts[j + 1].start()
        grad_chunk(dz_t, o_ref, own, core, j)
        gifts[j].wait_recv()
        while ready < no and OUT[ready][1] + OUT[ready][2] <= (j + 1) * CHUNK:
            out.one(ready, 0)
            ready += 1
    fill_mask(mask, pos)
    k_cols, v_cols = pl.ds(0, TILE), pl.ds(TILE, TILE)
    k_t[...] = kv_ref[:, k_cols].T
    dk_acc[...] = jnp.zeros_like(dk_acc)
    dv_acc[...] = jnp.zeros_like(dv_acc)

    def head(h, carry):
        cols = pl.ds(pl.multiple_of(h * TILE, TILE), TILE)
        for i in range(n_q // TILE):
            rows = pl.ds(i * TILE, TILE)
            qi, doi = q_ref[rows, cols], do_ref[rows, cols]
            inv = inv_ref[h, :, rows]
            n_keys = keys_for(i, n_q)
            total = jnp.zeros((8, TILE), jnp.float32)
            for c in range(n_keys // TILE):
                at = pl.ds(c * TILE, TILE)
                t = jnp.tanh(nt(kv_ref[at, k_cols], qi) * ratio)
                p = jnp.exp2(t * (SOFT_CAP * LOG2E)) * (mask[at, rows] * inv)
                dp = nt(kv_ref[at, v_cols], doi)
                p_scr[i, at, :] = p.astype(jnp.bfloat16)
                g_scr[i, at, :] = p * ((1.0 - t * t) * (ratio * SOFT_CAP))
                dp_scr[i, at, :] = dp
                total = total + jnp.sum((p * dp).reshape(TILE // 8, 8, TILE), axis=0)
            row_dot = jnp.sum(total, axis=0, keepdims=True)
            seen = pl.ds(0, n_keys)
            ds_scr[i, seen, :] = ((dp_scr[i, seen, :] - row_dot) * g_scr[i, seen, :]).astype(jnp.bfloat16)
            dq_t = nn(k_t[:, seen], ds_scr[i, seen, :])
            dq = dq_t.T.astype(bf)
            lo, hi = dq[:, :TILE // 2].astype(f32), dq[:, TILE // 2:].astype(f32)
            cos, sin = cos_ref[rows, :], sin_ref[rows, :]
            dqkv_ref[rows, cols] = jnp.concatenate([lo * cos + hi * sin, hi * cos - lo * sin], axis=1).astype(bf)
            dk_acc[seen, :] += nn(ds_scr[i, seen, :], qi)
            dv_acc[seen, :] += nn(p_scr[i, seen, :], doi)

        @pl.when(h == 3)
        def _():
            for s in range(no):
                out.two(s, 0)

        @pl.when(h == 6)
        def _():
            for s in range(no):
                out.three(s, 0)
        return carry
    lax.fori_loop(0, q_ref.shape[1] // TILE, head, 0)
    mine, other = pl.ds(n_q, n_q), pl.ds(0, n_q)
    dkv_out[:, k_cols] = dk_acc[other, :].astype(bf)
    dkv_out[:, v_cols] = dv_acc[other, :].astype(bf)
    swap.start()
    swap.wait_recv()
    q_cols = q_ref.shape[1]
    dqkv_ref[:, pl.ds(q_cols, TILE)] = rope_back((dk_acc[mine, :] + dkv_in[:, k_cols].astype(f32)).astype(bf))
    dqkv_ref[:, pl.ds(q_cols + TILE, TILE)] = (dv_acc[mine, :] + dkv_in[:, v_cols].astype(f32)).astype(bf)
    for s in range(len(OUT)):
        out.drain(s, 0)
    for copy in gifts + [swap]:
        copy.wait_send()


def attend_back(q, do, kv, pos, inv_sum, dz, o, cos_t, sin_t, ratio):
    n_q, n_k = q.shape[0], kv.shape[0]
    vmem = pl.BlockSpec(memory_space=pltpu.VMEM)
    tiles = n_q // TILE
    bf, f32 = jnp.bfloat16, jnp.float32
    return pl.pallas_call(
        functools.partial(attend_back_kernel, ratio), name="attend_back",
        out_shape=[jax.ShapeDtypeStruct((n_q, q.shape[1] + 2 * TILE), bf)]
        + [jax.ShapeDtypeStruct(*a) for a in acc_shapes(OUT, 32, (0,))],
        in_specs=[vmem] * 9, out_specs=[vmem] * (1 + len(OUT)),
        scratch_shapes=[pltpu.VMEM((n_k, n_q), f32), pltpu.VMEM((TILE, n_k), bf),
                        pltpu.VMEM((tiles, n_k, TILE), f32), pltpu.VMEM((tiles, n_k, TILE), f32),
                        pltpu.VMEM((tiles, n_k, TILE), bf), pltpu.VMEM((tiles, n_k, TILE), bf),
                        pltpu.VMEM((n_k, TILE), f32), pltpu.VMEM((n_k, TILE), f32),
                        pltpu.VMEM((n_q, 2 * TILE), bf), pltpu.VMEM((n_q, 2 * TILE), bf),
                        pltpu.VMEM((dz.shape[1], n_q), bf), pltpu.VMEM((dz.shape[1] // 32, 32, o.shape[1] // 2), f32)]
        + [pltpu.VMEM((dz.shape[1] // 32, 32, o.shape[1] // 2), bf)] * 2
        + wire_shapes(OUT, bf, 32, (0,)) * 2 + [pltpu.SemaphoreType.DMA((len(OUT), 3, 4))] * 2
        + [pltpu.SemaphoreType.DMA((o.shape[1] // 2 // CHUNK,))] * 2 + [pltpu.SemaphoreType.DMA((2,))],
        compiler_params=pltpu.CompilerParams(collective_id=4, has_side_effects=True, vmem_limit_bytes=56623104),
    )(q, do, kv, pos, inv_sum, dz, o, cos_t, sin_t)


def rope_tables(pos_ids, head_dim):
    half_dim = head_dim // 2
    inv_freq = ROPE_BASE ** (-2.0 * jnp.arange(half_dim, dtype=jnp.float32) / head_dim)
    angles = pos_ids.astype(jnp.float32)[..., None] * inv_freq
    return jnp.cos(angles)[..., None, :], jnp.sin(angles)[..., None, :]


def rotate(values, cos_t, sin_t):
    half_dim = values.shape[-1] // 2
    first_half = values[..., :half_dim].astype(jnp.float32)
    second_half = values[..., half_dim:].astype(jnp.float32)
    rotated = jnp.concatenate([first_half * cos_t - second_half * sin_t,
                               second_half * cos_t + first_half * sin_t], axis=-1)
    return rotated.astype(jnp.bfloat16)


def norm_forward(values, gain_vec):
    values_f = values.astype(jnp.float32)
    inv_rms = lax.rsqrt(jnp.mean(values_f * values_f, axis=-1, keepdims=True) + NORM_EPS)
    normed = values_f * inv_rms * (1.0 + gain_vec.astype(jnp.float32))
    return normed.astype(jnp.bfloat16), inv_rms


def norm_backward(values, inv_rms, gain_vec, grads):
    values_f = values.astype(jnp.float32)
    grads_f = grads.astype(jnp.float32)
    scaled = grads_f * (1.0 + gain_vec.astype(jnp.float32))
    d_values = inv_rms * scaled - values_f * inv_rms ** 3 * jnp.mean(scaled * values_f, axis=-1, keepdims=True)
    d_gain = jnp.sum(grads_f * values_f * inv_rms, axis=0)
    return d_values, d_gain


def dot(a, b, dims):
    return lax.dot_general(a, b, ((dims[:1], dims[1:]), ((), ())), preferred_element_type=jnp.float32)


def solution(mesh):
    tok_spec = P('fsdp', 'cp', None)
    ids_spec = P('fsdp', 'cp')
    in_spec = P('fsdp', None, None)
    out_spec = P(None, None, 'fsdp')
    gain_spec = P('fsdp')
    bf, f32 = jnp.bfloat16, jnp.float32

    def layer_local(hidden, doc_ids, doc_pos, grad_out, w_query, w_key, w_value, w_out, gain_pre, gain_post):
        _, n_tok, model_dim = hidden.shape
        hidden, grad_out = hidden[0], grad_out[0]
        n_heads, head_dim = w_query.shape[1], w_query.shape[2]
        rows = w_query.shape[0]
        q_cols = n_heads * head_dim
        w0 = jnp.concatenate([w_query.reshape(rows, q_cols), w_key.reshape(rows, head_dim),
                              w_value.reshape(rows, head_dim)], axis=1)
        w1 = w_out.reshape(q_cols, rows).T
        lane = lax.rem(lax.axis_index('fsdp'), SIDE) * rows
        w2 = jnp.zeros((8, 256), f32)
        for kind, g in enumerate((gain_pre, gain_post)):
            w2 = lax.dynamic_update_slice(w2, g.astype(f32)[None], (0, kind * 128 + lane))
        cos_t, sin_t = rope_tables(doc_pos[0], head_dim)
        q_scale = (head_dim if head_dim >= 256 else model_dim // n_heads) ** -0.5
        ratio = q_scale / SOFT_CAP
        wqkv, wo_t, gains, normed, inv_pre, q_flat, kv_all, attn_flat, inv_sum = forward(
            hidden, cos_t[:, 0], sin_t[:, 0], doc_pos, w0, w1, w2, n_heads, ratio)
        post_full = gains[1]
        wqkv = wqkv.reshape(model_dim // rows, rows, q_cols + 2 * head_dim)
        wo_t = wo_t.reshape(model_dim, q_cols)
        proj_out = dot(attn_flat, wo_t, (1, 1)).astype(bf)
        post_out, inv_post = norm_forward(proj_out, post_full)
        out_hidden = (hidden.astype(f32) + post_out.astype(f32)).astype(bf)

        d_proj, d_gain_post = norm_backward(proj_out, inv_post, post_full, grad_out)
        d_proj = d_proj.astype(bf)
        d_attn = dot(d_proj, wo_t, (1, 0)).astype(bf)

        d_qkv, *accs = attend_back(q_flat, d_attn, kv_all, doc_pos, inv_sum, d_proj, attn_flat, cos_t[:, 0], sin_t[:, 0], ratio)
        dx, g_q, g_k, g_v, g_o, g_g = scatter_grads(normed, d_qkv, wqkv, hidden, grad_out, inv_pre, gains,
                                                    d_gain_post[None], accs, n_heads)
        g_g = lax.dynamic_slice(g_g, (0, 0, lane), (2, 1, rows))[:, 0]
        return (out_hidden[None], dx[None], g_q, g_k, g_v, g_o.transpose(0, 2, 1),
                g_g[0], g_g[1])

    return jax.shard_map(layer_local, mesh=mesh,
                         in_specs=(tok_spec, ids_spec, ids_spec, tok_spec, in_spec, in_spec, in_spec, out_spec, gain_spec, gain_spec),
                         out_specs=(tok_spec, tok_spec, in_spec, in_spec, in_spec, out_spec, gain_spec, gain_spec),
                         check_vma=False)
```
